256 devices in a mesh: dp: 4 (over y_lo, core), sp: 8 (over y_hi, x), tp: 8 (over z).
Axes of the slice: x: 4, y: 4 (y_hi: 2, y_lo: 2; y = y_hi * 2 + y_lo), z: 8, core: 2. Of those that a mesh axis runs over, the one named last changes fastest.
Arguments:
- query: bfloat16 [4, 3072, 3072], P('dp', 'sp', 'tp'), may hold values from -110 to 110
- key: bfloat16 [4, 3072, 3072], P('dp', 'sp', 'tp'), may hold values from -8 to 8
- value: bfloat16 [4, 3072, 3072], P('dp', 'sp', 'tp'), may hold values from -6 to 6
- text_key: bfloat16 [4, 256, 3072], P('dp', None, 'tp'), may hold values from -6 to 6
- text_value: bfloat16 [4, 256, 3072], P('dp', None, 'tp'), may hold values from -6 to 6
- grad_out: bfloat16 [4, 3072, 3072], P('dp', 'sp', 'tp'), may hold values from -6 to 6
- gate: bfloat16 [4, 3072], P('dp'), may hold values from 0.5 to 1.5
- out_weight: bfloat16 [3072, 3072], P('tp', 'dp'), may hold values from -0.109375 to 0.109375
- windows: int32 [8, 2], P('sp'), may hold values from 0 to 2, as said below
- tile_map: int32 [8, 1], replicated, may hold values from 0 to 2, as said below
- text_count: int32 [4], P('dp'), may hold values from 1 to 256
Outputs:
- grad_query: bfloat16 [4, 3072, 3072], P('dp', 'sp', 'tp')
- grad_key: bfloat16 [4, 3072, 3072], P('dp', 'sp', 'tp')
- grad_value: bfloat16 [4, 3072, 3072], P('dp', 'sp', 'tp')
- grad_text_key: bfloat16 [4, 256, 3072], P('dp', None, 'tp')
- grad_text_value: bfloat16 [4, 256, 3072], P('dp', None, 'tp')
- grad_weight: float32 [3072, 3072], P('tp', 'dp')
The draws below stay inside these ranges and needn't reach their ends.
Inputs may be any that keep to these rules, and one draw needn't show every extreme that they name: `tile_map`: the positions within each row are distinct. `windows`: the time reach is 0 or 1; the first tile of every time slab has time reach 1 and spatial reach 2.
All inputs are finite; a program needn't handle non-finite values.
Results may differ from the reference program's by a relative error of at most 0.024.
Values may be sent and summed in bfloat16 or wider, within the bound.
A program may use at most 64 MiB of HBM per device.

```python
import jax
import jax.numpy as jnp
from jax import lax

D = 3072
HD = 128
TILE = 384
TILES_DEV = 1
TXT = 256
VTOK = 3072
SAMPLES = 4
NTILES = 8
N_SP = 8


def base_keys(key):
    raw = jax.random.normal(jax.random.fold_in(key, 11), (SAMPLES, VTOK, D), jnp.float32)
    return jnp.clip(raw, -6.0, 6.0)


def draw_key(key, part):
    keys = base_keys(key)
    return keys.astype(jnp.bfloat16)


def draw_query(key, part):
    fresh = jnp.clip(jax.random.normal(jax.random.fold_in(key, 13), (SAMPLES, VTOK, D), jnp.float32), -6.0, 6.0)
    return fresh.astype(jnp.bfloat16)


def draw_tile_map(key, part):
    streams = jax.random.split(jax.random.fold_in(key, 21), N_SP)
    orders = jax.vmap(lambda stream: jax.random.permutation(stream, 3 * TILES_DEV)[:TILES_DEV])(streams)
    orders = orders.astype(jnp.int32)
    highest = 3 * TILES_DEV - 1
    first_row = orders[0]
    has_lowest = jnp.any(first_row == 0)
    first_row = first_row.at[0].set(jnp.where(has_lowest, first_row[0], 0))
    orders = orders.at[0].set(first_row)
    last_row = orders[N_SP - 1]
    has_highest = jnp.any(last_row == highest)
    last_row = last_row.at[0].set(jnp.where(has_highest, last_row[0], highest))
    orders = orders.at[N_SP - 1].set(last_row)
    return orders.astype(jnp.int32)


def draw_windows(key, part):
    time_reach = jax.random.randint(jax.random.fold_in(key, 31), (NTILES,), 0, 2)
    space_reach = jax.random.randint(jax.random.fold_in(key, 32), (NTILES,), 0, 3 * TILES_DEV)
    first = jnp.arange(NTILES) % TILES_DEV == 0
    time_reach = jnp.where(first, 1, time_reach)
    space_reach = jnp.where(first, 3 * TILES_DEV - 1, space_reach)
    return jnp.stack([time_reach, space_reach], axis=1).astype(jnp.int32)


def place_ends(result, stream_key, least, top_value):
    longest = result.shape.index(max(result.shape))
    spots = []
    for shift in (0, 1):
        where = [jax.random.randint(jax.random.fold_in(stream_key, axis), (), 0, length) for axis, length in enumerate(result.shape)]
        where[longest] = (where[longest] + shift) % result.shape[longest]
        spots.append(tuple(where))
    return result.at[spots[0]].set(least).at[spots[1]].set(top_value)


def steps_of(own_key, shape, cuts, low, largest):
    level = 1.0
    for position, blocks in cuts:
        steps = jax.random.uniform(jax.random.fold_in(jax.random.fold_in(own_key, 6), position), (blocks,), jnp.float32, low / len(cuts), largest / len(cuts))
        level = level * jnp.repeat(jnp.exp(steps), shape[position] // blocks).reshape((-1,) + (1,) * (len(shape) - 1 - position))
    return level


def normal_values(own_key, dims, width, most, cuts=(), held_as=jnp.bfloat16):
    values = width * jax.random.normal(own_key, dims, jnp.float32)
    if cuts:
        values = values * steps_of(own_key, dims, cuts, -0.22, 0.18)
    return jnp.clip(values, -most, most).astype(held_as)


def setup_inputs(seed: int = 0) -> dict:
    streams_of = jax.random.split(jax.random.key(seed), 12)
    return {
        "query": draw_query(jax.random.fold_in(streams_of[11], 71), 0),
        "key": draw_key(jax.random.fold_in(streams_of[11], 71), 0),
        "value": normal_values(streams_of[2], (SAMPLES, VTOK, D), 1.0, 6.0, ((0, 4), (1, 8), (2, 8))),
        "text_key": normal_values(streams_of[3], (SAMPLES, TXT, D), 1.0, 6.0, ((0, 4), (2, 8))),
        "text_value": normal_values(streams_of[4], (SAMPLES, TXT, D), 1.0, 6.0, ((0, 4), (2, 8))),
        "grad_out": normal_values(streams_of[5], (SAMPLES, VTOK, D), 1.0, 6.0, ((0, 4), (1, 8), (2, 8))),
        "gate": jnp.clip(0.5 + 1.0 * jax.random.uniform(streams_of[6], (SAMPLES, D), jnp.float32) ** steps_of(streams_of[6], (SAMPLES, D), ((0, 4),), -0.2, 0.2), 0.5, 1.5).astype(jnp.bfloat16),
        "out_weight": normal_values(streams_of[7], (D, D), D ** -0.5, 0.109375, ((0, 8), (1, 4))),
        "windows": draw_windows(jax.random.fold_in(streams_of[11], 71), 0),
        "tile_map": draw_tile_map(jax.random.fold_in(streams_of[11], 71), 0),
        "text_count": place_ends(jax.random.randint(streams_of[10], (SAMPLES,), 1, TXT + 1), jax.random.fold_in(streams_of[10], 1), 1, TXT).astype(jnp.int32),
    }


def window_mask(own_map, side_maps, valid, spans, text_live):
    reach = jnp.abs(jnp.arange(3, dtype=jnp.int32) - 1)
    near_time = reach[None, :, None] <= spans[:, 0][:, None, None]
    near_space = jnp.abs(own_map[:, None, None] - side_maps[None, :, :]) <= spans[:, 1][:, None, None]
    allowed = near_time & near_space & valid[None, :, None]
    count = own_map.shape[0]
    tiles = allowed.reshape(count, 3 * count)
    video = jnp.broadcast_to(tiles[:, None, :, None], (count, TILE, 3 * count, TILE))
    video = video.reshape(count * TILE, 3 * count * TILE)
    text = jnp.broadcast_to(text_live[None, :], (count * TILE, text_live.shape[0]))
    return jnp.concatenate([video, text], axis=1)


def tile_attention(query, keys, values, grad_attn, allowed):
    factor = HD ** -0.5
    scores = factor * jnp.dot(query, keys.T, preferred_element_type=jnp.float32)
    scores = jnp.where(allowed, scores, -1e30)
    top = jnp.max(scores, axis=1, keepdims=True)
    weights = jnp.exp(scores - top)
    weights = weights / jnp.sum(weights, axis=1, keepdims=True)
    probs = weights.astype(jnp.bfloat16)
    attended = jnp.dot(probs, values, preferred_element_type=jnp.float32).astype(jnp.bfloat16)
    delta = jnp.sum(grad_attn.astype(jnp.float32) * attended.astype(jnp.float32), axis=1, keepdims=True)
    grad_probs = jnp.dot(grad_attn, values.T, preferred_element_type=jnp.float32)
    grad_scores = (weights * (grad_probs - delta)).astype(jnp.bfloat16)
    grad_query = factor * jnp.dot(grad_scores, keys, preferred_element_type=jnp.float32)
    grad_keys = factor * jnp.dot(grad_scores.T, query, preferred_element_type=jnp.float32)
    grad_values = jnp.dot(probs.T, grad_attn, preferred_element_type=jnp.float32)
    return attended, grad_query, grad_keys, grad_values


def gather_back(parts, slabs, tok):
    video = parts[:, :3 * tok].reshape(slabs, 3, tok, HD)
    empty = jnp.zeros((1, tok, HD), jnp.float32)
    total = video[:, 1] + jnp.concatenate([video[1:, 0], empty], axis=0)
    total = total + jnp.concatenate([empty, video[:-1, 2]], axis=0)
    return total.reshape(slabs * tok, HD), jnp.sum(parts[:, 3 * tok:], axis=0)


def reference(query, key, value, text_key, text_value, grad_out, gate, out_weight, windows, tile_map, text_count):
    slabs = N_SP
    tok = TILE * TILES_DEV
    heads = D // HD
    blank = jnp.zeros((1, TILES_DEV), jnp.int32)
    padded_map = jnp.concatenate([blank, tile_map.astype(jnp.int32), blank], axis=0)
    weight_grad = jnp.zeros((D, D), jnp.float32)
    outs = [[], [], [], [], []]
    for sample in range(SAMPLES):
        scaled = (grad_out[sample].astype(jnp.float32) * gate[sample].astype(jnp.float32)[None, :]).astype(jnp.bfloat16)
        grad_attn = jnp.dot(scaled, out_weight.T, preferred_element_type=jnp.float32).astype(jnp.bfloat16)
        text_live = jnp.arange(TXT, dtype=jnp.int32) < text_count[sample]

        def one_head(head):
            start = (head * HD).astype(jnp.int32)

            def cut(array):
                return lax.dynamic_slice_in_dim(array, start, HD, 1)

            queries = cut(query[sample]).reshape(slabs, tok, HD)
            grads = cut(grad_attn).reshape(slabs, tok, HD)
            zero_slab = jnp.zeros((1, tok, HD), jnp.bfloat16)
            keys = jnp.concatenate([zero_slab, cut(key[sample]).reshape(slabs, tok, HD), zero_slab], axis=0)
            vals = jnp.concatenate([zero_slab, cut(value[sample]).reshape(slabs, tok, HD), zero_slab], axis=0)
            text_k = cut(text_key[sample])
            text_v = cut(text_value[sample])

            def one_slab(slab):
                slab = slab.astype(jnp.int32)
                near_k = lax.dynamic_slice_in_dim(keys, slab, 3, 0).reshape(3 * tok, HD)
                near_v = lax.dynamic_slice_in_dim(vals, slab, 3, 0).reshape(3 * tok, HD)
                all_k = jnp.concatenate([near_k, text_k], axis=0)
                all_v = jnp.concatenate([near_v, text_v], axis=0)
                own_map = lax.dynamic_index_in_dim(tile_map.astype(jnp.int32), slab, 0, keepdims=False)
                side_maps = lax.dynamic_slice_in_dim(padded_map, slab, 3, 0)
                others = slab + jnp.arange(3, dtype=jnp.int32) - 1
                valid = (others >= 0) & (others < slabs)
                spans = lax.dynamic_slice_in_dim(windows.astype(jnp.int32), slab * TILES_DEV, TILES_DEV, 0)
                allowed = window_mask(own_map, side_maps, valid, spans, text_live)
                qs = lax.dynamic_index_in_dim(queries, slab, 0, keepdims=False)
                gs = lax.dynamic_index_in_dim(grads, slab, 0, keepdims=False)
                return tile_attention(qs, all_k, all_v, gs, allowed)

            attended, grad_q, grad_k, grad_v = lax.map(one_slab, jnp.arange(slabs, dtype=jnp.int32))
            video_k, text_gk = gather_back(grad_k, slabs, tok)
            video_v, text_gv = gather_back(grad_v, slabs, tok)
            return attended.reshape(slabs * tok, HD), grad_q.reshape(slabs * tok, HD), video_k, video_v, text_gk, text_gv

        results = lax.map(one_head, jnp.arange(heads, dtype=jnp.int32))

        def joined(stacked):
            return jnp.transpose(stacked, (1, 0, 2)).reshape(stacked.shape[1], D)

        attended = joined(results[0])
        weight_grad = weight_grad + jnp.dot(attended.T, scaled, preferred_element_type=jnp.float32)
        for place in range(5):
            outs[place].append(joined(results[place + 1]).astype(jnp.bfloat16))
    stacked = [jnp.stack(items, axis=0) for items in outs]
    return stacked[0], stacked[1], stacked[2], stacked[3], stacked[4], weight_grad
```

```python
import functools

import jax
import jax.numpy as jnp
from jax import lax
from jax.experimental import pallas as pl
from jax.experimental.pallas import tpu as pltpu
from jax.sharding import PartitionSpec as P

HD = 128
TILE = 384
TXT = 256
HEADS = 3
N_TP = 8
KEYS = 3 * TILE + TXT
R_TXT = TILE
R_NEAR = (TILE + TXT, 2 * TILE + TXT)
QS = 3 * TILE
FAR = 1e30
MESH = pl.DeviceIdType.MESH
F32 = jnp.float32
BF16 = jnp.bfloat16


def dot(a, b, ca, cb):
    return lax.dot_general(a, b, (((ca,), (cb,)), ((), ())), preferred_element_type=F32)


def body(
    q_in, k_in, v_in, tk_in, tv_in, g_in, gate_in, w_in, win, tmap, tcount,
    o_q, o_k, o_v, o_tk, o_tv, o_w,
    qc, kc, vc, graw, sbuf, wbuf, scores, probs, pnear, att, d_out, acc, d_near,
    st_out, st_in, dl_out, dl_in, dl_own, ds_keep,
    gbuf, g_d, g_a, g_y, g_r, g_r1, g_r2, g_hs, g_rh, g_fin,
    tx, t_r1, t_r2, t_hs, t_rh, t_fin,
    loc, zs, zr, hs_s, hs_r, qs_s, qs_r, ss_s, ss_r, do_s, do_r, ws, wr,
    ds_, dr_, ys, yr, gs, gr, ts, tr,
):
    factor = HD ** (-0.5)
    dp = lax.axis_index("dp")
    sp = lax.axis_index("sp")
    tp = lax.axis_index("tp")
    core = dp % 2
    ylo = dp // 2
    yhi = sp // 4
    x = sp % 4
    y = yhi * 2 + ylo

    def at_xy(xx, yy, cc):
        return ((yy % 2) * 2 + cc, (yy // 2) * 4 + xx, tp)

    z_dev = (
        (dp, sp, (tp + 1) % N_TP),
        (dp, sp, (tp + N_TP - 1) % N_TP),
    )
    partner = ((ylo * 2 + 1 - core), sp, tp)
    y_next = at_xy(x, (y + 1) % 4, core)
    y_prev = at_xy(x, (y + 3) % 4, core)
    p1 = (dp, yhi * 4 + x + 1 - 2 * (x % 2), tp)
    p2 = (dp, yhi * 4 + (x + 3 + 2 * (x % 2)) % 4, tp)
    across = (dp, (1 - yhi) * 4 + x, tp)
    near_dev = ((dp, jnp.maximum(sp - 1, 0), tp), (dp, jnp.minimum(sp + 1, 7), tp))
    has = (sp > 0, sp < 7)

    def rc(src, dst, s_sem, r_sem, dev):
        return pltpu.make_async_remote_copy(
            src_ref=src, dst_ref=dst, send_sem=s_sem, recv_sem=r_sem,
            device_id=dev, device_id_type=MESH,
        )

    barrier = pltpu.get_barrier_semaphore()
    for dev in (z_dev[0], z_dev[1], partner, y_next, y_prev, p1, p2, across):
        pl.semaphore_signal(barrier, inc=1, device_id=dev, device_id_type=MESH)

    @pl.when(sp == 3)
    def _():
        pl.semaphore_signal(barrier, inc=1, device_id=near_dev[1], device_id_type=MESH)

    @pl.when(sp == 4)
    def _():
        pl.semaphore_signal(barrier, inc=1, device_id=near_dev[0], device_id_type=MESH)

    gcopy = pltpu.make_async_copy(g_in, graw, loc.at[0])
    gcopy.start()
    wcopy = pltpu.make_async_copy(w_in, wbuf.at[dp], loc.at[1])
    wcopy.start()
    kcopies, qcopies, vcopies = [], [], []
    for h in range(HEADS):
        cols = slice(h * HD, (h + 1) * HD)
        kcopies.append(pltpu.make_async_copy(k_in.at[:, cols], kc.at[h, 0:TILE], loc.at[2 + h]))
        vcopies.append(pltpu.make_async_copy(v_in.at[:, cols], vc.at[h, 0:TILE], loc.at[5 + h]))
        qcopies.append(pltpu.make_async_copy(q_in.at[:, cols], qc.at[h, 0:TILE], loc.at[8 + h]))
        kcopies.append(
            pltpu.make_async_copy(tk_in.at[:, cols], kc.at[h, R_TXT : R_TXT + TXT], loc.at[11 + h])
        )
        vcopies.append(
            pltpu.make_async_copy(tv_in.at[:, cols], vc.at[h, R_TXT : R_TXT + TXT], loc.at[14 + h])
        )
    for copy in kcopies + vcopies + qcopies:
        copy.start()

    for n in range(2):

        @pl.when(jnp.logical_not(has[n]))
        def _():
            rows = slice(R_NEAR[n], R_NEAR[n] + TILE)
            qrows = slice(TILE * (n + 1), TILE * (n + 2))
            for h in range(HEADS):
                kc[h, rows, :] = jnp.zeros((TILE, HD), BF16)
                vc[h, rows, :] = jnp.zeros((TILE, HD), BF16)
                qc[h, qrows, :] = jnp.zeros((TILE, HD), BF16)
            d_near[n] = jnp.zeros((TILE, TILE), BF16)
            st_in[n] = jnp.full((8, TILE), FAR, F32)
            dl_in[n] = jnp.zeros((8, TILE), F32)

    gcopy.wait()
    gate_own = gate_in[:, pl.ds(pl.multiple_of(tp * TILE, 128), TILE)].astype(F32)
    sbuf[tp] = (graw[...].astype(F32) * gate_own).astype(BF16)

    n_extra = jnp.where((sp == 3) | (sp == 4), 1, 0)
    pl.semaphore_wait(barrier, 8 + n_extra)

    def z_unit(k, u, d):
        step = 1 - 2 * d
        chunk = (tp + N_TP - step * k) % N_TP
        ref = sbuf.at[chunk, pl.ds(u * 192, 192), :]
        return rc(ref, ref, zs.at[d, k, u], zr.at[d, k, u], z_dev[d])

    def z_wait(k, u, d):
        step = 1 - 2 * d
        chunk = (tp + N_TP - step * (k + 1)) % N_TP
        ref = sbuf.at[chunk, pl.ds(u * 192, 192), :]
        rc(ref, ref, zs.at[d, k, u], zr.at[d, k, u], z_dev[d]).wait_recv()

    for u in range(2):
        for d in range(2):
            z_unit(0, u, d).start()

    def z_service(k):
        for u in range(2):
            for d in range(2):
                z_wait(k - 1, u, d)
                if u == d:
                    z_unit(k, u, d).start()
                else:

                    @pl.when(k < 3)
                    def _():
                        z_unit(k, u, d).start()

    for copy in kcopies + vcopies:
        copy.wait()

    def halo(h, n, which, mine):
        src = (kc, vc)[which]
        slot = R_NEAR[1 - n] if mine else R_NEAR[n]
        return rc(
            src.at[h, 0:TILE], src.at[h, pl.ds(slot, TILE)],
            hs_s.at[n, h, which], hs_r.at[1 - n if mine else n, h, which], near_dev[n],
        )

    def q_halo(n, mine):
        slot = TILE * (2 - n) if mine else TILE * (1 + n)
        return rc(
            qc.at[:, pl.ds(0, TILE)], qc.at[:, pl.ds(slot, TILE)],
            qs_s.at[n], qs_r.at[1 - n if mine else n], near_dev[n],
        )

    for copy in qcopies:
        copy.wait()
    wcopy.wait()
    w_part = rc(wbuf.at[dp], wbuf.at[dp], ws.at[0], wr.at[0], partner)
    w_next = rc(wbuf.at[dp, 0:192], wbuf.at[dp, 0:192], ws.at[1], wr.at[1], y_next)
    w_prev = rc(wbuf.at[dp, 192:384], wbuf.at[dp, 192:384], ws.at[2], wr.at[2], y_prev)
    w_next.start()
    w_prev.start()
    w_part.start()
    for n in range(2):

        @pl.when(has[n])
        def _():
            for h in range(HEADS):
                halo(h, n, 0, True).start()
                halo(h, n, 1, True).start()
            q_halo(n, True).start()

    own_pos = tmap[sp, 0]
    bias = []
    for n in range(2):
        other = tmap[(jnp.maximum(sp - 1, 0), jnp.minimum(sp + 1, 7))[n], 0]
        seen = (win[0, 0] >= 1) & (jnp.abs(own_pos - other) <= win[0, 1]) & has[n]
        bias.append(jnp.where(seen, 0.0, -FAR).astype(F32))
    text_rows = lax.broadcasted_iota(jnp.int32, (TXT, 1), 0)
    text_bias = jnp.where(text_rows < tcount[0], 0.0, -FAR).astype(F32)

    def early(h, carry):
        queries = qc[h, 0:TILE, :]
        own = factor * dot(kc[h, 0:TILE, :], queries, 1, 1)
        scores[h, 0:TILE, :] = own
        text = factor * dot(kc[h, R_TXT : R_TXT + TXT, :], queries, 1, 1) + text_bias
        scores[h, R_TXT : R_TXT + TXT, :] = text
        return carry

    lax.fori_loop(0, HEADS, early, 0)

    other = (1 - ylo) * 2 + core
    w_fwd = []
    for half in range(2):
        rows = slice(half * 192, half * 192 + 192)
        ref = wbuf.at[other, rows]
        rc(ref, ref, ws.at[1 + half], wr.at[1 + half], y_next).wait_recv()
        fwd = rc(ref, ref, ws.at[3 + half], wr.at[3 + half], partner)
        fwd.start()
        w_fwd.append(fwd)
    mate = ylo * 2 + 1 - core
    mate_other = (1 - ylo) * 2 + 1 - core
    rc(wbuf.at[mate], wbuf.at[mate], ws.at[0], wr.at[0], partner).wait_recv()
    for half in range(2):
        ref = wbuf.at[mate_other, half * 192 : half * 192 + 192]
        rc(ref, ref, ws.at[3 + half], wr.at[3 + half], partner).wait_recv()

    def take(chunk):
        cols = pl.ds(pl.multiple_of((chunk % 2) * TILE, 128), TILE)
        return dot(wbuf[chunk // 2, :, cols], sbuf[chunk], 1, 1)

    acc[...] = take(tp)

    def forward(h, carry):
        queries = qc[h, 0:TILE, :]
        for n in range(2):

            @pl.when(has[n])
            def _():
                halo(h, n, 0, False).wait_recv()
                halo(h, n, 1, False).wait_recv()

            rows = slice(R_NEAR[n], R_NEAR[n] + TILE)
            scores[h, rows, :] = factor * dot(kc[h, rows, :], queries, 1, 1) + bias[n]
        top = jnp.max(scores[h], axis=0, keepdims=True)
        weights = jnp.exp(scores[h] - top)
        inv = 1.0 / jnp.sum(weights, axis=0, keepdims=True)
        probs[h] = (weights * inv).astype(BF16)
        for n in range(2):
            st_out[n, pl.ds(h, 1), :] = jnp.where(bias[n] < 0.0, FAR, top)
            st_out[n, pl.ds(h + 4, 1), :] = inv
        att[h] = dot(vc[h], probs[h], 0, 0).astype(BF16)
        z_service(h + 1)
        acc[...] += take((tp + h + 1) % N_TP) + take((tp + N_TP - h - 1) % N_TP)
        return carry

    lax.fori_loop(0, HEADS, forward, 0)

    def st_copy(n, mine):
        return rc(
            st_out.at[n], st_in.at[1 - n if mine else n],
            ss_s.at[n], ss_r.at[1 - n if mine else n], near_dev[n],
        )

    for n in range(2):

        @pl.when(has[n])
        def _():
            st_copy(n, True).start()

    def grad_w(chunk):
        full = dot(att[...].reshape(HEADS * HD, TILE), sbuf[chunk], 1, 0)
        cols = pl.ds(pl.multiple_of((chunk % 2) * TILE, 128), TILE)
        gbuf[chunk // 2, :, cols] = full.astype(BF16)

    def grad_w_step(i, carry):
        grad_w((tp + i + 5) % N_TP)
        return carry

    lax.fori_loop(0, 7, grad_w_step, 0)

    for n in range(2):

        @pl.when(has[n])
        def _():
            q_halo(n, False).wait_recv()
            st_copy(n, False).wait_recv()

        def near_probs(h, carry):
            s = factor * dot(kc[h, 0:TILE, :], qc[h, TILE * (n + 1) : TILE * (n + 2), :], 1, 1)
            p = jnp.exp(s - st_in[n, pl.ds(h, 1), :]) * st_in[n, pl.ds(h + 4, 1), :]
            pnear[n, h] = p.astype(BF16)
            return carry

        lax.fori_loop(0, HEADS, near_probs, 0)

    z_wait(3, 0, 0)
    z_wait(3, 1, 1)
    last = (tp + 4) % N_TP
    total = acc[...] + take(last)
    d_out[...] = total.astype(BF16)
    dl_out[...] = jnp.zeros((8, TILE), F32)
    for h in range(HEADS):
        both = d_out[h * HD : (h + 1) * HD, :].astype(F32) * att[h].astype(F32)
        dl_out[h : h + 1, :] = jnp.sum(both, axis=0, keepdims=True)

    def do_copy(n, mine, which):
        to = 1 - n if mine else n
        src, dst = ((d_out, d_near.at[to]), (dl_out, dl_in.at[to]))[which]
        return rc(src, dst, do_s.at[n, which], do_r.at[to, which], near_dev[n])

    for n in range(2):

        @pl.when(has[n])
        def _():
            do_copy(n, True, 1).start()
            do_copy(n, True, 0).start()

    grad_w(last)

    def d_copy(i, src_core):
        return rc(gbuf.at[i * 2 + 1 - core], g_d.at[i], ds_.at[i], dr_.at[i], partner)

    for i in range(2):
        d_copy(i, core).start()

    def backward(h, carry):
        lanes = pl.ds(pl.multiple_of(h * HD, 128), HD)
        grads = d_out[pl.ds(pl.multiple_of(h * HD, 128), HD), :]
        delta = dl_out[pl.ds(h, 1), :]
        g = dot(vc[h], grads, 1, 0)
        ds = (probs[h].astype(F32) * (g - delta)).astype(BF16)
        ds_keep[h] = ds[0:TILE, :]
        gq = factor * dot(kc[h], ds, 0, 0)
        o_q[:, lanes] = gq.T.astype(BF16)
        trows = slice(R_TXT, R_TXT + TXT)
        tx[0:TXT, lanes] = (factor * dot(ds[trows, :], qc[h, 0:TILE, :], 1, 0)).astype(BF16)
        tx[TXT : 2 * TXT, lanes] = dot(probs[h, trows, :], grads, 1, 1).astype(BF16)
        return carry

    lax.fori_loop(0, HEADS, backward, 0)

    g1 = (x % 2 + x // 2) % 2
    g2 = x // 2

    def summer(src, fin, r1, r2, hs, rh, s_sem, r_sem):
        rows = src.shape[0]
        part, half, quarter = rows // 2, rows // 4, rows // 8

        def at(ref, start, size):
            return ref.at[pl.ds(pl.multiple_of(start, 16), size), :]

        def rd(ref, start, size):
            return ref[pl.ds(pl.multiple_of(start, 16), size), :].astype(F32)

        a1, b1 = g1 * half, part + g2 * half
        a2, b2 = a1 + g2 * quarter, b1 + g1 * quarter
        na1, nb1 = (1 - g1) * half, part + (1 - g2) * half
        na2, nb2 = a1 + (1 - g2) * quarter, b1 + (1 - g1) * quarter
        copies = [
            (rc(at(src, na1, half), r1.at[0:half], s_sem.at[0], r_sem.at[0], p1),
             rc(at(src, nb1, half), r1.at[half : 2 * half], s_sem.at[1], r_sem.at[1], p2)),
            (rc(at(src, na2, quarter), r2.at[0:quarter], s_sem.at[2], r_sem.at[2], p2),
             rc(at(src, nb2, quarter), r2.at[quarter : 2 * quarter], s_sem.at[3], r_sem.at[3], p1)),
            (rc(hs, rh, s_sem.at[4], r_sem.at[4], across),),
            (rc(at(fin, a2, quarter), at(fin, a2, quarter), s_sem.at[5], r_sem.at[5], p2),
             rc(at(fin, b2, quarter), at(fin, b2, quarter), s_sem.at[6], r_sem.at[6], p1)),
            (rc(at(fin, a1, half), at(fin, a1, half), s_sem.at[7], r_sem.at[7], p1),
             rc(at(fin, b1, half), at(fin, b1, half), s_sem.at[8], r_sem.at[8], p2)),
        ]
        arrive = [
            (rc(at(fin, na2, quarter), at(fin, na2, quarter), s_sem.at[5], r_sem.at[5], p2),
             rc(at(fin, nb2, quarter), at(fin, nb2, quarter), s_sem.at[6], r_sem.at[6], p1)),
            (rc(at(fin, na1, half), at(fin, na1, half), s_sem.at[7], r_sem.at[7], p1),
             rc(at(fin, nb1, half), at(fin, nb1, half), s_sem.at[8], r_sem.at[8], p2)),
        ]

        def go(stage):
            if stage == 1:
                for c in copies[0]:
                    c.wait_recv()
                for start, low in ((a1, 0), (b1, half)):
                    at(src, start, half)[...] = (
                        rd(src, start, half) + r1[low : low + half, :].astype(F32)
                    ).astype(BF16)
            elif stage == 2:
                for c in copies[1]:
                    c.wait_recv()
                for start, low in ((a2, 0), (b2, quarter)):
                    hs[low : low + quarter, :] = (
                        rd(src, start, quarter) + r2[low : low + quarter, :].astype(F32)
                    ).astype(BF16)
            elif stage == 3:
                copies[2][0].wait_recv()
                for start, low in ((a2, 0), (b2, quarter)):
                    at(fin, start, quarter)[...] = (
                        hs[low : low + quarter, :].astype(F32)
                        + rh[low : low + quarter, :].astype(F32)
                    ).astype(BF16)
            elif stage >= 4:
                for c in arrive[stage - 4]:
                    c.wait_recv()
            if stage < 5:
                for c in copies[stage]:
                    c.start()
            else:
                for group in copies:
                    for c in group:
                        c.wait_send()

        return go

    t_go = summer(tx, t_fin, t_r1, t_r2, t_hs, t_rh, ts, tr)
    t_go(0)

    for i in range(2):
        d_copy(i, core).wait_recv()
    g_a[...] = (gbuf[(1 - ylo) * 2 + core].astype(F32) + g_d[1 - ylo].astype(F32)).astype(BF16)
    y_sends = [
        rc(g_a.at[0:192], g_y.at[0:192], ys.at[0], yr.at[0], y_next),
        rc(g_a.at[192:384], g_y.at[192:384], ys.at[1], yr.at[1], y_prev),
    ]
    for c in y_sends:
        c.start()
    g_r[...] = (gbuf[ylo * 2 + core].astype(F32) + g_d[ylo].astype(F32)).astype(BF16)

    t_go(1)
    for c in y_sends:
        c.wait_recv()
    g_r[...] = (g_r[...].astype(F32) + g_y[...].astype(F32)).astype(BF16)
    g_go = summer(g_r, g_fin, g_r1, g_r2, g_hs, g_rh, gs, gr)
    g_go(0)
    t_go(2)

    for n in range(2):

        @pl.when(has[n])
        def _():
            do_copy(n, False, 1).wait_recv()
            do_copy(n, False, 0).wait_recv()

    def own_keys(h, carry):
        lanes = pl.ds(pl.multiple_of(h * HD, 128), HD)
        hrows = pl.ds(pl.multiple_of(h * HD, 128), HD)
        gk = dot(ds_keep[h], qc[h, 0:TILE, :], 1, 0)
        gv = dot(probs[h, 0:TILE, :], d_out[hrows, :], 1, 1)
        for n in range(2):
            grads = d_near[n, hrows, :]
            p = pnear[n, h]
            g = dot(vc[h, 0:TILE, :], grads, 1, 0)
            ds = (p.astype(F32) * (g - dl_in[n, pl.ds(h, 1), :])).astype(BF16)
            gk += dot(ds, qc[h, TILE * (n + 1) : TILE * (n + 2), :], 1, 0)
            gv += dot(p, grads, 1, 1)
        o_k[:, lanes] = (factor * gk).astype(BF16)
        o_v[:, lanes] = gv.astype(BF16)
        return carry

    lax.fori_loop(0, HEADS, own_keys, 0)

    g_go(1)
    t_go(3)
    g_go(2)
    t_go(4)
    g_go(3)
    t_go(5)
    o_tk[...] = t_fin[0:TXT, :]
    o_tv[...] = t_fin[TXT : 2 * TXT, :]
    g_go(4)
    g_go(5)
    o_w[...] = g_fin[...].astype(F32)

    for d in range(2):
        for k in range(4):
            for u in range(2):
                if k < 3 or u == d:
                    z_unit(k, u, d).wait_send()
    for c in (w_part, w_next, w_prev, *w_fwd, *y_sends):
        c.wait_send()
    for i in range(2):
        d_copy(i, core).wait_send()
    for n in range(2):

        @pl.when(has[n])
        def _():
            for h in range(HEADS):
                halo(h, n, 0, True).wait_send()
                halo(h, n, 1, True).wait_send()
            q_halo(n, True).wait_send()
            st_copy(n, True).wait_send()
            do_copy(n, True, 0).wait_send()
            do_copy(n, True, 1).wait_send()


def per_device(
    query, key, value, text_key, text_value, grad_out, gate, out_weight, windows, tile_map, text_count
):
    anyspec = pl.BlockSpec(memory_space=pl.ANY)
    vmem = pl.BlockSpec(memory_space=pltpu.VMEM)
    smem = pl.BlockSpec(memory_space=pltpu.SMEM)
    sds = jax.ShapeDtypeStruct
    v = pltpu.VMEM
    dma = pltpu.SemaphoreType.DMA
    out = pl.pallas_call(
        body,
        out_shape=(
            sds((TILE, TILE), BF16),
            sds((TILE, TILE), BF16),
            sds((TILE, TILE), BF16),
            sds((TXT, TILE), BF16),
            sds((TXT, TILE), BF16),
            sds((TILE, 768), F32),
        ),
        in_specs=[anyspec] * 6 + [vmem, anyspec] + [smem] * 3,
        out_specs=(vmem,) * 6,
        scratch_shapes=[
            v((HEADS, QS, HD), BF16),
            v((HEADS, KEYS, HD), BF16),
            v((HEADS, KEYS, HD), BF16),
            v((TILE, TILE), BF16),
            v((N_TP, TILE, TILE), BF16),
            v((4, TILE, 768), BF16),
            v((HEADS, KEYS, TILE), F32),
            v((HEADS, KEYS, TILE), BF16),
            v((2, HEADS, TILE, TILE), BF16),
            v((HEADS, HD, TILE), BF16),
            v((TILE, TILE), BF16),
            v((TILE, TILE), F32),
            v((2, TILE, TILE), BF16),
            v((2, 8, TILE), F32),
            v((2, 8, TILE), F32),
            v((8, TILE), F32),
            v((2, 8, TILE), F32),
            v((8, TILE), F32),
            v((HEADS, TILE, TILE), BF16),
            v((4, TILE, 768), BF16),
            v((2, TILE, 768), BF16),
            v((TILE, 768), BF16),
            v((TILE, 768), BF16),
            v((TILE, 768), BF16),
            v((192, 768), BF16),
            v((96, 768), BF16),
            v((96, 768), BF16),
            v((96, 768), BF16),
            v((TILE, 768), BF16),
            v((2 * TXT, TILE), BF16),
            v((TXT, TILE), BF16),
            v((TXT // 2, TILE), BF16),
            v((TXT // 2, TILE), BF16),
            v((TXT // 2, TILE), BF16),
            v((2 * TXT, TILE), BF16),
            dma((17,)),
            dma((2, 4, 2)),
            dma((2, 4, 2)),
            dma((2, HEADS, 2)),
            dma((2, HEADS, 2)),
            dma((2,)),
            dma((2,)),
            dma((2,)),
            dma((2,)),
            dma((2, 2)),
            dma((2, 2)),
            dma((5,)),
            dma((5,)),
            dma((2,)),
            dma((2,)),
            dma((2,)),
            dma((2,)),
            dma((9,)),
            dma((9,)),
            dma((9,)),
            dma((9,)),
        ],
        compiler_params=pltpu.CompilerParams(
            collective_id=0, has_side_effects=True, vmem_limit_bytes=60 * 1024 * 1024
        ),
    )(
        query[0], key[0], value[0], text_key[0], text_value[0], grad_out[0], gate, out_weight,
        windows, tile_map, text_count,
    )
    return tuple(o[None] for o in out[:5]) + (out[5],)


def solution(mesh):
    placed = (
        P("dp", "sp", "tp"),
        P("dp", "sp", "tp"),
        P("dp", "sp", "tp"),
        P("dp", None, "tp"),
        P("dp", None, "tp"),
        P("dp", "sp", "tp"),
        P("dp", None),
        P("tp", "dp"),
        P("sp", None),
        P(),
        P("dp"),
    )
    return jax.shard_map(
        per_device,
        mesh=mesh,
        in_specs=placed,
        out_specs=(
            P("dp", "sp", "tp"),
            P("dp", "sp", "tp"),
            P("dp", "sp", "tp"),
            P("dp", None, "tp"),
            P("dp", None, "tp"),
            P("tp", "dp"),
        ),
        check_vma=False,
    )
```

```python
import functools

import jax
import jax.numpy as jnp
from jax import lax
from jax.experimental import pallas as pl
from jax.experimental.pallas import tpu as pltpu
from jax.sharding import PartitionSpec as P

HD = 128
TILE = 384
TXT = 256
HEADS = 3
N_TP = 8
KEYS = 3 * TILE + TXT
R_TXT = TILE
R_NEAR = (TILE + TXT, 2 * TILE + TXT)
QS = 3 * TILE
FAR = 1e30
MESH = pl.DeviceIdType.MESH
F32 = jnp.float32
BF16 = jnp.bfloat16


def dot(a, b, ca, cb):
    return lax.dot_general(a, b, (((ca,), (cb,)), ((), ())), preferred_element_type=F32)


def body(
    q_in, k_in, v_in, tk_in, tv_in, g_in, gate_in, w_in, win, tmap, tcount,
    o_q, o_k, o_v, o_tk, o_tv, o_w,
    qc, kc, vc, graw, sbuf, wbuf, scores, probs, pnear, att, d_out, acc, d_near,
    st_out, st_in, dl_out, dl_in, dl_own, ds_keep,
    gbuf, g_d, g_a, g_y, g_r, g_r1, g_r2, g_hs, g_rh, g_fin,
    tx, t_r1, t_r2, t_hs, t_rh, t_fin,
    rbuf, dbuf, loc, zs, zr, hs_s, hs_r, qs_s, qs_r, ss_s, ss_r, do_s, do_r, ws, wr,
    ds_, dr_, ys, yr, gs, gr, ts, tr, rs_s, rs_r, rf_s, rf_r, rd_s, rd_r, rg_s, rg_r,
):
    factor = HD ** (-0.5)
    dp = lax.axis_index("dp")
    sp = lax.axis_index("sp")
    tp = lax.axis_index("tp")
    core = dp % 2
    ylo = dp // 2
    yhi = sp // 4
    x = sp % 4
    y = yhi * 2 + ylo

    def at_xy(xx, yy, cc):
        return ((yy % 2) * 2 + cc, (yy // 2) * 4 + xx, tp)

    z_dev = (
        (dp, sp, (tp + 1) % N_TP),
        (dp, sp, (tp + N_TP - 1) % N_TP),
    )
    partner = ((ylo * 2 + 1 - core), sp, tp)
    y_next = at_xy(x, (y + 1) % 4, core)
    y_prev = at_xy(x, (y + 3) % 4, core)
    p1 = (dp, yhi * 4 + x + 1 - 2 * (x % 2), tp)
    p2 = (dp, yhi * 4 + (x + 3 + 2 * (x % 2)) % 4, tp)
    across = (dp, (1 - yhi) * 4 + x, tp)
    near_dev = ((dp, jnp.maximum(sp - 1, 0), tp), (dp, jnp.minimum(sp + 1, 7), tp))
    has = (sp > 0, sp < 7)

    def rc(src, dst, s_sem, r_sem, dev):
        return pltpu.make_async_remote_copy(
            src_ref=src, dst_ref=dst, send_sem=s_sem, recv_sem=r_sem,
            device_id=dev, device_id_type=MESH,
        )

    barrier = pltpu.get_barrier_semaphore()
    for dev in (z_dev[0], z_dev[1], partner, y_next, y_prev, p1, p2, across):
        pl.semaphore_signal(barrier, inc=1, device_id=dev, device_id_type=MESH)

    other = (1 - ylo) * 2 + core
    end = (sp == 3) | (sp == 4)
    relay = (x == 0) | (x == 3)
    to_later = (x == 0).astype(jnp.int32)
    relay_from = (other, 4 - to_later, tp)
    relay_to = (other, 3 + to_later, tp)
    relay_half = (yhi + 2 - ylo - to_later) % 2
    relays = []
    for half in range(2):
        mid = (half + ylo + jnp.where(sp == 3, 0, 1)) % 2
        relays.append((other, mid * 4 + jnp.where(sp == 3, 0, 3), tp))
    from_side = jnp.where(sp == 4, 0, 1)

    @pl.when(end)
    def _():
        for dev in ((other, 0, tp), (other, 3, tp), (other, 4, tp), (other, 7, tp), (dp, jnp.where(sp == 3, 4, 3), tp)):
            pl.semaphore_signal(barrier, inc=1, device_id=dev, device_id_type=MESH)

    @pl.when(relay)
    def _():
        for dev in ((other, 3, tp), (other, 4, tp)):
            pl.semaphore_signal(barrier, inc=1, device_id=dev, device_id_type=MESH)

    gcopy = pltpu.make_async_copy(g_in, graw, loc.at[0])
    gcopy.start()
    wcopy = pltpu.make_async_copy(w_in, wbuf.at[dp], loc.at[1])
    wcopy.start()
    kcopies, qcopies, vcopies = [], [], []
    for h in range(HEADS):
        cols = slice(h * HD, (h + 1) * HD)
        kcopies.append(pltpu.make_async_copy(k_in.at[:, cols], kc.at[h, 0:TILE], loc.at[2 + h]))
        vcopies.append(pltpu.make_async_copy(v_in.at[:, cols], vc.at[h, 0:TILE], loc.at[5 + h]))
        qcopies.append(pltpu.make_async_copy(q_in.at[:, cols], qc.at[h, 0:TILE], loc.at[8 + h]))
        kcopies.append(
            pltpu.make_async_copy(tk_in.at[:, cols], kc.at[h, R_TXT : R_TXT + TXT], loc.at[11 + h])
        )
        vcopies.append(
            pltpu.make_async_copy(tv_in.at[:, cols], vc.at[h, R_TXT : R_TXT + TXT], loc.at[14 + h])
        )
    for copy in kcopies + vcopies + qcopies:
        copy.start()

    for n in range(2):

        @pl.when(jnp.logical_not(has[n]))
        def _():
            rows = slice(R_NEAR[n], R_NEAR[n] + TILE)
            qrows = slice(TILE * (n + 1), TILE * (n + 2))
            for h in range(HEADS):
                kc[h, rows, :] = jnp.zeros((TILE, HD), BF16)
                vc[h, rows, :] = jnp.zeros((TILE, HD), BF16)
                qc[h, qrows, :] = jnp.zeros((TILE, HD), BF16)
            d_near[n] = jnp.zeros((TILE, TILE), BF16)
            st_in[n] = jnp.full((8, TILE), FAR, F32)
            dl_in[n] = jnp.zeros((8, TILE), F32)

    gcopy.wait()
    gate_own = gate_in[:, pl.ds(pl.multiple_of(tp * TILE, 128), TILE)].astype(F32)
    sbuf[tp] = (graw[...].astype(F32) * gate_own).astype(BF16)

    n_extra = jnp.where(end, 5, 0) + jnp.where(relay, 2, 0)
    pl.semaphore_wait(barrier, 8 + n_extra)

    def z_unit(k, u, d):
        step = 1 - 2 * d
        chunk = (tp + N_TP - step * k) % N_TP
        ref = sbuf.at[chunk, pl.ds(u * 192, 192), :]
        return rc(ref, ref, zs.at[d, k, u], zr.at[d, k, u], z_dev[d])

    def z_wait(k, u, d):
        step = 1 - 2 * d
        chunk = (tp + N_TP - step * (k + 1)) % N_TP
        ref = sbuf.at[chunk, pl.ds(u * 192, 192), :]
        rc(ref, ref, zs.at[d, k, u], zr.at[d, k, u], z_dev[d]).wait_recv()

    for u in range(2):
        for d in range(2):
            z_unit(0, u, d).start()

    def z_service(k):
        for u in range(2):
            for d in range(2):
                z_wait(k - 1, u, d)
                if k < 3 or u == d:
                    z_unit(k, u, d).start()

    for copy in kcopies + vcopies:
        copy.wait()

    def halo(h, n, which, mine):
        src = (kc, vc)[which]
        slot = R_NEAR[1 - n] if mine else R_NEAR[n]
        return rc(
            src.at[h, 0:TILE], src.at[h, pl.ds(slot, TILE)],
            hs_s.at[n, h, which], hs_r.at[1 - n if mine else n, h, which], near_dev[n],
        )

    def q_halo(n, mine):
        slot = TILE * (2 - n) if mine else TILE * (1 + n)
        return rc(
            qc.at[:, pl.ds(0, TILE)], qc.at[:, pl.ds(slot, TILE)],
            qs_s.at[n], qs_r.at[1 - n if mine else n], near_dev[n],
        )

    for copy in qcopies:
        copy.wait()
    wcopy.wait()
    w_part = rc(wbuf.at[dp], wbuf.at[dp], ws.at[0], wr.at[0], partner)
    w_next = rc(wbuf.at[dp, 0:192], wbuf.at[dp, 0:192], ws.at[1], wr.at[1], y_next)
    w_prev = rc(wbuf.at[dp, 192:384], wbuf.at[dp, 192:384], ws.at[2], wr.at[2], y_prev)
    w_next.start()
    w_prev.start()
    w_part.start()
    def side(n):
        return (sp == 4) if n == 0 else (sp == 3)

    plain = tuple(has[n] & jnp.logical_not(side(n)) for n in range(2))

    def piece_src(piece):
        if piece < 6:
            return (kc, vc)[piece % 2].at[piece // 2]
        return qc.at[piece - 6]

    def end_send(piece, half):
        rows = slice(half * 192, half * 192 + 192)
        return rc(
            piece_src(piece).at[rows], rbuf.at[piece],
            rs_s.at[half, piece], rs_r.at[piece], relays[half],
        )

    def forward_piece(piece):
        base = R_NEAR[0] if piece < 6 else TILE
        start = base + (1 - to_later) * TILE + relay_half * 192
        dst = piece_src(piece).at[pl.ds(pl.multiple_of(start, 16), 192), :]
        return rc(rbuf.at[piece], dst, rf_s.at[piece], rf_r.at[relay_half, piece], relay_to)

    def relay_pieces(pieces):
        @pl.when(relay)
        def _():
            for piece in pieces:
                rc(rbuf.at[piece], rbuf.at[piece], rf_s.at[piece], rs_r.at[piece], relay_from).wait_recv()
                forward_piece(piece).start()

    def end_wait(piece):
        for half in range(2):
            start = (R_NEAR[0] if piece < 6 else TILE) + from_side * TILE + half * 192
            dst = piece_src(piece).at[pl.ds(pl.multiple_of(start, 16), 192), :]
            rc(dst, dst, rf_s.at[piece], rf_r.at[half, piece], relays[half]).wait_recv()

    @pl.when(end)
    def _():
        for piece in range(9):
            for half in range(2):
                end_send(piece, half).start()

    for n in range(2):

        @pl.when(plain[n])
        def _():
            for h in range(HEADS):
                halo(h, n, 0, True).start()
                halo(h, n, 1, True).start()
            q_halo(n, True).start()

    own_pos = tmap[pl.ds(sp, 1), :]
    bias = []
    for n in range(2):
        near_pos = tmap[pl.ds((jnp.maximum(sp - 1, 0), jnp.minimum(sp + 1, 7))[n], 1), :]
        reach = jnp.where((win[0, 0] >= 1) & has[n], win[0, 1], -1)
        bias.append(jnp.where(jnp.abs(own_pos - near_pos) <= reach, 0.0, -FAR).astype(F32))
    text_rows = lax.broadcasted_iota(jnp.int32, (TXT, 1), 0)
    text_bias = jnp.where(text_rows < tcount[0], 0.0, -FAR).astype(F32)

    def early(h, carry):
        queries = qc[h, 0:TILE, :]
        own = factor * dot(kc[h, 0:TILE, :], queries, 1, 1)
        scores[h, 0:TILE, :] = own
        text = factor * dot(kc[h, R_TXT : R_TXT + TXT, :], queries, 1, 1) + text_bias
        scores[h, R_TXT : R_TXT + TXT, :] = text
        return carry

    lax.fori_loop(0, HEADS, early, 0)

    def take(chunk):
        cols = pl.ds(pl.multiple_of((chunk % 2) * TILE, 128), TILE)
        return dot(wbuf[chunk // 2, :, cols], sbuf[chunk], 1, 1)

    def forward(h):
        queries = qc[h, 0:TILE, :]
        for n in range(2):

            @pl.when(plain[n])
            def _():
                halo(h, n, 0, False).wait_recv()
                halo(h, n, 1, False).wait_recv()

        @pl.when(end)
        def _():
            end_wait(2 * h)
            end_wait(2 * h + 1)

        for n in range(2):
            rows = slice(R_NEAR[n], R_NEAR[n] + TILE)
            scores[h, rows, :] = factor * dot(kc[h, rows, :], queries, 1, 1) + bias[n]
        top = jnp.max(scores[h], axis=0, keepdims=True)
        weights = jnp.exp(scores[h] - top)
        inv = 1.0 / jnp.sum(weights, axis=0, keepdims=True)
        probs[h] = (weights * inv).astype(BF16)
        for n in range(2):
            st_out[n, h : h + 1, :] = jnp.where(bias[n] < 0.0, FAR, top)
            st_out[n, h + 4 : h + 5, :] = inv
        att[h] = dot(vc[h], probs[h], 0, 0).astype(BF16)

    relay_pieces((0, 1))
    z_service(1)
    forward(0)
    relay_pieces((2, 3))
    forward(1)
    w_fwd = []
    for half in range(2):
        rows = slice(half * 192, half * 192 + 192)
        ref = wbuf.at[other, rows]
        rc(ref, ref, ws.at[1 + half], wr.at[1 + half], y_next).wait_recv()
        fwd = rc(ref, ref, ws.at[3 + half], wr.at[3 + half], partner)
        fwd.start()
        w_fwd.append(fwd)
    z_service(2)
    relay_pieces((4, 5))
    forward(2)
    def st_copy(n, mine):
        return rc(
            st_out.at[n], st_in.at[1 - n if mine else n],
            ss_s.at[n], ss_r.at[1 - n if mine else n], near_dev[n],
        )

    for n in range(2):

        @pl.when(has[n])
        def _():
            st_copy(n, True).start()

    mate = ylo * 2 + 1 - core
    mate_other = (1 - ylo) * 2 + 1 - core
    rc(wbuf.at[mate], wbuf.at[mate], ws.at[0], wr.at[0], partner).wait_recv()
    for half in range(2):
        ref = wbuf.at[mate_other, half * 192 : half * 192 + 192]
        rc(ref, ref, ws.at[3 + half], wr.at[3 + half], partner).wait_recv()

    acc[...] = take(tp)

    def more(h, carry):
        acc[...] += take((tp + h + 1) % N_TP) + take((tp + N_TP - h - 1) % N_TP)
        return carry

    lax.fori_loop(0, 2, more, 0)

    def grad_w(chunk):
        full = dot(att[...].reshape(HEADS * HD, TILE), sbuf[chunk], 1, 0)
        cols = pl.ds(pl.multiple_of((chunk % 2) * TILE, 128), TILE)
        gbuf[chunk // 2, :, cols] = full.astype(BF16)

    def grad_w_step(i, carry):
        grad_w((tp + i + 5) % N_TP)
        return carry

    lax.fori_loop(1, 6, grad_w_step, 0)
    relay_pieces((6, 7, 8))
    z_service(3)
    more(2, 0)
    grad_w((tp + 5) % N_TP)
    grad_w((tp + 3) % N_TP)

    for n in range(2):

        @pl.when(plain[n])
        def _():
            q_halo(n, False).wait_recv()

        @pl.when(side(n))
        def _():
            for piece in (6, 7, 8):
                end_wait(piece)

        @pl.when(has[n])
        def _():
            st_copy(n, False).wait_recv()

        def near_probs(h, carry):
            s = factor * dot(kc[h, 0:TILE, :], qc[h, TILE * (n + 1) : TILE * (n + 2), :], 1, 1)
            p = jnp.exp(s - st_in[n, pl.ds(h, 1), :]) * st_in[n, pl.ds(h + 4, 1), :]
            pnear[n, h] = p.astype(BF16)
            return carry

        lax.fori_loop(0, HEADS, near_probs, 0)

    z_wait(3, 0, 0)
    z_wait(3, 1, 1)
    last = (tp + 4) % N_TP
    total = acc[...] + take(last)
    d_out[...] = total.astype(BF16)
    dl_out[...] = jnp.zeros((8, TILE), F32)
    for h in range(HEADS):
        both = d_out[h * HD : (h + 1) * HD, :].astype(F32) * att[h].astype(F32)
        dl_out[h : h + 1, :] = jnp.sum(both, axis=0, keepdims=True)

    def do_copy(n, mine, which):
        to = 1 - n if mine else n
        src, dst = ((d_out, d_near.at[to]), (dl_out, dl_in.at[to]))[which]
        return rc(src, dst, do_s.at[n, which], do_r.at[to, which], near_dev[n])

    half_rows = HD // 2

    def end_grad(h, half):
        rows = slice(h * HD + half * half_rows, h * HD + (half + 1) * half_rows)
        return rc(d_out.at[rows], dbuf.at[h], rd_s.at[half, h], rd_r.at[h], relays[half])

    def forward_grad(h):
        rows = pl.ds(pl.multiple_of(h * HD + relay_half * half_rows, 16), half_rows)
        dst = d_near.at[1 - to_later, rows, :]
        return rc(dbuf.at[h], dst, rg_s.at[h], rg_r.at[relay_half, h], relay_to)

    def relay_grads():
        @pl.when(relay)
        def _():
            for h in range(HEADS):
                rc(dbuf.at[h], dbuf.at[h], rg_s.at[h], rd_r.at[h], relay_from).wait_recv()
                forward_grad(h).start()

    def end_grad_wait():
        for h in range(HEADS):
            for half in range(2):
                rows = slice(h * HD + half * half_rows, h * HD + (half + 1) * half_rows)
                dst = d_near.at[from_side, rows, :]
                rc(dst, dst, rg_s.at[h], rg_r.at[half, h], relays[half]).wait_recv()

    @pl.when(end)
    def _():
        for h in range(HEADS):
            for half in range(2):
                end_grad(h, half).start()

    for n in range(2):

        @pl.when(has[n])
        def _():
            do_copy(n, True, 1).start()

        @pl.when(plain[n])
        def _():
            do_copy(n, True, 0).start()

    grad_w(last)

    def d_copy(i, src_core):
        return rc(gbuf.at[i * 2 + 1 - core], g_d.at[i], ds_.at[i], dr_.at[i], partner)

    for i in range(2):
        d_copy(i, core).start()

    def backward(h, carry):
        lanes = pl.ds(pl.multiple_of(h * HD, 128), HD)
        grads = d_out[pl.ds(pl.multiple_of(h * HD, 128), HD), :]
        delta = dl_out[pl.ds(h, 1), :]
        g = dot(vc[h], grads, 1, 0)
        ds = (probs[h].astype(F32) * (g - delta)).astype(BF16)
        ds_keep[h] = ds[0:TILE, :]
        gq = factor * dot(kc[h], ds, 0, 0)
        o_q[:, lanes] = gq.T.astype(BF16)
        trows = slice(R_TXT, R_TXT + TXT)
        tx[0:TXT, lanes] = (factor * dot(ds[trows, :], qc[h, 0:TILE, :], 1, 0)).astype(BF16)
        tx[TXT : 2 * TXT, lanes] = dot(probs[h, trows, :], grads, 1, 1).astype(BF16)
        return carry

    lax.fori_loop(0, HEADS, backward, 0)

    g1 = (x % 2 + x // 2) % 2
    g2 = x // 2

    def summer(src, fin, r1, r2, hs, rh, s_sem, r_sem):
        rows = src.shape[0]
        part, half, quarter = rows // 2, rows // 4, rows // 8

        def at(ref, start, size):
            return ref.at[pl.ds(pl.multiple_of(start, 16), size), :]

        def rd(ref, start, size):
            return ref[pl.ds(pl.multiple_of(start, 16), size), :].astype(F32)

        a1, b1 = g1 * half, part + g2 * half
        a2, b2 = a1 + g2 * quarter, b1 + g1 * quarter
        na1, nb1 = (1 - g1) * half, part + (1 - g2) * half
        na2, nb2 = a1 + (1 - g2) * quarter, b1 + (1 - g1) * quarter
        copies = [
            (rc(at(src, na1, half), r1.at[0:half], s_sem.at[0], r_sem.at[0], p1),
             rc(at(src, nb1, half), r1.at[half : 2 * half], s_sem.at[1], r_sem.at[1], p2)),
            (rc(at(src, na2, quarter), r2.at[0:quarter], s_sem.at[2], r_sem.at[2], p2),
             rc(at(src, nb2, quarter), r2.at[quarter : 2 * quarter], s_sem.at[3], r_sem.at[3], p1)),
            (rc(hs, rh, s_sem.at[4], r_sem.at[4], across),),
            (rc(at(fin, a2, quarter), at(fin, a2, quarter), s_sem.at[5], r_sem.at[5], p2),
             rc(at(fin, b2, quarter), at(fin, b2, quarter), s_sem.at[6], r_sem.at[6], p1)),
            (rc(at(fin, a1, half), at(fin, a1, half), s_sem.at[7], r_sem.at[7], p1),
             rc(at(fin, b1, half), at(fin, b1, half), s_sem.at[8], r_sem.at[8], p2)),
        ]
        arrive = [
            (rc(at(fin, na2, quarter), at(fin, na2, quarter), s_sem.at[5], r_sem.at[5], p2),
             rc(at(fin, nb2, quarter), at(fin, nb2, quarter), s_sem.at[6], r_sem.at[6], p1)),
            (rc(at(fin, na1, half), at(fin, na1, half), s_sem.at[7], r_sem.at[7], p1),
             rc(at(fin, nb1, half), at(fin, nb1, half), s_sem.at[8], r_sem.at[8], p2)),
        ]

        def go(stage):
            if stage == 1:
                for c in copies[0]:
                    c.wait_recv()
                for start, low in ((a1, 0), (b1, half)):
                    at(src, start, half)[...] = (
                        rd(src, start, half) + r1[low : low + half, :].astype(F32)
                    ).astype(BF16)
            elif stage == 2:
                for c in copies[1]:
                    c.wait_recv()
                for start, low in ((a2, 0), (b2, quarter)):
                    hs[low : low + quarter, :] = (
                        rd(src, start, quarter) + r2[low : low + quarter, :].astype(F32)
                    ).astype(BF16)
            elif stage == 3:
                copies[2][0].wait_recv()
                for start, low in ((a2, 0), (b2, quarter)):
                    at(fin, start, quarter)[...] = (
                        hs[low : low + quarter, :].astype(F32)
                        + rh[low : low + quarter, :].astype(F32)
                    ).astype(BF16)
            elif stage >= 4:
                for c in arrive[stage - 4]:
                    c.wait_recv()
            if stage < 5:
                for c in copies[stage]:
                    c.start()
            else:
                for group in copies:
                    for c in group:
                        c.wait_send()

        return go

    t_go = summer(tx, t_fin, t_r1, t_r2, t_hs, t_rh, ts, tr)
    t_go(0)

    relay_grads()
    for i in range(2):
        d_copy(i, core).wait_recv()
    g_a[...] = (gbuf[(1 - ylo) * 2 + core].astype(F32) + g_d[1 - ylo].astype(F32)).astype(BF16)
    y_sends = [
        rc(g_a.at[0:192], g_y.at[0:192], ys.at[0], yr.at[0], y_next),
        rc(g_a.at[192:384], g_y.at[192:384], ys.at[1], yr.at[1], y_prev),
    ]
    for c in y_sends:
        c.start()
    g_r[...] = (gbuf[ylo * 2 + core].astype(F32) + g_d[ylo].astype(F32)).astype(BF16)

    t_go(1)
    for c in y_sends:
        c.wait_recv()
    g_r[...] = (g_r[...].astype(F32) + g_y[...].astype(F32)).astype(BF16)
    g_go = summer(g_r, g_fin, g_r1, g_r2, g_hs, g_rh, gs, gr)
    g_go(0)
    t_go(2)

    for n in range(2):

        @pl.when(has[n])
        def _():
            do_copy(n, False, 1).wait_recv()

        @pl.when(plain[n])
        def _():
            do_copy(n, False, 0).wait_recv()

    @pl.when(end)
    def _():
        end_grad_wait()

    def own_keys(h, carry):
        lanes = pl.ds(pl.multiple_of(h * HD, 128), HD)
        hrows = pl.ds(pl.multiple_of(h * HD, 128), HD)
        gk = dot(ds_keep[h], qc[h, 0:TILE, :], 1, 0)
        gv = dot(probs[h, 0:TILE, :], d_out[hrows, :], 1, 1)
        for n in range(2):
            grads = d_near[n, hrows, :]
            p = pnear[n, h]
            g = dot(vc[h, 0:TILE, :], grads, 1, 0)
            ds = (p.astype(F32) * (g - dl_in[n, pl.ds(h, 1), :])).astype(BF16)
            gk += dot(ds, qc[h, TILE * (n + 1) : TILE * (n + 2), :], 1, 0)
            gv += dot(p, grads, 1, 1)
        o_k[:, lanes] = (factor * gk).astype(BF16)
        o_v[:, lanes] = gv.astype(BF16)
        return carry

    lax.fori_loop(0, HEADS, own_keys, 0)

    g_go(1)
    t_go(3)
    g_go(2)
    t_go(4)
    g_go(3)
    t_go(5)
    o_tk[...] = t_fin[0:TXT, :]
    o_tv[...] = t_fin[TXT : 2 * TXT, :]
    g_go(4)
    g_go(5)
    o_w[...] = g_fin[...]

    for d in range(2):
        for k in range(4):
            for u in range(2):
                if k < 3 or u == d:
                    z_unit(k, u, d).wait_send()
    for c in (w_part, w_next, w_prev, *w_fwd, *y_sends):
        c.wait_send()
    for i in range(2):
        d_copy(i, core).wait_send()
    for n in range(2):

        @pl.when(plain[n])
        def _():
            for h in range(HEADS):
                halo(h, n, 0, True).wait_send()
                halo(h, n, 1, True).wait_send()
            q_halo(n, True).wait_send()
            do_copy(n, True, 0).wait_send()

        @pl.when(has[n])
        def _():
            st_copy(n, True).wait_send()
            do_copy(n, True, 1).wait_send()

    @pl.when(end)
    def _():
        for half in range(2):
            for piece in range(9):
                end_send(piece, half).wait_send()
            for h in range(HEADS):
                end_grad(h, half).wait_send()

    @pl.when(relay)
    def _():
        for piece in range(9):
            forward_piece(piece).wait_send()
        for h in range(HEADS):
            forward_grad(h).wait_send()


def finish(*refs):
    given, results, wide, sems = refs[:6], refs[6:12], refs[12], refs[13]
    copies = []
    for i in range(5):
        copies.append(pltpu.make_async_copy(given[i], results[i].at[0], sems.at[i]))
        copies[-1].start()
    wide[...] = given[5][...].astype(F32)
    copies.append(pltpu.make_async_copy(wide, results[5], sems.at[5]))
    copies[-1].start()
    for copy in copies:
        copy.wait()


def per_device(
    query, key, value, text_key, text_value, grad_out, gate, out_weight, windows, tile_map, text_count
):
    anyspec = pl.BlockSpec(memory_space=pl.ANY)
    vmem = pl.BlockSpec(memory_space=pltpu.VMEM)
    smem = pl.BlockSpec(memory_space=pltpu.SMEM)
    sds = jax.ShapeDtypeStruct
    v = pltpu.VMEM
    dma = pltpu.SemaphoreType.DMA
    out = pl.pallas_call(
        body,
        out_shape=(
            sds((TILE, TILE), BF16),
            sds((TILE, TILE), BF16),
            sds((TILE, TILE), BF16),
            sds((TXT, TILE), BF16),
            sds((TXT, TILE), BF16),
            sds((TILE, 768), BF16),
        ),
        in_specs=[anyspec] * 6 + [vmem, anyspec, smem, vmem, smem],
        out_specs=(vmem,) * 6,
        scratch_shapes=[
            v((HEADS, QS, HD), BF16),
            v((HEADS, KEYS, HD), BF16),
            v((HEADS, KEYS, HD), BF16),
            v((TILE, TILE), BF16),
            v((N_TP, TILE, TILE), BF16),
            v((4, TILE, 768), BF16),
            v((HEADS, KEYS, TILE), F32),
            v((HEADS, KEYS, TILE), BF16),
            v((2, HEADS, TILE, TILE), BF16),
            v((HEADS, HD, TILE), BF16),
            v((TILE, TILE), BF16),
            v((TILE, TILE), F32),
            v((2, TILE, TILE), BF16),
            v((2, 8, TILE), F32),
            v((2, 8, TILE), F32),
            v((8, TILE), F32),
            v((2, 8, TILE), F32),
            v((8, TILE), F32),
            v((HEADS, TILE, TILE), BF16),
            v((4, TILE, 768), BF16),
            v((2, TILE, 768), BF16),
            v((TILE, 768), BF16),
            v((TILE, 768), BF16),
            v((TILE, 768), BF16),
            v((192, 768), BF16),
            v((96, 768), BF16),
            v((96, 768), BF16),
            v((96, 768), BF16),
            v((TILE, 768), BF16),
            v((2 * TXT, TILE), BF16),
            v((TXT, TILE), BF16),
            v((TXT // 2, TILE), BF16),
            v((TXT // 2, TILE), BF16),
            v((TXT // 2, TILE), BF16),
            v((2 * TXT, TILE), BF16),
            v((9, 192, HD), BF16),
            v((HEADS, HD // 2, TILE), BF16),
            dma((17,)),
            dma((2, 4, 2)),
            dma((2, 4, 2)),
            dma((2, HEADS, 2)),
            dma((2, HEADS, 2)),
            dma((2,)),
            dma((2,)),
            dma((2,)),
            dma((2,)),
            dma((2, 2)),
            dma((2, 2)),
            dma((5,)),
            dma((5,)),
            dma((2,)),
            dma((2,)),
            dma((2,)),
            dma((2,)),
            dma((9,)),
            dma((9,)),
            dma((9,)),
            dma((9,)),
            dma((2, 9)),
            dma((9,)),
            dma((9,)),
            dma((2, 9)),
            dma((2, HEADS)),
            dma((HEADS,)),
            dma((HEADS,)),
            dma((2, HEADS)),
        ],
        compiler_params=pltpu.CompilerParams(
            collective_id=0, has_side_effects=True, vmem_limit_bytes=60 * 1024 * 1024
        ),
    )(
        query[0], key[0], value[0], text_key[0], text_value[0], grad_out[0], gate, out_weight,
        windows, tile_map, text_count,
    )
    return pl.pallas_call(
        finish,
        out_shape=(
            sds((1, TILE, TILE), BF16),
            sds((1, TILE, TILE), BF16),
            sds((1, TILE, TILE), BF16),
            sds((1, TXT, TILE), BF16),
            sds((1, TXT, TILE), BF16),
            sds((TILE, 768), F32),
        ),
        in_specs=[vmem] * 6,
        out_specs=(anyspec,) * 6,
        scratch_shapes=[v((TILE, 768), F32), dma((6,))],
    )(*out)


def solution(mesh):
    placed = (
        P("dp", "sp", "tp"),
        P("dp", "sp", "tp"),
        P("dp", "sp", "tp"),
        P("dp", None, "tp"),
        P("dp", None, "tp"),
        P("dp", "sp", "tp"),
        P("dp", None),
        P("tp", "dp"),
        P("sp", None),
        P(),
        P("dp"),
    )
    return jax.shard_map(
        per_device,
        mesh=mesh,
        in_specs=placed,
        out_specs=(
            P("dp", "sp", "tp"),
            P("dp", "sp", "tp"),
            P("dp", "sp", "tp"),
            P("dp", None, "tp"),
            P("dp", None, "tp"),
            P("tp", "dp"),
        ),
        check_vma=False,
    )
```

```python
import functools

import jax
import jax.numpy as jnp
from jax import lax
from jax.experimental import pallas as pl
from jax.experimental.pallas import tpu as pltpu
from jax.sharding import PartitionSpec as P

HD = 128
TILE = 384
TXT = 256
HEADS = 3
N_TP = 8
KEYS = 3 * TILE + TXT
R_TXT = TILE
R_NEAR = (TILE + TXT, 2 * TILE + TXT)
QS = 3 * TILE
FAR = 1e30
MESH = pl.DeviceIdType.MESH
F32 = jnp.float32
BF16 = jnp.bfloat16


def dot(a, b, ca, cb):
    return lax.dot_general(a, b, (((ca,), (cb,)), ((), ())), preferred_element_type=F32)


def body(
    q_in, k_in, v_in, tk_in, tv_in, g_in, gate_in, w_in, win, tmap, tcount,
    o_q, o_k, o_v, o_tk, o_tv, o_w,
    qc, kc, vc, graw, sbuf, wbuf, scores, probs, pnear, att, d_out, acc, d_near,
    st_out, st_in, dl_out, dl_in, dl_own, ds_keep,
    gbuf, g_d, g_a, g_y, g_r, g_r1, g_r2, g_hs, g_rh, g_fin,
    tx, t_r1, t_r2, t_hs, t_rh, t_fin,
    gate_ref, q_acc, k_acc, v_acc, rbuf, dbuf, loc, zs, zr, hs_s, hs_r, qs_s, qs_r, ss_s, ss_r, do_s, do_r, ws, wr,
    ds_, dr_, ys, yr, gs, gr, ts, tr, rs_s, rs_r, rf_s, rf_r, rd_s, rd_r, rg_s, rg_r,
):
    factor = HD ** (-0.5)
    dp = lax.axis_index("dp")
    sp = lax.axis_index("sp")
    tp = lax.axis_index("tp")
    core = dp % 2
    ylo = dp // 2
    yhi = sp // 4
    x = sp % 4
    y = yhi * 2 + ylo

    def at_xy(xx, yy, cc):
        return ((yy % 2) * 2 + cc, (yy // 2) * 4 + xx, tp)

    z_dev = (
        (dp, sp, (tp + 1) % N_TP),
        (dp, sp, (tp + N_TP - 1) % N_TP),
    )
    partner = ((ylo * 2 + 1 - core), sp, tp)
    y_next = at_xy(x, (y + 1) % 4, core)
    y_prev = at_xy(x, (y + 3) % 4, core)
    p1 = (dp, yhi * 4 + x + 1 - 2 * (x % 2), tp)
    p2 = (dp, yhi * 4 + (x + 3 + 2 * (x % 2)) % 4, tp)
    across = (dp, (1 - yhi) * 4 + x, tp)
    near_dev = ((dp, jnp.maximum(sp - 1, 0), tp), (dp, jnp.minimum(sp + 1, 7), tp))
    has = (sp > 0, sp < 7)

    def rc(src, dst, s_sem, r_sem, dev):
        return pltpu.make_async_remote_copy(
            src_ref=src, dst_ref=dst, send_sem=s_sem, recv_sem=r_sem,
            device_id=dev, device_id_type=MESH,
        )

    barrier = pltpu.get_barrier_semaphore()
    for dev in (z_dev[0], z_dev[1], partner, y_next, y_prev, p1, p2, across):
        pl.semaphore_signal(barrier, inc=1, device_id=dev, device_id_type=MESH)

    other = (1 - ylo) * 2 + core
    end = (sp == 3) | (sp == 4)
    relay = (sp == 0) | (sp == 7)
    relays = ((other, 0, tp), (other, 7, tp))
    relay_to = ((other, 4, tp), (other, 3, tp))
    relay_half = sp // 7
    flow = jnp.where(sp == 3, 0, 1)
    from_side = 1 - flow

    @pl.when(end)
    def _():
        for dev in (*relays, (dp, jnp.where(sp == 3, 4, 3), tp)):
            pl.semaphore_signal(barrier, inc=1, device_id=dev, device_id_type=MESH)

    @pl.when(relay)
    def _():
        for dev in relay_to:
            pl.semaphore_signal(barrier, inc=1, device_id=dev, device_id_type=MESH)

    gcopy = pltpu.make_async_copy(g_in, graw, loc.at[0])
    gcopy.start()
    gate_copy = pltpu.make_async_copy(
        gate_in.at[:, pl.ds(pl.multiple_of(tp * TILE, 128), TILE)], gate_ref, loc.at[5]
    )
    gate_copy.start()
    wcopy = pltpu.make_async_copy(w_in, wbuf.at[dp], loc.at[1])
    wcopy.start()
    kcopies, qcopies, vcopies = [], [], []
    for h in range(HEADS):
        cols = slice(h * HD, (h + 1) * HD)
        kcopies.append(pltpu.make_async_copy(k_in.at[:, cols], kc.at[h, 0:TILE], loc.at[2]))
        vcopies.append(pltpu.make_async_copy(v_in.at[:, cols], vc.at[h, 0:TILE], loc.at[3]))
        qcopies.append(pltpu.make_async_copy(q_in.at[:, cols], qc.at[h, 0:TILE], loc.at[4]))
        kcopies.append(
            pltpu.make_async_copy(tk_in.at[:, cols], kc.at[h, R_TXT : R_TXT + TXT], loc.at[2])
        )
        vcopies.append(
            pltpu.make_async_copy(tv_in.at[:, cols], vc.at[h, R_TXT : R_TXT + TXT], loc.at[3])
        )
    for copy in kcopies + vcopies + qcopies:
        copy.start()

    for n in range(2):

        @pl.when(jnp.logical_not(has[n]))
        def _():
            rows = slice(R_NEAR[n], R_NEAR[n] + TILE)
            qrows = slice(TILE * (n + 1), TILE * (n + 2))
            for h in range(HEADS):
                kc[h, rows, :] = jnp.zeros((TILE, HD), BF16)
                vc[h, rows, :] = jnp.zeros((TILE, HD), BF16)
                qc[h, qrows, :] = jnp.zeros((TILE, HD), BF16)
            d_near[n] = jnp.zeros((TILE, TILE), BF16)
            st_in[n] = jnp.full((8, TILE), FAR, F32)
            dl_in[n] = jnp.zeros((8, TILE), F32)

    gcopy.wait()
    gate_copy.wait()
    gate_own = gate_ref[...].astype(F32)
    sbuf[tp] = (graw[...].astype(F32) * gate_own).astype(BF16)

    n_extra = jnp.where(end, 3, 0) + jnp.where(relay, 2, 0)
    pl.semaphore_wait(barrier, 8 + n_extra)

    def z_unit(k, u, d):
        step = 1 - 2 * d
        chunk = (tp + N_TP - step * k) % N_TP
        ref = sbuf.at[chunk, pl.ds(u * 192, 192), :]
        return rc(ref, ref, zs.at[d, k // 3], zr.at[d, k, u], z_dev[d])

    def z_wait(k, u, d):
        step = 1 - 2 * d
        chunk = (tp + N_TP - step * (k + 1)) % N_TP
        ref = sbuf.at[chunk, pl.ds(u * 192, 192), :]
        rc(ref, ref, zs.at[d, k // 3], zr.at[d, k, u], z_dev[d]).wait_recv()

    for u in range(2):
        for d in range(2):
            z_unit(0, u, d).start()

    def z_service(k, units=(0, 1)):
        for u in units:
            for d in range(2):
                z_wait(k - 1, u, d)
                if k < 3 or u == d:
                    z_unit(k, u, d).start()

    def drain(ref, sem):
        pltpu.make_async_copy(ref, ref, sem).wait()

    drain(kc.at[:, 0 : TILE + TXT], loc.at[2])
    drain(vc.at[:, 0 : TILE + TXT], loc.at[3])

    def halo(h, n, which, mine):
        src = (kc, vc)[which]
        slot = R_NEAR[1 - n] if mine else R_NEAR[n]
        return rc(
            src.at[h, 0:TILE], src.at[h, pl.ds(slot, TILE)],
            hs_s.at[n], hs_r.at[1 - n if mine else n, h], near_dev[n],
        )

    def q_halo(n, mine):
        slot = TILE * (2 - n) if mine else TILE * (1 + n)
        return rc(
            qc.at[:, pl.ds(0, TILE)], qc.at[:, pl.ds(slot, TILE)],
            qs_s.at[n], qs_r.at[1 - n if mine else n], near_dev[n],
        )

    drain(qc.at[:, 0:TILE], loc.at[4])
    wcopy.wait()
    w_part = rc(wbuf.at[dp], wbuf.at[dp], ws.at[0], wr.at[0], partner)
    w_next = rc(wbuf.at[dp, 0:192], wbuf.at[dp, 0:192], ws.at[1], wr.at[1], y_next)
    w_prev = rc(wbuf.at[dp, 192:384], wbuf.at[dp, 192:384], ws.at[2], wr.at[2], y_prev)
    def side(n):
        return (sp == 4) if n == 0 else (sp == 3)

    plain = tuple(has[n] & jnp.logical_not(side(n)) for n in range(2))

    def piece_src(piece):
        if piece < 6:
            return (kc, vc)[piece % 2].at[piece // 2]
        return qc.at[piece - 6]

    def end_send(piece, half):
        rows = slice(half * 192, half * 192 + 192)
        return rc(
            piece_src(piece).at[rows], rbuf.at[flow, piece],
            rs_s.at[half], rs_r.at[flow, min(piece // 2, 3)], relays[half],
        )

    def forward_piece(piece, f):
        start = (R_NEAR[0] if piece < 6 else TILE) + f * TILE + relay_half * 192
        dst = piece_src(piece).at[pl.ds(pl.multiple_of(start, 16), 192), :]
        return rc(rbuf.at[f, piece], dst, rf_s.at[f], rf_r.at[relay_half, min(piece // 2, 3)], relay_to[f])

    def relay_pieces(pieces):
        @pl.when(relay)
        def _():
            group = min(pieces[0] // 2, 3)
            for f in range(2):
                ref = rbuf.at[f, pieces[0] : pieces[-1] + 1]
                rc(ref, ref, rf_s.at[f], rs_r.at[f, group], relay_to[1 - f]).wait_recv()
                for piece in pieces:
                    forward_piece(piece, f).start()

    def end_wait(group):
        for half in range(2):
            ref = rbuf.at[0, 2 * group : 2 * group + (2 if group < 3 else 3)]
            rc(ref, ref, rf_s.at[0], rf_r.at[half, group], relays[half]).wait_recv()

    @pl.when(end)
    def _():
        for piece in range(9):
            for half in range(2):
                end_send(piece, half).start()

    for n in range(2):

        @pl.when(plain[n])
        def _():
            for h in range(HEADS):
                halo(h, n, 0, True).start()
                halo(h, n, 1, True).start()
            q_halo(n, True).start()

    own_pos = tmap[sp]
    bias = []
    for n in range(2):
        near_pos = tmap[(jnp.maximum(sp - 1, 0), jnp.minimum(sp + 1, 7))[n]]
        reach = jnp.where((win[0] >= 1) & has[n], win[1], -1)
        bias.append(jnp.where(jnp.abs(own_pos - near_pos) <= reach, 0.0, -FAR).astype(F32))
    text_rows = lax.broadcasted_iota(jnp.int32, (TXT, 1), 0)
    text_bias = jnp.where(text_rows < tcount[0], 0.0, -FAR).astype(F32)

    def early(h, carry):
        queries = qc[h, 0:TILE, :]
        own = factor * dot(kc[h, 0:TILE, :], queries, 1, 1)
        scores[h, 0:TILE, :] = own
        text = factor * dot(kc[h, R_TXT : R_TXT + TXT, :], queries, 1, 1) + text_bias
        scores[h, R_TXT : R_TXT + TXT, :] = text
        return carry

    lax.fori_loop(0, HEADS, early, 0)

    def take(chunk):
        cols = pl.ds(pl.multiple_of((chunk % 2) * TILE, 128), TILE)
        return dot(wbuf[chunk // 2, :, cols], sbuf[chunk], 1, 1)

    def forward(h):
        queries = qc[h, 0:TILE, :]
        for n in range(2):

            @pl.when(plain[n])
            def _():
                both = kc.at[0:2, 0:TILE]
                rc(both, both, hs_s.at[n], hs_r.at[n, h], near_dev[n]).wait_recv()

        @pl.when(end)
        def _():
            end_wait(h)

        for n in range(2):
            rows = slice(R_NEAR[n], R_NEAR[n] + TILE)
            scores[h, rows, :] = factor * dot(kc[h, rows, :], queries, 1, 1) + bias[n]
        top = jnp.max(scores[h], axis=0, keepdims=True)
        weights = jnp.exp(scores[h] - top)
        inv = 1.0 / jnp.sum(weights, axis=0, keepdims=True)
        probs[h] = (weights * inv).astype(BF16)
        for n in range(2):
            st_out[n, h : h + 1, :] = jnp.where(bias[n] < 0.0, FAR, top)
            st_out[n, h + 4 : h + 5, :] = inv
        att[h] = dot(vc[h], probs[h], 0, 0).astype(BF16)

    z_service(1, (0,))
    relay_pieces((0, 1))
    z_service(1, (1,))
    forward(0)
    relay_pieces((2, 3))
    w_next.start()
    w_prev.start()
    w_part.start()
    forward(1)
    relay_pieces((4, 5))
    z_service(2)
    forward(2)
    def st_copy(n, mine):
        return rc(
            st_out.at[n], st_in.at[1 - n if mine else n],
            ss_s.at[n], ss_r.at[1 - n if mine else n], near_dev[n],
        )

    for n in range(2):

        @pl.when(has[n])
        def _():
            st_copy(n, True).start()

    def grad_w(chunk):
        full = dot(att[...].reshape(HEADS * HD, TILE), sbuf[chunk], 1, 0)
        cols = pl.ds(pl.multiple_of((chunk % 2) * TILE, 128), TILE)
        gbuf[chunk // 2, :, cols] = full.astype(BF16)

    def grad_w_step(i, carry):
        grad_w((tp + i + 5) % N_TP)
        return carry

    g1 = (x % 2 + x // 2) % 2
    g2 = x // 2

    def summer(src, fin, r1, r2, hs, rh, s_sem, r_sem):
        rows = src.shape[0]
        part, half, quarter = rows // 2, rows // 4, rows // 8

        def at(ref, start, size):
            return ref.at[pl.ds(pl.multiple_of(start, 16), size), :]

        def rd(ref, start, size):
            return ref[pl.ds(pl.multiple_of(start, 16), size), :].astype(F32)

        a1, b1 = g1 * half, part + g2 * half
        a2, b2 = a1 + g2 * quarter, b1 + g1 * quarter
        na1, nb1 = (1 - g1) * half, part + (1 - g2) * half
        na2, nb2 = a1 + (1 - g2) * quarter, b1 + (1 - g1) * quarter
        copies = [
            (rc(at(src, na1, half), r1.at[0:half], s_sem.at[0], r_sem.at[0], p1),
             rc(at(src, nb1, half), r1.at[half : 2 * half], s_sem.at[1], r_sem.at[1], p2)),
            (rc(at(src, na2, quarter), r2.at[0:quarter], s_sem.at[2], r_sem.at[2], p2),
             rc(at(src, nb2, quarter), r2.at[quarter : 2 * quarter], s_sem.at[3], r_sem.at[3], p1)),
            (rc(hs, rh, s_sem.at[4], r_sem.at[4], across),),
            (rc(at(fin, a2, quarter), at(fin, a2, quarter), s_sem.at[5], r_sem.at[5], p2),
             rc(at(fin, b2, quarter), at(fin, b2, quarter), s_sem.at[6], r_sem.at[6], p1)),
            (rc(at(fin, a1, half), at(fin, a1, half), s_sem.at[7], r_sem.at[7], p1),
             rc(at(fin, b1, half), at(fin, b1, half), s_sem.at[8], r_sem.at[8], p2)),
        ]
        arrive = [
            (rc(at(fin, na2, quarter), at(fin, na2, quarter), s_sem.at[5], r_sem.at[5], p2),
             rc(at(fin, nb2, quarter), at(fin, nb2, quarter), s_sem.at[6], r_sem.at[6], p1)),
            (rc(at(fin, na1, half), at(fin, na1, half), s_sem.at[7], r_sem.at[7], p1),
             rc(at(fin, nb1, half), at(fin, nb1, half), s_sem.at[8], r_sem.at[8], p2)),
        ]

        def go(stage):
            if stage == 1:
                for c in copies[0]:
                    c.wait_recv()
                for start, low in ((a1, 0), (b1, half)):
                    at(src, start, half)[...] = (
                        rd(src, start, half) + r1[low : low + half, :].astype(F32)
                    ).astype(BF16)
            elif stage == 2:
                for c in copies[1]:
                    c.wait_recv()
                for start, low in ((a2, 0), (b2, quarter)):
                    hs[low : low + quarter, :] = (
                        rd(src, start, quarter) + r2[low : low + quarter, :].astype(F32)
                    ).astype(BF16)
            elif stage == 3:
                copies[2][0].wait_recv()
                for start, low in ((a2, 0), (b2, quarter)):
                    at(fin, start, quarter)[...] = (
                        hs[low : low + quarter, :].astype(F32)
                        + rh[low : low + quarter, :].astype(F32)
                    ).astype(BF16)
            elif stage >= 4:
                for c in arrive[stage - 4]:
                    c.wait_recv()
            if stage < 5:
                for c in copies[stage]:
                    c.start()
            else:
                for group in copies:
                    for c in group:
                        c.wait_send()

        return go

    g_go = summer(g_r, g_fin, g_r1, g_r2, g_hs, g_rh, gs, gr)
    t_go = summer(tx, t_fin, t_r1, t_r2, t_hs, t_rh, ts, tr)

    turn = 2 * (tp % 2) - 1
    blocks = tuple((tp // 2 + d + 4) % 4 for d in (0, turn, -turn, 2))

    def d_copy(i):
        b = blocks[i]
        return rc(gbuf.at[b], g_d.at[b // 2], ds_.at[i], dr_.at[i], partner)

    def d_send(i):
        @pl.when(blocks[i] % 2 != core)
        def _():
            d_copy(i).start()

    y_sends = [
        rc(g_a.at[0:192], g_y.at[0:192], ys.at[0], yr.at[0], y_next),
        rc(g_a.at[192:384], g_y.at[192:384], ys.at[1], yr.at[1], y_prev),
    ]

    def y_send(i):
        b = blocks[i]

        @pl.when(b % 2 == core)
        def _():
            d_copy(i).wait_recv()
            both = (gbuf[b].astype(F32) + g_d[b // 2].astype(F32)).astype(BF16)

            @pl.when(b != dp)
            def _():
                g_a[...] = both
                for c in y_sends:
                    c.start()

            @pl.when(b == dp)
            def _():
                g_r[...] = both

    def y_take(i):
        @pl.when(blocks[i] == dp)
        def _():
            for c in y_sends:
                c.wait_recv()
            g_r[...] = (g_r[...].astype(F32) + g_y[...].astype(F32)).astype(BF16)
            g_go(0)

    def g_early(stage):
        @pl.when(blocks[3] != dp)
        def _():
            g_go(stage)

    def g_late(stage):
        @pl.when(blocks[3] == dp)
        def _():
            g_go(stage)

    lax.fori_loop(2, 5, grad_w_step, 0)
    d_send(0)
    grad_w((tp + 6) % N_TP)
    grad_w((tp + 2) % N_TP)
    d_send(1)
    w_fwd = []
    for half in range(2):
        rows = slice(half * 192, half * 192 + 192)
        ref = wbuf.at[other, rows]
        rc(ref, ref, ws.at[1 + half], wr.at[1 + half], y_next).wait_recv()
        fwd = rc(ref, ref, ws.at[3 + half], wr.at[3 + half], partner)
        fwd.start()
        w_fwd.append(fwd)
    y_send(0)
    mate = ylo * 2 + 1 - core
    mate_other = (1 - ylo) * 2 + 1 - core
    rc(wbuf.at[mate], wbuf.at[mate], ws.at[0], wr.at[0], partner).wait_recv()
    for half in range(2):
        ref = wbuf.at[mate_other, half * 192 : half * 192 + 192]
        rc(ref, ref, ws.at[3 + half], wr.at[3 + half], partner).wait_recv()

    acc[...] = take(tp)

    def more(h, carry):
        acc[...] += take((tp + h + 1) % N_TP) + take((tp + N_TP - h - 1) % N_TP)
        return carry

    lax.fori_loop(0, 2, more, 0)

    relay_pieces((6, 7, 8))
    z_service(3)
    more(2, 0)
    grad_w((tp + 5) % N_TP)
    grad_w((tp + 3) % N_TP)
    d_send(2)
    y_send(1)

    for n in range(2):

        @pl.when(plain[n])
        def _():
            q_halo(n, False).wait_recv()

        @pl.when(side(n))
        def _():
            end_wait(3)

        @pl.when(has[n])
        def _():
            st_copy(n, False).wait_recv()

        def near_probs(h, carry):
            s = factor * dot(kc[h, 0:TILE, :], qc[h, TILE * (n + 1) : TILE * (n + 2), :], 1, 1)
            p = jnp.exp(s - st_in[n, pl.ds(h, 1), :]) * st_in[n, pl.ds(h + 4, 1), :]
            pnear[n, h] = p.astype(BF16)
            return carry

        lax.fori_loop(0, HEADS, near_probs, 0)

    y_send(2)
    y_take(0)
    y_take(1)
    z_wait(3, 0, 0)
    z_wait(3, 1, 1)
    last = (tp + 4) % N_TP
    total = acc[...] + take(last)
    d_out[...] = total.astype(BF16)
    dl_out[...] = jnp.zeros((8, TILE), F32)
    for h in range(HEADS):
        both = d_out[h * HD : (h + 1) * HD, :].astype(F32) * att[h].astype(F32)
        dl_out[h : h + 1, :] = jnp.sum(both, axis=0, keepdims=True)

    def do_copy(n, mine, which):
        to = 1 - n if mine else n
        src, dst = ((d_out, d_near.at[to]), (dl_out, dl_in.at[to]))[which]
        return rc(src, dst, do_s.at[n, which], do_r.at[to, which], near_dev[n])

    half_rows = HD // 2

    def end_grad(h, half):
        rows = slice(h * HD + half * half_rows, h * HD + (half + 1) * half_rows)
        return rc(
            d_out.at[rows], dbuf.at[flow, h], rd_s.at[half], rd_r.at[flow, h], relays[half]
        )

    def forward_grad(h, f):
        rows = pl.ds(pl.multiple_of(h * HD + relay_half * half_rows, 16), half_rows)
        return rc(
            dbuf.at[f, h], d_near.at[f, rows, :], rg_s.at[f], rg_r.at[relay_half], relay_to[f]
        )

    def relay_grads():
        @pl.when(relay)
        def _():
            for h in range(HEADS):
                for f in range(2):
                    ref = dbuf.at[f, h]
                    rc(ref, ref, rg_s.at[f], rd_r.at[f, h], relay_to[1 - f]).wait_recv()
                    forward_grad(h, f).start()

    def end_grad_wait():
        for half in range(2):
            rc(dbuf.at[0], dbuf.at[0], rg_s.at[0], rg_r.at[half], relays[half]).wait_recv()

    @pl.when(end)
    def _():
        for h in range(HEADS):
            for half in range(2):
                end_grad(h, half).start()

    for n in range(2):

        @pl.when(has[n])
        def _():
            do_copy(n, True, 1).start()

        @pl.when(plain[n])
        def _():
            do_copy(n, True, 0).start()

    grad_w(last)
    d_send(3)
    y_take(2)
    def backward(h):
        lanes = slice(h * HD, (h + 1) * HD)
        grads = d_out[lanes, :]
        delta = dl_out[h : h + 1, :]
        g = dot(vc[h], grads, 1, 0)
        ds = (probs[h].astype(F32) * (g - delta)).astype(BF16)
        ds_keep[h] = ds[0:TILE, :]
        gq = factor * dot(kc[h], ds, 0, 0)
        q_acc[:, lanes] = gq.T.astype(BF16)
        trows = slice(R_TXT, R_TXT + TXT)
        tx[0:TXT, lanes] = (factor * dot(ds[trows, :], qc[h, 0:TILE, :], 1, 0)).astype(BF16)
        tx[TXT : 2 * TXT, lanes] = dot(probs[h, trows, :], grads, 1, 1).astype(BF16)


    backward(0)
    y_send(3)
    backward(1)
    g_early(1)
    backward(2)
    q_out = pltpu.make_async_copy(q_acc, o_q, loc.at[6])
    q_out.start()
    t_go(0)
    relay_grads()
    g_early(2)
    y_take(3)
    t_go(1)
    g_early(3)
    for n in range(2):

        @pl.when(has[n])
        def _():
            do_copy(n, False, 1).wait_recv()

        @pl.when(plain[n])
        def _():
            do_copy(n, False, 0).wait_recv()

    @pl.when(end)
    def _():
        end_grad_wait()

    def own_keys(h):
        lanes = slice(h * HD, (h + 1) * HD)
        hrows = lanes
        gk = dot(ds_keep[h], qc[h, 0:TILE, :], 1, 0)
        gv = dot(probs[h, 0:TILE, :], d_out[hrows, :], 1, 1)
        for n in range(2):
            grads = d_near[n, hrows, :]
            p = pnear[n, h]
            g = dot(vc[h, 0:TILE, :], grads, 1, 0)
            ds = (p.astype(F32) * (g - dl_in[n, h : h + 1, :])).astype(BF16)
            gk += dot(ds, qc[h, TILE * (n + 1) : TILE * (n + 2), :], 1, 0)
            gv += dot(p, grads, 1, 1)
        k_acc[:, lanes] = (factor * gk).astype(BF16)
        v_acc[:, lanes] = gv.astype(BF16)

    g_late(1)
    own_keys(0)
    t_go(2)
    g_late(2)
    own_keys(1)
    g_early(4)
    t_go(3)
    own_keys(2)
    k_out = pltpu.make_async_copy(k_acc, o_k, loc.at[7])
    k_out.start()
    v_out = pltpu.make_async_copy(v_acc, o_v, loc.at[8])
    v_out.start()
    g_late(3)
    t_go(4)
    g_late(4)
    g_early(5)
    t_go(5)
    tk_out = pltpu.make_async_copy(t_fin.at[0:TXT], o_tk, loc.at[9])
    tk_out.start()
    tv_out = pltpu.make_async_copy(t_fin.at[TXT : 2 * TXT], o_tv, loc.at[10])
    tv_out.start()
    g_late(5)
    w_out = pltpu.make_async_copy(g_fin, o_w, loc.at[11])
    w_out.start()
    def drain_sends(ref, sem):
        rc(ref, ref, sem, zr.at[0, 0, 0], partner).wait_send()

    for d in range(2):
        drain_sends(sbuf.at[0:3], zs.at[d, 0])
        drain_sends(sbuf.at[0, 0:192], zs.at[d, 1])
    for c in (w_part, w_next, w_prev, *w_fwd, *y_sends):
        c.wait_send()
    for i in range(4):

        @pl.when(blocks[i] % 2 != core)
        def _():
            d_copy(i).wait_send()

    for c in (q_out, k_out, v_out, tk_out, tv_out, w_out):
        c.wait()
    for n in range(2):

        @pl.when(plain[n])
        def _():
            drain_sends(kc.at[:, 0 : 2 * TILE], hs_s.at[n])
            q_halo(n, True).wait_send()
            do_copy(n, True, 0).wait_send()

        @pl.when(has[n])
        def _():
            st_copy(n, True).wait_send()
            do_copy(n, True, 1).wait_send()

    @pl.when(end)
    def _():
        for half in range(2):
            drain_sends(rbuf.at[0], rs_s.at[half])
            drain_sends(dbuf.at[0], rd_s.at[half])

    @pl.when(relay)
    def _():
        for f in range(2):
            drain_sends(rbuf.at[f], rf_s.at[f])
            drain_sends(dbuf.at[f], rg_s.at[f])


def finish(*refs):
    given, results, held, wide, sems = refs[:6], refs[6:12], refs[12:18], refs[18], refs[19]
    loads = [pltpu.make_async_copy(given[i], held[i], sems.at[0, i]) for i in range(6)]
    for i in (5, 0, 1, 2, 3, 4):
        loads[i].start()
    stores = []
    for i in (5, 0, 1, 2, 3, 4):
        loads[i].wait()
        if i == 5:
            wide[...] = held[i][...].astype(F32)
            stores.append(pltpu.make_async_copy(wide, results[i], sems.at[1, i]))
        else:
            stores.append(pltpu.make_async_copy(held[i], results[i].at[0], sems.at[1, i]))
        stores[-1].start()
    for copy in stores:
        copy.wait()


def per_device(
    query, key, value, text_key, text_value, grad_out, gate, out_weight, windows, tile_map, text_count
):
    anyspec = pl.BlockSpec(memory_space=pl.ANY)
    vmem = pl.BlockSpec(memory_space=pltpu.VMEM)
    smem = pl.BlockSpec(memory_space=pltpu.SMEM)
    sds = jax.ShapeDtypeStruct
    v = pltpu.VMEM
    dma = pltpu.SemaphoreType.DMA
    out = pl.pallas_call(
        body,
        out_shape=(
            sds((TILE, TILE), BF16),
            sds((TILE, TILE), BF16),
            sds((TILE, TILE), BF16),
            sds((TXT, TILE), BF16),
            sds((TXT, TILE), BF16),
            sds((TILE, 768), BF16),
        ),
        in_specs=[anyspec] * 8 + [smem] * 3,
        out_specs=(anyspec,) * 6,
        scratch_shapes=[
            v((HEADS, QS, HD), BF16),
            v((HEADS, KEYS, HD), BF16),
            v((HEADS, KEYS, HD), BF16),
            v((TILE, TILE), BF16),
            v((N_TP, TILE, TILE), BF16),
            v((4, TILE, 768), BF16),
            v((HEADS, KEYS, TILE), F32),
            v((HEADS, KEYS, TILE), BF16),
            v((2, HEADS, TILE, TILE), BF16),
            v((HEADS, HD, TILE), BF16),
            v((TILE, TILE), BF16),
            v((TILE, TILE), F32),
            v((2, TILE, TILE), BF16),
            v((2, 8, TILE), F32),
            v((2, 8, TILE), F32),
            v((8, TILE), F32),
            v((2, 8, TILE), F32),
            v((8, TILE), F32),
            v((HEADS, TILE, TILE), BF16),
            v((4, TILE, 768), BF16),
            v((2, TILE, 768), BF16),
            v((TILE, 768), BF16),
            v((TILE, 768), BF16),
            v((TILE, 768), BF16),
            v((192, 768), BF16),
            v((96, 768), BF16),
            v((96, 768), BF16),
            v((96, 768), BF16),
            v((TILE, 768), BF16),
            v((2 * TXT, TILE), BF16),
            v((TXT, TILE), BF16),
            v((TXT // 2, TILE), BF16),
            v((TXT // 2, TILE), BF16),
            v((TXT // 2, TILE), BF16),
            v((2 * TXT, TILE), BF16),
            v((1, TILE), BF16),
            v((TILE, TILE), BF16),
            v((TILE, TILE), BF16),
            v((TILE, TILE), BF16),
            v((2, 9, 192, HD), BF16),
            v((2, HEADS, HD // 2, TILE), BF16),
            dma((12,)),
            dma((2, 2)),
            dma((2, 4, 2)),
            dma((2,)),
            dma((2, HEADS)),
            dma((2,)),
            dma((2,)),
            dma((2,)),
            dma((2,)),
            dma((2, 2)),
            dma((2, 2)),
            dma((5,)),
            dma((5,)),
            dma((4,)),
            dma((4,)),
            dma((2,)),
            dma((2,)),
            dma((9,)),
            dma((9,)),
            dma((9,)),
            dma((9,)),
            dma((2,)),
            dma((2, 4)),
            dma((2,)),
            dma((2, 4)),
            dma((2,)),
            dma((2, HEADS)),
            dma((2,)),
            dma((2,)),
        ],
        compiler_params=pltpu.CompilerParams(
            collective_id=0, has_side_effects=True, vmem_limit_bytes=60 * 1024 * 1024
        ),
    )(
        query[0], key[0], value[0], text_key[0], text_value[0], grad_out[0], gate, out_weight,
        windows.reshape(2), tile_map.reshape(8), text_count,
    )
    return pl.pallas_call(
        finish,
        out_shape=(
            sds((1, TILE, TILE), BF16),
            sds((1, TILE, TILE), BF16),
            sds((1, TILE, TILE), BF16),
            sds((1, TXT, TILE), BF16),
            sds((1, TXT, TILE), BF16),
            sds((TILE, 768), F32),
        ),
        in_specs=[anyspec] * 6,
        out_specs=(anyspec,) * 6,
        scratch_shapes=[
            v((TILE, TILE), BF16),
            v((TILE, TILE), BF16),
            v((TILE, TILE), BF16),
            v((TXT, TILE), BF16),
            v((TXT, TILE), BF16),
            v((TILE, 768), BF16),
            v((TILE, 768), F32),
            dma((2, 6)),
        ],
    )(*out)


def solution(mesh):
    placed = (
        P("dp", "sp", "tp"),
        P("dp", "sp", "tp"),
        P("dp", "sp", "tp"),
        P("dp", None, "tp"),
        P("dp", None, "tp"),
        P("dp", "sp", "tp"),
        P("dp", None),
        P("tp", "dp"),
        P("sp", None),
        P(),
        P("dp"),
    )
    return jax.shard_map(
        per_device,
        mesh=mesh,
        in_specs=placed,
        out_specs=(
            P("dp", "sp", "tp"),
            P("dp", "sp", "tp"),
            P("dp", "sp", "tp"),
            P("dp", None, "tp"),
            P("dp", None, "tp"),
            P("tp", "dp"),
        ),
        check_vma=False,
    )
```

```python
import functools

import jax
import jax.numpy as jnp
from jax import lax
from jax.experimental import pallas as pl
from jax.experimental.pallas import tpu as pltpu
from jax.sharding import PartitionSpec as P

HD = 128
TILE = 384
TXT = 256
HEADS = 3
N_TP = 8
KEYS = 3 * TILE + TXT
R_TXT = TILE
R_NEAR = (TILE + TXT, 2 * TILE + TXT)
QS = 3 * TILE
FAR = 1e30
MESH = pl.DeviceIdType.MESH
F32 = jnp.float32
BF16 = jnp.bfloat16


def dot(a, b, ca, cb):
    return lax.dot_general(a, b, (((ca,), (cb,)), ((), ())), preferred_element_type=F32)


def body(
    q_in, k_in, v_in, tk_in, tv_in, g_in, gate_in, w_in, win, tmap, tcount,
    o_q, o_k, o_v, o_tk, o_tv, o_w,
    qc, kc, vc, graw, sbuf, wbuf, scores, probs, pnear, att, d_out, acc, d_near,
    st_out, st_in, dl_out, dl_in, dl_own, ds_keep,
    gbuf, g_d, g_a, g_y, g_r, g_r1, g_r2, g_hs, g_rh, g_fin,
    tx, t_r1, t_r2, t_hs, t_rh, t_fin,
    gate_ref, q_acc, k_acc, v_acc, rbuf, dbuf, loc, zs, zr, hs_s, hs_r, qs_s, qs_r, ss_s, ss_r, do_s, do_r, dl_s, ws, wr,
    ds_, dr_, ys, yr, gs, gr, ts, tr, rs_s, rs_r, rf_s, rf_r, rd_s, rd_r, rg_s, rg_r,
):
    factor = HD ** (-0.5)
    dp = lax.axis_index("dp")
    sp = lax.axis_index("sp")
    tp = lax.axis_index("tp")
    core = dp % 2
    ylo = dp // 2
    yhi = sp // 4
    x = sp % 4
    y = yhi * 2 + ylo

    def at_xy(xx, yy, cc):
        return ((yy % 2) * 2 + cc, (yy // 2) * 4 + xx, tp)

    z_dev = (
        (dp, sp, (tp + 1) % N_TP),
        (dp, sp, (tp + N_TP - 1) % N_TP),
    )
    partner = ((ylo * 2 + 1 - core), sp, tp)
    y_next = at_xy(x, (y + 1) % 4, core)
    y_prev = at_xy(x, (y + 3) % 4, core)
    p1 = (dp, yhi * 4 + x + 1 - 2 * (x % 2), tp)
    p2 = (dp, yhi * 4 + (x + 3 + 2 * (x % 2)) % 4, tp)
    across = (dp, (1 - yhi) * 4 + x, tp)
    near_dev = ((dp, jnp.maximum(sp - 1, 0), tp), (dp, jnp.minimum(sp + 1, 7), tp))
    has = (sp > 0, sp < 7)

    def rc(src, dst, s_sem, r_sem, dev):
        return pltpu.make_async_remote_copy(
            src_ref=src, dst_ref=dst, send_sem=s_sem, recv_sem=r_sem,
            device_id=dev, device_id_type=MESH,
        )

    barrier = pltpu.get_barrier_semaphore()
    for dev in (z_dev[0], z_dev[1], partner, y_next, y_prev, p1, p2, across):
        pl.semaphore_signal(barrier, inc=1, device_id=dev, device_id_type=MESH)

    other = (1 - ylo) * 2 + core
    end = (sp == 3) | (sp == 4)
    relay = (sp == 0) | (sp == 7)
    relays = ((other, 0, tp), (other, 7, tp))
    relay_to = ((other, 4, tp), (other, 3, tp))
    relay_half = sp // 7
    flow = jnp.where(sp == 3, 0, 1)
    from_side = 1 - flow

    @pl.when(end)
    def _():
        for dev in (*relays, (dp, jnp.where(sp == 3, 4, 3), tp)):
            pl.semaphore_signal(barrier, inc=1, device_id=dev, device_id_type=MESH)

    @pl.when(relay)
    def _():
        for dev in relay_to:
            pl.semaphore_signal(barrier, inc=1, device_id=dev, device_id_type=MESH)

    gcopy = pltpu.make_async_copy(g_in, graw, loc.at[0])
    gcopy.start()
    gate_copy = pltpu.make_async_copy(
        gate_in.at[:, pl.ds(pl.multiple_of(tp * TILE, 128), TILE)], gate_ref, loc.at[5]
    )
    gate_copy.start()
    wcopy = pltpu.make_async_copy(w_in, wbuf.at[dp], loc.at[1])
    wcopy.start()
    kcopies, qcopies, vcopies = [], [], []
    for h in range(HEADS):
        cols = slice(h * HD, (h + 1) * HD)
        kcopies.append(pltpu.make_async_copy(k_in.at[:, cols], kc.at[h, 0:TILE], loc.at[2]))
        vcopies.append(pltpu.make_async_copy(v_in.at[:, cols], vc.at[h, 0:TILE], loc.at[3]))
        qcopies.append(pltpu.make_async_copy(q_in.at[:, cols], qc.at[h, 0:TILE], loc.at[4]))
        kcopies.append(
            pltpu.make_async_copy(tk_in.at[:, cols], kc.at[h, R_TXT : R_TXT + TXT], loc.at[2])
        )
        vcopies.append(
            pltpu.make_async_copy(tv_in.at[:, cols], vc.at[h, R_TXT : R_TXT + TXT], loc.at[3])
        )
    for copy in kcopies + vcopies + qcopies:
        copy.start()

    for n in range(2):

        @pl.when(jnp.logical_not(has[n]))
        def _():
            rows = slice(R_NEAR[n], R_NEAR[n] + TILE)
            qrows = slice(TILE * (n + 1), TILE * (n + 2))
            for h in range(HEADS):
                kc[h, rows, :] = jnp.zeros((TILE, HD), BF16)
                vc[h, rows, :] = jnp.zeros((TILE, HD), BF16)
                qc[h, qrows, :] = jnp.zeros((TILE, HD), BF16)
            d_near[n] = jnp.zeros((TILE, TILE), BF16)
            st_in[n] = jnp.full((8, TILE), FAR, F32)
            dl_in[n] = jnp.zeros((8, TILE), F32)

    gcopy.wait()
    gate_copy.wait()
    gate_own = gate_ref[...].astype(F32)
    sbuf[tp] = (graw[...].astype(F32) * gate_own).astype(BF16)

    n_extra = jnp.where(end, 3, 0) + jnp.where(relay, 2, 0)
    pl.semaphore_wait(barrier, 8 + n_extra)

    def z_unit(k, u, d):
        step = 1 - 2 * d
        chunk = (tp + N_TP - step * k) % N_TP
        ref = sbuf.at[chunk, pl.ds(u * 192, 192), :]
        return rc(ref, ref, zs.at[d, k // 3], zr.at[d, k, u], z_dev[d])

    def z_wait(k, u, d):
        step = 1 - 2 * d
        chunk = (tp + N_TP - step * (k + 1)) % N_TP
        ref = sbuf.at[chunk, pl.ds(u * 192, 192), :]
        rc(ref, ref, zs.at[d, k // 3], zr.at[d, k, u], z_dev[d]).wait_recv()

    for u in range(2):
        for d in range(2):
            z_unit(0, u, d).start()

    def z_service(k, units=(0, 1)):
        for u in units:
            for d in range(2):
                z_wait(k - 1, u, d)
                if k < 3 or u == d:
                    z_unit(k, u, d).start()

    def drain(ref, sem):
        pltpu.make_async_copy(ref, ref, sem).wait()

    drain(kc.at[:, 0 : TILE + TXT], loc.at[2])
    drain(vc.at[:, 0 : TILE + TXT], loc.at[3])

    def halo(h, n, which, mine):
        src = (kc, vc)[which]
        slot = R_NEAR[1 - n] if mine else R_NEAR[n]
        return rc(
            src.at[h, 0:TILE], src.at[h, pl.ds(slot, TILE)],
            hs_s.at[n], hs_r.at[1 - n if mine else n, h], near_dev[n],
        )

    def q_halo(n, mine):
        slot = TILE * (2 - n) if mine else TILE * (1 + n)
        return rc(
            qc.at[:, pl.ds(0, TILE)], qc.at[:, pl.ds(slot, TILE)],
            qs_s.at[n], qs_r.at[1 - n if mine else n], near_dev[n],
        )

    drain(qc.at[:, 0:TILE], loc.at[4])
    wcopy.wait()
    w_part = rc(wbuf.at[dp], wbuf.at[dp], ws.at[0], wr.at[0], partner)
    w_next = rc(wbuf.at[dp, 0:192], wbuf.at[dp, 0:192], ws.at[1], wr.at[1], y_next)
    w_prev = rc(wbuf.at[dp, 192:384], wbuf.at[dp, 192:384], ws.at[2], wr.at[2], y_prev)
    def side(n):
        return (sp == 4) if n == 0 else (sp == 3)

    plain = tuple(has[n] & jnp.logical_not(side(n)) for n in range(2))

    def piece_src(piece):
        if piece < 6:
            return (kc, vc)[piece % 2].at[piece // 2]
        return qc.at[piece - 6]

    def end_send(piece, half):
        rows = slice(half * 192, half * 192 + 192)
        return rc(
            piece_src(piece).at[rows], rbuf.at[flow, piece],
            rs_s.at[half], rs_r.at[flow, min(piece // 2, 3)], relays[half],
        )

    def forward_piece(piece, f):
        start = (R_NEAR[0] if piece < 6 else TILE) + f * TILE + relay_half * 192
        dst = piece_src(piece).at[pl.ds(pl.multiple_of(start, 16), 192), :]
        return rc(rbuf.at[f, piece], dst, rf_s.at[f], rf_r.at[relay_half, min(piece // 2, 3)], relay_to[f])

    def relay_pieces(pieces):
        @pl.when(relay)
        def _():
            group = min(pieces[0] // 2, 3)
            for f in range(2):
                ref = rbuf.at[f, pieces[0] : pieces[-1] + 1]
                rc(ref, ref, rf_s.at[f], rs_r.at[f, group], relay_to[1 - f]).wait_recv()
                for piece in pieces:
                    forward_piece(piece, f).start()

    def end_wait(group):
        for half in range(2):
            ref = rbuf.at[0, 2 * group : 2 * group + (2 if group < 3 else 3)]
            rc(ref, ref, rf_s.at[0], rf_r.at[half, group], relays[half]).wait_recv()

    @pl.when(end)
    def _():
        for piece in range(9):
            for half in range(2):
                end_send(piece, half).start()

    for n in range(2):

        @pl.when(plain[n])
        def _():
            for h in range(HEADS):
                halo(h, n, 0, True).start()
                halo(h, n, 1, True).start()
            q_halo(n, True).start()

    own_pos = tmap[sp]
    bias = []
    for n in range(2):
        near_pos = tmap[(jnp.maximum(sp - 1, 0), jnp.minimum(sp + 1, 7))[n]]
        reach = jnp.where((win[0] >= 1) & has[n], win[1], -1)
        bias.append(jnp.where(jnp.abs(own_pos - near_pos) <= reach, 0.0, -FAR).astype(F32))
    text_rows = lax.broadcasted_iota(jnp.int32, (TXT, 1), 0)
    text_bias = jnp.where(text_rows < tcount[0], 0.0, -FAR).astype(F32)

    def early(h, carry):
        queries = qc[h, 0:TILE, :]
        own = factor * dot(kc[h, 0:TILE, :], queries, 1, 1)
        scores[h, 0:TILE, :] = own
        text = factor * dot(kc[h, R_TXT : R_TXT + TXT, :], queries, 1, 1) + text_bias
        scores[h, R_TXT : R_TXT + TXT, :] = text
        return carry

    lax.fori_loop(0, HEADS, early, 0)

    def take(chunk):
        cols = pl.ds(pl.multiple_of((chunk % 2) * TILE, 128), TILE)
        return dot(wbuf[chunk // 2, :, cols], sbuf[chunk], 1, 1)

    def forward(h):
        queries = qc[h, 0:TILE, :]
        for n in range(2):

            @pl.when(plain[n])
            def _():
                both = kc.at[0:2, 0:TILE]
                rc(both, both, hs_s.at[n], hs_r.at[n, h], near_dev[n]).wait_recv()

        @pl.when(end)
        def _():
            end_wait(h)

        for n in range(2):
            rows = slice(R_NEAR[n], R_NEAR[n] + TILE)
            scores[h, rows, :] = factor * dot(kc[h, rows, :], queries, 1, 1) + bias[n]
        top = jnp.max(scores[h], axis=0, keepdims=True)
        weights = jnp.exp(scores[h] - top)
        inv = 1.0 / jnp.sum(weights, axis=0, keepdims=True)
        probs[h] = (weights * inv).astype(BF16)
        for n in range(2):
            st_out[n, h : h + 1, :] = jnp.where(bias[n] < 0.0, FAR, top)
            st_out[n, h + 4 : h + 5, :] = inv
        att[h] = dot(vc[h], probs[h], 0, 0).astype(BF16)

    z_service(1, (0,))
    relay_pieces((0, 1))
    z_service(1, (1,))
    forward(0)
    relay_pieces((2, 3))
    w_part.start()

    @pl.when(jnp.logical_not(relay))
    def _():
        w_next.start()
        w_prev.start()

    forward(1)
    relay_pieces((4, 5))

    @pl.when(relay)
    def _():
        w_next.start()
        w_prev.start()

    z_service(2)
    forward(2)
    def st_copy(n, mine):
        return rc(
            st_out.at[n], st_in.at[1 - n if mine else n],
            ss_s.at[n], ss_r.at[1 - n if mine else n], near_dev[n],
        )

    for n in range(2):

        @pl.when(has[n])
        def _():
            st_copy(n, True).start()

    def grad_w(chunk):
        full = dot(att[...].reshape(HEADS * HD, TILE), sbuf[chunk], 1, 0)
        cols = pl.ds(pl.multiple_of((chunk % 2) * TILE, 128), TILE)
        gbuf[chunk // 2, :, cols] = full.astype(BF16)

    def grad_w_step(i, carry):
        grad_w((tp + i + 5) % N_TP)
        return carry

    g1 = (x % 2 + x // 2) % 2
    g2 = x // 2

    def summer(src, fin, r1, r2, hs, rh, s_sem, r_sem, sent):
        rows = src.shape[0]
        part, half, quarter = rows // 2, rows // 4, rows // 8

        def at(ref, start, size):
            return ref.at[pl.ds(pl.multiple_of(start, 16), size), :]

        def rd(ref, start, size):
            return ref[pl.ds(pl.multiple_of(start, 16), size), :].astype(F32)

        a1, b1 = g1 * half, part + g2 * half
        a2, b2 = a1 + g2 * quarter, b1 + g1 * quarter
        na1, nb1 = (1 - g1) * half, part + (1 - g2) * half
        na2, nb2 = a1 + (1 - g2) * quarter, b1 + (1 - g1) * quarter
        copies = [
            (rc(at(src, na1, half), r1.at[0:half], s_sem.at[0], r_sem.at[0], p1),
             rc(at(src, nb1, half), r1.at[half : 2 * half], s_sem.at[0], r_sem.at[1], p2)),
            (rc(at(src, na2, quarter), r2.at[0:quarter], s_sem.at[0], r_sem.at[2], p2),
             rc(at(src, nb2, quarter), r2.at[quarter : 2 * quarter], s_sem.at[0], r_sem.at[3], p1)),
            (rc(hs, rh, s_sem.at[0], r_sem.at[4], across),),
            (rc(at(fin, a2, quarter), at(fin, a2, quarter), s_sem.at[0], r_sem.at[5], p2),
             rc(at(fin, b2, quarter), at(fin, b2, quarter), s_sem.at[0], r_sem.at[6], p1)),
            (rc(at(fin, a1, half), at(fin, a1, half), s_sem.at[0], r_sem.at[7], p1),
             rc(at(fin, b1, half), at(fin, b1, half), s_sem.at[0], r_sem.at[8], p2)),
        ]
        arrive = [
            (rc(at(fin, na2, quarter), at(fin, na2, quarter), s_sem.at[0], r_sem.at[5], p2),
             rc(at(fin, nb2, quarter), at(fin, nb2, quarter), s_sem.at[0], r_sem.at[6], p1)),
            (rc(at(fin, na1, half), at(fin, na1, half), s_sem.at[0], r_sem.at[7], p1),
             rc(at(fin, nb1, half), at(fin, nb1, half), s_sem.at[0], r_sem.at[8], p2)),
        ]

        def go(stage):
            if stage == 1:
                for c in copies[0]:
                    c.wait_recv()
                for start, low in ((a1, 0), (b1, half)):
                    at(src, start, half)[...] = (
                        rd(src, start, half) + r1[low : low + half, :].astype(F32)
                    ).astype(BF16)
            elif stage == 2:
                for c in copies[1]:
                    c.wait_recv()
                for start, low in ((a2, 0), (b2, quarter)):
                    hs[low : low + quarter, :] = (
                        rd(src, start, quarter) + r2[low : low + quarter, :].astype(F32)
                    ).astype(BF16)
            elif stage == 3:
                copies[2][0].wait_recv()
                for start, low in ((a2, 0), (b2, quarter)):
                    at(fin, start, quarter)[...] = (
                        hs[low : low + quarter, :].astype(F32)
                        + rh[low : low + quarter, :].astype(F32)
                    ).astype(BF16)
            elif stage >= 4:
                for c in arrive[stage - 4]:
                    c.wait_recv()
            if stage < 5:
                for c in copies[stage]:
                    c.start()
            else:
                rc(sent, sent, s_sem.at[0], r_sem.at[0], p1).wait_send()

        return go

    g_go = summer(g_r, g_fin, g_r1, g_r2, g_hs, g_rh, gs, gr, gbuf.at[0:2, 0:336])
    t_go = summer(tx, t_fin, t_r1, t_r2, t_hs, t_rh, ts, tr, sbuf.at[0:4, 0:224])

    turn = 2 * (tp % 2) - 1
    blocks = tuple((tp // 2 + d + 4) % 4 for d in (0, turn, -turn, 2))

    def d_copy(i):
        b = blocks[i]
        return rc(gbuf.at[b], g_d.at[b // 2], ds_.at[i], dr_.at[i], partner)

    def d_send(i):
        @pl.when(blocks[i] % 2 != core)
        def _():
            d_copy(i).start()

    y_sends = [
        rc(g_a.at[0:192], g_y.at[0:192], ys.at[0], yr.at[0], y_next),
        rc(g_a.at[192:384], g_y.at[192:384], ys.at[1], yr.at[1], y_prev),
    ]

    def y_send(i):
        b = blocks[i]

        @pl.when(b % 2 == core)
        def _():
            d_copy(i).wait_recv()
            both = (gbuf[b].astype(F32) + g_d[b // 2].astype(F32)).astype(BF16)

            @pl.when(b != dp)
            def _():
                g_a[...] = both
                for c in y_sends:
                    c.start()

            @pl.when(b == dp)
            def _():
                g_r[...] = both

    def y_take(i):
        @pl.when(blocks[i] == dp)
        def _():
            for c in y_sends:
                c.wait_recv()
            g_r[...] = (g_r[...].astype(F32) + g_y[...].astype(F32)).astype(BF16)
            g_go(0)

    def g_early(stage):
        @pl.when((blocks[0] == dp) | (blocks[1] == dp))
        def _():
            g_go(stage)

    def g_late(stage):
        @pl.when((blocks[2] == dp) | (blocks[3] == dp))
        def _():
            g_go(stage)

    lax.fori_loop(2, 5, grad_w_step, 0)
    d_send(0)
    grad_w((tp + 6) % N_TP)
    grad_w((tp + 2) % N_TP)
    d_send(1)
    def near_all():
        for n in range(2):

            @pl.when(plain[n])
            def _():
                q_halo(n, False).wait_recv()

            @pl.when(side(n))
            def _():
                end_wait(3)

            @pl.when(has[n])
            def _():
                st_copy(n, False).wait_recv()

            def near_probs(h, carry):
                s = factor * dot(kc[h, 0:TILE, :], qc[h, TILE * (n + 1) : TILE * (n + 2), :], 1, 1)
                p = jnp.exp(s - st_in[n, pl.ds(h, 1), :]) * st_in[n, pl.ds(h + 4, 1), :]
                pnear[n, h] = p.astype(BF16)
                return carry

            lax.fori_loop(0, HEADS, near_probs, 0)


    y_send(0)
    relay_pieces((6, 7, 8))
    z_service(3)
    w_fwd = []
    for half in range(2):
        rows = slice(half * 192, half * 192 + 192)
        ref = wbuf.at[other, rows]
        rc(ref, ref, ws.at[1 + half], wr.at[1 + half], y_next).wait_recv()
        fwd = rc(ref, ref, ws.at[3 + half], wr.at[3 + half], partner)
        fwd.start()
        w_fwd.append(fwd)
    y_send(1)
    acc[...] = jnp.zeros_like(acc)
    last = (tp + 4) % N_TP

    def take_group(first):
        def one(i, carry):
            @pl.when(first + i != last)
            def _():
                acc[...] += take(first + i)

            return carry

        lax.fori_loop(0, 4, one, 0)

    mate = ylo * 2 + 1 - core
    rc(wbuf.at[mate], wbuf.at[mate], ws.at[0], wr.at[0], partner).wait_recv()
    take_group(ylo * 4)
    grad_w((tp + 5) % N_TP)
    grad_w((tp + 3) % N_TP)
    d_send(2)

    @pl.when(jnp.logical_not(end))
    def _():
        near_all()

    mate_other = (1 - ylo) * 2 + 1 - core
    for half in range(2):
        ref = wbuf.at[mate_other, half * 192 : half * 192 + 192]
        rc(ref, ref, ws.at[3 + half], wr.at[3 + half], partner).wait_recv()

    take_group(4 - ylo * 4)
    @pl.when(end)
    def _():
        near_all()

    y_take(0)
    y_send(2)
    y_take(1)
    z_wait(3, 0, 0)
    z_wait(3, 1, 1)
    total = acc[...] + take(last)
    d_out[...] = total.astype(BF16)
    dl_out[...] = jnp.zeros((8, TILE), F32)
    for h in range(HEADS):
        both = d_out[h * HD : (h + 1) * HD, :].astype(F32) * att[h].astype(F32)
        dl_out[h : h + 1, :] = jnp.sum(both, axis=0, keepdims=True)

    def do_copy(n, mine, h):
        to = 1 - n if mine else n
        rows = slice(h * HD, h * HD + HD)
        return rc(d_out.at[rows], d_near.at[to, rows], do_s.at[n], do_r.at[to, h], near_dev[n])

    def dl_copy(n, mine):
        to = 1 - n if mine else n
        return rc(dl_out, dl_in.at[to], dl_s.at[n], do_r.at[to, 3], near_dev[n])

    half_rows = HD // 2

    def end_grad(h, half):
        rows = slice(h * HD + half * half_rows, h * HD + (half + 1) * half_rows)
        return rc(
            d_out.at[rows], dbuf.at[flow, h], rd_s.at[half], rd_r.at[flow, h], relays[half]
        )

    def forward_grad(h, f):
        rows = pl.ds(pl.multiple_of(h * HD + relay_half * half_rows, 16), half_rows)
        return rc(
            dbuf.at[f, h], d_near.at[f, rows, :], rg_s.at[f], rg_r.at[relay_half, h], relay_to[f]
        )

    def relay_grads(h):
        @pl.when(relay)
        def _():
            for f in range(2):
                ref = dbuf.at[f, h]
                rc(ref, ref, rg_s.at[f], rd_r.at[f, h], relay_to[1 - f]).wait_recv()
                forward_grad(h, f).start()

    def send_grads(h):
        @pl.when(end)
        def _():
            for half in range(2):
                end_grad(h, half).start()

        for n in range(2):

            @pl.when(plain[n])
            def _():
                do_copy(n, True, h).start()

    def wait_grads(h):
        @pl.when(end)
        def _():
            for half in range(2):
                ref = dbuf.at[0, h]
                rc(ref, ref, rg_s.at[0], rg_r.at[half, h], relays[half]).wait_recv()

        for n in range(2):

            @pl.when(plain[n])
            def _():
                do_copy(n, False, h).wait_recv()

    for n in range(2):

        @pl.when(has[n])
        def _():
            dl_copy(n, True).start()

    send_grads(0)
    grad_w(last)
    d_send(3)
    def backward(h):
        lanes = slice(h * HD, (h + 1) * HD)
        grads = d_out[lanes, :]
        delta = dl_out[h : h + 1, :]
        g = dot(vc[h], grads, 1, 0)
        ds = (probs[h].astype(F32) * (g - delta)).astype(BF16)
        ds_keep[h] = ds[0:TILE, :]
        gq = factor * dot(kc[h], ds, 0, 0)
        q_acc[:, lanes] = gq.T.astype(BF16)
        trows = slice(R_TXT, R_TXT + TXT)
        tx[0:TXT, lanes] = (factor * dot(ds[trows, :], qc[h, 0:TILE, :], 1, 0)).astype(BF16)
        tx[TXT : 2 * TXT, lanes] = dot(probs[h, trows, :], grads, 1, 1).astype(BF16)


    backward(0)
    backward(1)
    y_send(3)
    backward(2)
    q_out = pltpu.make_async_copy(q_acc, o_q, loc.at[6])
    q_out.start()
    t_go(0)
    g_early(1)
    y_take(2)
    send_grads(1)
    g_early(2)
    y_take(3)
    send_grads(2)
    relay_grads(0)
    t_go(1)
    relay_grads(1)
    for n in range(2):

        @pl.when(has[n])
        def _():
            dl_copy(n, False).wait_recv()

    def own_keys(h):
        lanes = slice(h * HD, (h + 1) * HD)
        hrows = lanes
        gk = dot(ds_keep[h], qc[h, 0:TILE, :], 1, 0)
        gv = dot(probs[h, 0:TILE, :], d_out[hrows, :], 1, 1)
        for n in range(2):
            grads = d_near[n, hrows, :]
            p = pnear[n, h]
            g = dot(vc[h, 0:TILE, :], grads, 1, 0)
            ds = (p.astype(F32) * (g - dl_in[n, h : h + 1, :])).astype(BF16)
            gk += dot(ds, qc[h, TILE * (n + 1) : TILE * (n + 2), :], 1, 0)
            gv += dot(p, grads, 1, 1)
        k_acc[:, lanes] = (factor * gk).astype(BF16)
        v_acc[:, lanes] = gv.astype(BF16)

    wait_grads(0)
    own_keys(0)
    g_late(1)
    relay_grads(2)
    g_early(3)
    t_go(2)
    wait_grads(1)
    own_keys(1)
    g_late(2)
    g_early(4)
    t_go(3)
    wait_grads(2)
    own_keys(2)
    k_out = pltpu.make_async_copy(k_acc, o_k, loc.at[7])
    k_out.start()
    v_out = pltpu.make_async_copy(v_acc, o_v, loc.at[8])
    v_out.start()
    g_late(3)
    t_go(4)
    g_early(5)
    g_late(4)
    t_go(5)
    tk_out = pltpu.make_async_copy(t_fin.at[0:TXT], o_tk, loc.at[9])
    tk_out.start()
    tv_out = pltpu.make_async_copy(t_fin.at[TXT : 2 * TXT], o_tv, loc.at[10])
    tv_out.start()
    g_late(5)
    w_out = pltpu.make_async_copy(g_fin, o_w, loc.at[11])
    w_out.start()
    def drain_sends(ref, sem):
        rc(ref, ref, sem, zr.at[0, 0, 0], partner).wait_send()

    for d in range(2):
        drain_sends(sbuf.at[0:3], zs.at[d, 0])
        drain_sends(sbuf.at[0, 0:192], zs.at[d, 1])
    for c in (w_part, w_next, w_prev, *w_fwd, *y_sends):
        c.wait_send()
    for i in range(4):

        @pl.when(blocks[i] % 2 != core)
        def _():
            d_copy(i).wait_send()

    for c in (q_out, k_out, v_out, tk_out, tv_out, w_out):
        c.wait()
    for n in range(2):

        @pl.when(plain[n])
        def _():
            drain_sends(kc.at[:, 0 : 2 * TILE], hs_s.at[n])
            q_halo(n, True).wait_send()
            drain_sends(d_out, do_s.at[n])

        @pl.when(has[n])
        def _():
            st_copy(n, True).wait_send()
            dl_copy(n, True).wait_send()

    @pl.when(end)
    def _():
        for half in range(2):
            drain_sends(rbuf.at[0], rs_s.at[half])
            drain_sends(dbuf.at[0], rd_s.at[half])

    @pl.when(relay)
    def _():
        for f in range(2):
            drain_sends(rbuf.at[f], rf_s.at[f])
            drain_sends(dbuf.at[f], rg_s.at[f])


def finish(*refs):
    given, results, held, wide, sems = refs[:6], refs[6:12], refs[12:18], refs[18], refs[19]
    loads = [pltpu.make_async_copy(given[i], held[i], sems.at[0, i]) for i in range(6)]
    for i in (5, 0, 1, 2, 3, 4):
        loads[i].start()
    stores = []
    for i in (5, 0, 1, 2, 3, 4):
        loads[i].wait()
        if i == 5:
            wide[...] = held[i][...].astype(F32)
            stores.append(pltpu.make_async_copy(wide, results[i], sems.at[1, i]))
        else:
            stores.append(pltpu.make_async_copy(held[i], results[i].at[0], sems.at[1, i]))
        stores[-1].start()
    for copy in stores:
        copy.wait()


def per_device(
    query, key, value, text_key, text_value, grad_out, gate, out_weight, windows, tile_map, text_count
):
    anyspec = pl.BlockSpec(memory_space=pl.ANY)
    vmem = pl.BlockSpec(memory_space=pltpu.VMEM)
    smem = pl.BlockSpec(memory_space=pltpu.SMEM)
    sds = jax.ShapeDtypeStruct
    v = pltpu.VMEM
    dma = pltpu.SemaphoreType.DMA
    out = pl.pallas_call(
        body,
        out_shape=(
            sds((TILE, TILE), BF16),
            sds((TILE, TILE), BF16),
            sds((TILE, TILE), BF16),
            sds((TXT, TILE), BF16),
            sds((TXT, TILE), BF16),
            sds((TILE, 768), BF16),
        ),
        in_specs=[anyspec] * 8 + [smem] * 3,
        out_specs=(anyspec,) * 6,
        scratch_shapes=[
            v((HEADS, QS, HD), BF16),
            v((HEADS, KEYS, HD), BF16),
            v((HEADS, KEYS, HD), BF16),
            v((TILE, TILE), BF16),
            v((N_TP, TILE, TILE), BF16),
            v((4, TILE, 768), BF16),
            v((HEADS, KEYS, TILE), F32),
            v((HEADS, KEYS, TILE), BF16),
            v((2, HEADS, TILE, TILE), BF16),
            v((HEADS, HD, TILE), BF16),
            v((TILE, TILE), BF16),
            v((TILE, TILE), F32),
            v((2, TILE, TILE), BF16),
            v((2, 8, TILE), F32),
            v((2, 8, TILE), F32),
            v((8, TILE), F32),
            v((2, 8, TILE), F32),
            v((8, TILE), F32),
            v((HEADS, TILE, TILE), BF16),
            v((4, TILE, 768), BF16),
            v((2, TILE, 768), BF16),
            v((TILE, 768), BF16),
            v((TILE, 768), BF16),
            v((TILE, 768), BF16),
            v((192, 768), BF16),
            v((96, 768), BF16),
            v((96, 768), BF16),
            v((96, 768), BF16),
            v((TILE, 768), BF16),
            v((2 * TXT, TILE), BF16),
            v((TXT, TILE), BF16),
            v((TXT // 2, TILE), BF16),
            v((TXT // 2, TILE), BF16),
            v((TXT // 2, TILE), BF16),
            v((2 * TXT, TILE), BF16),
            v((1, TILE), BF16),
            v((TILE, TILE), BF16),
            v((TILE, TILE), BF16),
            v((TILE, TILE), BF16),
            v((2, 9, 192, HD), BF16),
            v((2, HEADS, HD // 2, TILE), BF16),
            dma((12,)),
            dma((2, 2)),
            dma((2, 4, 2)),
            dma((2,)),
            dma((2, HEADS)),
            dma((2,)),
            dma((2,)),
            dma((2,)),
            dma((2,)),
            dma((2,)),
            dma((2, 4)),
            dma((2,)),
            dma((5,)),
            dma((5,)),
            dma((4,)),
            dma((4,)),
            dma((2,)),
            dma((2,)),
            dma((1,)),
            dma((9,)),
            dma((1,)),
            dma((9,)),
            dma((2,)),
            dma((2, 4)),
            dma((2,)),
            dma((2, 4)),
            dma((2,)),
            dma((2, HEADS)),
            dma((2,)),
            dma((2, HEADS)),
        ],
        compiler_params=pltpu.CompilerParams(
            collective_id=0, has_side_effects=True, vmem_limit_bytes=60 * 1024 * 1024
        ),
    )(
        query[0], key[0], value[0], text_key[0], text_value[0], grad_out[0], gate, out_weight,
        windows.reshape(2), tile_map.reshape(8), text_count,
    )
    return pl.pallas_call(
        finish,
        out_shape=(
            sds((1, TILE, TILE), BF16),
            sds((1, TILE, TILE), BF16),
            sds((1, TILE, TILE), BF16),
            sds((1, TXT, TILE), BF16),
            sds((1, TXT, TILE), BF16),
            sds((TILE, 768), F32),
        ),
        in_specs=[anyspec] * 6,
        out_specs=(anyspec,) * 6,
        scratch_shapes=[
            v((TILE, TILE), BF16),
            v((TILE, TILE), BF16),
            v((TILE, TILE), BF16),
            v((TXT, TILE), BF16),
            v((TXT, TILE), BF16),
            v((TILE, 768), BF16),
            v((TILE, 768), F32),
            dma((2, 6)),
        ],
    )(*out)


def solution(mesh):
    placed = (
        P("dp", "sp", "tp"),
        P("dp", "sp", "tp"),
        P("dp", "sp", "tp"),
        P("dp", None, "tp"),
        P("dp", None, "tp"),
        P("dp", "sp", "tp"),
        P("dp", None),
        P("tp", "dp"),
        P("sp", None),
        P(),
        P("dp"),
    )
    return jax.shard_map(
        per_device,
        mesh=mesh,
        in_specs=placed,
        out_specs=(
            P("dp", "sp", "tp"),
            P("dp", "sp", "tp"),
            P("dp", "sp", "tp"),
            P("dp", None, "tp"),
            P("dp", None, "tp"),
            P("tp", "dp"),
        ),
        check_vma=False,
    )
```

```python
import functools

import jax
import jax.numpy as jnp
from jax import lax
from jax.experimental import pallas as pl
from jax.experimental.pallas import tpu as pltpu
from jax.sharding import PartitionSpec as P

HD = 128
TILE = 384
TXT = 256
HEADS = 3
N_TP = 8
KEYS = 3 * TILE + TXT
R_TXT = TILE
R_NEAR = (TILE + TXT, 2 * TILE + TXT)
QS = 3 * TILE
FAR = 1e30
MESH = pl.DeviceIdType.MESH
F32 = jnp.float32
BF16 = jnp.bfloat16


def dot(a, b, ca, cb):
    return lax.dot_general(a, b, (((ca,), (cb,)), ((), ())), preferred_element_type=F32)


def body(
    q_in, k_in, v_in, tk_in, tv_in, g_in, gate_in, w_in, win, tmap, tcount,
    o_q, o_k, o_v, o_tk, o_tv, o_w,
    qc, kc, vc, graw, sbuf, wbuf, scores, probs, pnear, att, d_out, acc, d_near,
    st_out, st_in, dl_out, dl_in, dl_own, ds_keep,
    gbuf, g_d, g_a, g_y, g_r, g_r1, g_r2, g_hs, g_rh, g_fin,
    tx, t_r1, t_r2, t_hs, t_rh, t_fin,
    gate_ref, q_acc, k_acc, v_acc, rbuf, dbuf, loc, zs, zr, hs_s, hs_r, qs_s, qs_r, ss_s, ss_r, do_s, do_r, dl_s, ws, wr,
    ds_, dr_, ys, yr, gs, gr, ts, tr, rs_s, rs_r, rf_s, rf_r, rd_s, rd_r, rg_s, rg_r,
):
    factor = HD ** (-0.5)
    dp = lax.axis_index("dp")
    sp = lax.axis_index("sp")
    tp = lax.axis_index("tp")
    core = dp % 2
    ylo = dp // 2
    yhi = sp // 4
    x = sp % 4
    y = yhi * 2 + ylo

    def at_xy(xx, yy, cc):
        return ((yy % 2) * 2 + cc, (yy // 2) * 4 + xx, tp)

    z_dev = (
        (dp, sp, (tp + 1) % N_TP),
        (dp, sp, (tp + N_TP - 1) % N_TP),
    )
    partner = ((ylo * 2 + 1 - core), sp, tp)
    y_next = at_xy(x, (y + 1) % 4, core)
    y_prev = at_xy(x, (y + 3) % 4, core)
    p1 = (dp, yhi * 4 + x + 1 - 2 * (x % 2), tp)
    p2 = (dp, yhi * 4 + (x + 3 + 2 * (x % 2)) % 4, tp)
    across = (dp, (1 - yhi) * 4 + x, tp)
    near_dev = ((dp, jnp.maximum(sp - 1, 0), tp), (dp, jnp.minimum(sp + 1, 7), tp))
    has = (sp > 0, sp < 7)

    def rc(src, dst, s_sem, r_sem, dev):
        return pltpu.make_async_remote_copy(
            src_ref=src, dst_ref=dst, send_sem=s_sem, recv_sem=r_sem,
            device_id=dev, device_id_type=MESH,
        )

    barrier = pltpu.get_barrier_semaphore()
    for dev in (z_dev[0], z_dev[1], partner, y_next, y_prev, p1, p2, across):
        pl.semaphore_signal(barrier, inc=1, device_id=dev, device_id_type=MESH)

    other = (1 - ylo) * 2 + core
    end = (sp == 3) | (sp == 4)
    relay = (sp == 0) | (sp == 7)
    relays = ((other, 0, tp), (other, 7, tp))
    relay_to = ((other, 4, tp), (other, 3, tp))
    relay_half = sp // 7
    flow = jnp.where(sp == 3, 0, 1)
    from_side = 1 - flow

    @pl.when(end)
    def _():
        for dev in (*relays, (dp, jnp.where(sp == 3, 4, 3), tp)):
            pl.semaphore_signal(barrier, inc=1, device_id=dev, device_id_type=MESH)

    @pl.when(relay)
    def _():
        for dev in relay_to:
            pl.semaphore_signal(barrier, inc=1, device_id=dev, device_id_type=MESH)

    gcopy = pltpu.make_async_copy(g_in, graw, loc.at[0])
    gcopy.start()
    gate_copy = pltpu.make_async_copy(
        gate_in.at[:, pl.ds(pl.multiple_of(tp * TILE, 128), TILE)], gate_ref, loc.at[5]
    )
    gate_copy.start()
    wcopy = pltpu.make_async_copy(w_in, wbuf.at[dp], loc.at[1])
    wcopy.start()
    kcopies, qcopies, vcopies = [], [], []
    for h in range(HEADS):
        cols = slice(h * HD, (h + 1) * HD)
        kcopies.append(pltpu.make_async_copy(k_in.at[:, cols], kc.at[h, 0:TILE], loc.at[2]))
        vcopies.append(pltpu.make_async_copy(v_in.at[:, cols], vc.at[h, 0:TILE], loc.at[3]))
        qcopies.append(pltpu.make_async_copy(q_in.at[:, cols], qc.at[h, 0:TILE], loc.at[4]))
        kcopies.append(
            pltpu.make_async_copy(tk_in.at[:, cols], kc.at[h, R_TXT : R_TXT + TXT], loc.at[2])
        )
        vcopies.append(
            pltpu.make_async_copy(tv_in.at[:, cols], vc.at[h, R_TXT : R_TXT + TXT], loc.at[3])
        )
    for copy in kcopies + vcopies + qcopies:
        copy.start()

    for n in range(2):

        @pl.when(jnp.logical_not(has[n]))
        def _():
            rows = slice(R_NEAR[n], R_NEAR[n] + TILE)
            qrows = slice(TILE * (n + 1), TILE * (n + 2))
            for h in range(HEADS):
                kc[h, rows, :] = jnp.zeros((TILE, HD), BF16)
                vc[h, rows, :] = jnp.zeros((TILE, HD), BF16)
                qc[h, qrows, :] = jnp.zeros((TILE, HD), BF16)
            d_near[n] = jnp.zeros((TILE, TILE), BF16)
            st_in[n] = jnp.full((8, TILE), FAR, F32)
            dl_in[n] = jnp.zeros((8, TILE), F32)

    gcopy.wait()
    gate_copy.wait()
    gate_own = gate_ref[...].astype(F32)
    sbuf[tp] = (graw[...].astype(F32) * gate_own).astype(BF16)

    n_extra = jnp.where(end, 3, 0) + jnp.where(relay, 2, 0)
    pl.semaphore_wait(barrier, 8 + n_extra)

    def z_unit(k, u, d):
        step = 1 - 2 * d
        chunk = (tp + N_TP - step * k) % N_TP
        ref = sbuf.at[chunk, pl.ds(u * 192, 192), :]
        return rc(ref, ref, zs.at[d, k // 3], zr.at[d, k, u], z_dev[d])

    def z_wait(k, u, d):
        step = 1 - 2 * d
        chunk = (tp + N_TP - step * (k + 1)) % N_TP
        ref = sbuf.at[chunk, pl.ds(u * 192, 192), :]
        rc(ref, ref, zs.at[d, k // 3], zr.at[d, k, u], z_dev[d]).wait_recv()

    for u in range(2):
        for d in range(2):
            z_unit(0, u, d).start()

    def z_service(k, units=(0, 1)):
        for u in units:
            for d in range(2):
                z_wait(k - 1, u, d)
                if k < 3 or u == d:
                    z_unit(k, u, d).start()

    def drain(ref, sem):
        pltpu.make_async_copy(ref, ref, sem).wait()

    drain(kc.at[:, 0 : TILE + TXT], loc.at[2])
    drain(vc.at[:, 0 : TILE + TXT], loc.at[3])

    def halo(h, n, which, mine):
        src = (kc, vc)[which]
        slot = R_NEAR[1 - n] if mine else R_NEAR[n]
        return rc(
            src.at[h, 0:TILE], src.at[h, pl.ds(slot, TILE)],
            hs_s.at[n], hs_r.at[1 - n if mine else n, h], near_dev[n],
        )

    def q_halo(n, mine):
        slot = TILE * (2 - n) if mine else TILE * (1 + n)
        return rc(
            qc.at[:, pl.ds(0, TILE)], qc.at[:, pl.ds(slot, TILE)],
            qs_s.at[n], qs_r.at[1 - n if mine else n], near_dev[n],
        )

    drain(qc.at[:, 0:TILE], loc.at[4])
    wcopy.wait()
    w_part = rc(wbuf.at[dp], wbuf.at[dp], ws.at[0], wr.at[0], partner)
    w_next = rc(wbuf.at[dp, 0:192], wbuf.at[dp, 0:192], ws.at[1], wr.at[1], y_next)
    w_prev = rc(wbuf.at[dp, 192:384], wbuf.at[dp, 192:384], ws.at[2], wr.at[2], y_prev)
    def side(n):
        return (sp == 4) if n == 0 else (sp == 3)

    plain = tuple(has[n] & jnp.logical_not(side(n)) for n in range(2))

    def piece_src(piece):
        if piece < 6:
            return (kc, vc)[piece % 2].at[piece // 2]
        return qc.at[piece - 6]

    def end_send(piece, half):
        rows = slice(half * 192, half * 192 + 192)
        return rc(
            piece_src(piece).at[rows], rbuf.at[flow, piece],
            rs_s.at[half], rs_r.at[flow, min(piece // 2, 3)], relays[half],
        )

    def forward_piece(piece, f):
        start = (R_NEAR[0] if piece < 6 else TILE) + f * TILE + relay_half * 192
        dst = piece_src(piece).at[pl.ds(pl.multiple_of(start, 16), 192), :]
        return rc(rbuf.at[f, piece], dst, rf_s.at[f], rf_r.at[relay_half, min(piece // 2, 3)], relay_to[f])

    def relay_pieces(pieces):
        @pl.when(relay)
        def _():
            group = min(pieces[0] // 2, 3)
            for f in range(2):
                ref = rbuf.at[f, pieces[0] : pieces[-1] + 1]
                rc(ref, ref, rf_s.at[f], rs_r.at[f, group], relay_to[1 - f]).wait_recv()
                for piece in pieces:
                    forward_piece(piece, f).start()

    def end_wait(group):
        for half in range(2):
            ref = rbuf.at[0, 2 * group : 2 * group + (2 if group < 3 else 3)]
            rc(ref, ref, rf_s.at[0], rf_r.at[half, group], relays[half]).wait_recv()

    @pl.when(end)
    def _():
        for piece in range(9):
            for half in range(2):
                end_send(piece, half).start()

    for n in range(2):

        @pl.when(plain[n])
        def _():
            for h in range(HEADS):
                halo(h, n, 0, True).start()
                halo(h, n, 1, True).start()
            q_halo(n, True).start()

    own_pos = tmap[sp]
    bias = []
    for n in range(2):
        near_pos = tmap[(jnp.maximum(sp - 1, 0), jnp.minimum(sp + 1, 7))[n]]
        reach = jnp.where((win[0] >= 1) & has[n], win[1], -1)
        bias.append(jnp.where(jnp.abs(own_pos - near_pos) <= reach, 0.0, -FAR).astype(F32))
    text_rows = lax.broadcasted_iota(jnp.int32, (TXT, 1), 0)
    text_bias = jnp.where(text_rows < tcount[0], 0.0, -FAR).astype(F32)

    def early(h, carry):
        queries = qc[h, 0:TILE, :]
        own = factor * dot(kc[h, 0:TILE, :], queries, 1, 1)
        scores[h, 0:TILE, :] = own
        text = factor * dot(kc[h, R_TXT : R_TXT + TXT, :], queries, 1, 1) + text_bias
        scores[h, R_TXT : R_TXT + TXT, :] = text
        return carry

    lax.fori_loop(0, HEADS, early, 0)

    def take(chunk):
        cols = pl.ds(pl.multiple_of((chunk % 2) * TILE, 128), TILE)
        return dot(wbuf[chunk // 2, :, cols], sbuf[chunk], 1, 1)

    def forward(h):
        queries = qc[h, 0:TILE, :]
        for n in range(2):

            @pl.when(plain[n])
            def _():
                both = kc.at[0:2, 0:TILE]
                rc(both, both, hs_s.at[n], hs_r.at[n, h], near_dev[n]).wait_recv()

        @pl.when(end)
        def _():
            end_wait(h)

        for n in range(2):
            rows = slice(R_NEAR[n], R_NEAR[n] + TILE)
            scores[h, rows, :] = factor * dot(kc[h, rows, :], queries, 1, 1) + bias[n]
        top = jnp.max(scores[h], axis=0, keepdims=True)
        weights = jnp.exp(scores[h] - top)
        inv = 1.0 / jnp.sum(weights, axis=0, keepdims=True)
        probs[h] = (weights * inv).astype(BF16)
        for n in range(2):
            st_out[n, h : h + 1, :] = jnp.where(bias[n] < 0.0, FAR, top)
            st_out[n, h + 4 : h + 5, :] = inv
        att[h] = dot(vc[h], probs[h], 0, 0).astype(BF16)

    z_service(1, (0,))
    relay_pieces((0, 1))
    z_service(1, (1,))
    forward(0)
    relay_pieces((2, 3))
    w_part.start()

    @pl.when(jnp.logical_not(relay))
    def _():
        w_next.start()
        w_prev.start()

    forward(1)
    relay_pieces((4, 5))

    @pl.when(relay)
    def _():
        w_next.start()
        w_prev.start()

    z_service(2)
    forward(2)
    def st_copy(n, mine):
        return rc(
            st_out.at[n], st_in.at[1 - n if mine else n],
            ss_s.at[n], ss_r.at[1 - n if mine else n], near_dev[n],
        )

    for n in range(2):

        @pl.when(has[n])
        def _():
            st_copy(n, True).start()

    def grad_w(chunk):
        full = dot(att[...].reshape(HEADS * HD, TILE), sbuf[chunk], 1, 0)
        cols = pl.ds(pl.multiple_of((chunk % 2) * TILE, 128), TILE)
        gbuf[chunk // 2, :, cols] = full.astype(BF16)

    def grad_w_step(i, carry):
        grad_w((tp + i + 5) % N_TP)
        return carry

    g1 = (x % 2 + x // 2) % 2
    g2 = x // 2

    def summer(src, fin, r1, r2, hs, rh, s_sem, r_sem, sent):
        rows = src.shape[0]
        part, half, q = rows // 2, rows // 4, rows // 8

        def at(ref, start):
            return ref.at[pl.ds(pl.multiple_of(start, 16), q), :]

        def rd(ref, start):
            return ref[pl.ds(pl.multiple_of(start, 16), q), :].astype(F32)

        def low(ref, i):
            return ref[i * q : i * q + q, :].astype(F32)

        def send(from_ref, start, to_ref, sem, dev):
            return rc(at(from_ref, start), to_ref, s_sem.at[0], r_sem.at[sem], dev)

        def same(start, sem, dev):
            return send(fin, start, at(fin, start), sem, dev)

        ka, kb = g1 * half + g2 * q, part + g2 * half + g1 * q
        sa, sb = g1 * half + (1 - g2) * q, part + g2 * half + (1 - g1) * q
        fa, fb = (1 - g1) * half + (1 - g2) * q, part + (1 - g2) * half + (1 - g1) * q
        la, lb = (1 - g1) * half + g2 * q, part + (1 - g2) * half + g1 * q
        first = (
            send(src, fa, r1.at[0:q], 0, p1),
            send(src, fb, r1.at[q : 2 * q], 1, p2),
            send(src, la, r1.at[2 * q : 3 * q], 2, p1),
            send(src, lb, r1.at[3 * q : 4 * q], 3, p2),
        )
        second = (
            send(src, sa, r2.at[0:q], 4, p2),
            send(src, sb, r2.at[q : 2 * q], 5, p1),
        )
        swap = rc(hs, rh, s_sem.at[0], r_sem.at[6], across)
        spread = (same(ka, 7, p2), same(kb, 8, p1), same(ka, 9, p1), same(kb, 10, p2))
        onward = (same(sa, 11, p1), same(sb, 12, p2))
        near = (same(sa, 7, p2), same(sb, 8, p1))
        far = (same(la, 9, p1), same(lb, 10, p2), same(fa, 11, p1), same(fb, 12, p2))

        def go(stage):
            if stage == 0:
                for c in first:
                    c.start()
            elif stage == 1:
                for i, start in ((0, sa), (1, sb)):
                    first[i].wait_recv()
                    at(src, start)[...] = (rd(src, start) + low(r1, i)).astype(BF16)
                    second[i].start()
            elif stage == 2:
                for i, start in ((0, ka), (1, kb)):
                    first[2 + i].wait_recv()
                    second[i].wait_recv()
                    total = rd(src, start) + low(r1, 2 + i) + low(r2, i)
                    hs[i * q : i * q + q, :] = total.astype(BF16)
                swap.start()
            elif stage == 3:
                swap.wait_recv()
                for i, start in ((0, ka), (1, kb)):
                    at(fin, start)[...] = (low(hs, i) + low(rh, i)).astype(BF16)
                for c in spread:
                    c.start()
            elif stage == 4:
                for i in range(2):
                    near[i].wait_recv()
                    onward[i].start()
            else:
                for c in far:
                    c.wait_recv()
                rc(sent, sent, s_sem.at[0], r_sem.at[0], p1).wait_send()

        return go

    g_go = summer(g_r, g_fin, g_r1, g_r2, g_hs, g_rh, gs, gr, gbuf.at[0:2, 0:336])
    t_go = summer(tx, t_fin, t_r1, t_r2, t_hs, t_rh, ts, tr, sbuf.at[0:4, 0:224])

    turn = 2 * (tp % 2) - 1
    blocks = tuple((tp // 2 + d + 4) % 4 for d in (0, turn, -turn, 2))

    def d_copy(i):
        b = blocks[i]
        return rc(gbuf.at[b], g_d.at[b // 2], ds_.at[i], dr_.at[i], partner)

    def d_send(i):
        @pl.when(blocks[i] % 2 != core)
        def _():
            d_copy(i).start()

    y_sends = [
        rc(g_a.at[0:192], g_y.at[0:192], ys.at[0], yr.at[0], y_next),
        rc(g_a.at[192:384], g_y.at[192:384], ys.at[1], yr.at[1], y_prev),
    ]

    def y_send(i):
        b = blocks[i]

        @pl.when(b % 2 == core)
        def _():
            d_copy(i).wait_recv()
            both = (gbuf[b].astype(F32) + g_d[b // 2].astype(F32)).astype(BF16)

            @pl.when(b != dp)
            def _():
                g_a[...] = both
                for c in y_sends:
                    c.start()

            @pl.when(b == dp)
            def _():
                g_r[...] = both

    def y_take(i):
        @pl.when(blocks[i] == dp)
        def _():
            for c in y_sends:
                c.wait_recv()
            g_r[...] = (g_r[...].astype(F32) + g_y[...].astype(F32)).astype(BF16)
            g_go(0)

    def g_early(stage):
        @pl.when((blocks[0] == dp) | (blocks[1] == dp))
        def _():
            g_go(stage)

    def g_late(stage):
        @pl.when((blocks[2] == dp) | (blocks[3] == dp))
        def _():
            g_go(stage)

    lax.fori_loop(2, 5, grad_w_step, 0)
    d_send(0)
    grad_w((tp + 6) % N_TP)
    grad_w((tp + 2) % N_TP)
    d_send(1)
    def near_all():
        for n in range(2):

            @pl.when(plain[n])
            def _():
                q_halo(n, False).wait_recv()

            @pl.when(side(n))
            def _():
                end_wait(3)

            @pl.when(has[n])
            def _():
                st_copy(n, False).wait_recv()

            def near_probs(h, carry):
                s = factor * dot(kc[h, 0:TILE, :], qc[h, TILE * (n + 1) : TILE * (n + 2), :], 1, 1)
                p = jnp.exp(s - st_in[n, pl.ds(h, 1), :]) * st_in[n, pl.ds(h + 4, 1), :]
                pnear[n, h] = p.astype(BF16)
                return carry

            lax.fori_loop(0, HEADS, near_probs, 0)


    relay_pieces((6, 7, 8))
    y_send(0)
    acc[...] = jnp.zeros_like(acc)
    last = (tp + 4) % N_TP

    def take_group(first, least, most):
        def one(i, carry):
            away = (first + i + N_TP - tp) % N_TP
            away = jnp.minimum(away, N_TP - away)

            @pl.when((away >= least) & (away <= most))
            def _():
                acc[...] += take(first + i)

            return carry

        lax.fori_loop(0, 4, one, 0)

    mate = ylo * 2 + 1 - core
    rc(wbuf.at[mate], wbuf.at[mate], ws.at[0], wr.at[0], partner).wait_recv()
    take_group(ylo * 4, 0, 2)
    z_service(3)
    w_fwd = []
    for half in range(2):
        rows = slice(half * 192, half * 192 + 192)
        ref = wbuf.at[other, rows]
        rc(ref, ref, ws.at[1 + half], wr.at[1 + half], y_next).wait_recv()
        fwd = rc(ref, ref, ws.at[3 + half], wr.at[3 + half], partner)
        fwd.start()
        w_fwd.append(fwd)
    y_send(1)
    take_group(ylo * 4, 3, 3)
    grad_w((tp + 5) % N_TP)
    grad_w((tp + 3) % N_TP)
    d_send(2)

    @pl.when(jnp.logical_not(end))
    def _():
        near_all()

    mate_other = (1 - ylo) * 2 + 1 - core
    for half in range(2):
        ref = wbuf.at[mate_other, half * 192 : half * 192 + 192]
        rc(ref, ref, ws.at[3 + half], wr.at[3 + half], partner).wait_recv()

    take_group(4 - ylo * 4, 0, 3)
    @pl.when(end)
    def _():
        near_all()

    y_take(0)
    y_send(2)
    y_take(1)
    z_wait(3, 0, 0)
    z_wait(3, 1, 1)
    total = acc[...] + take(last)
    d_out[...] = total.astype(BF16)
    dl_out[...] = jnp.zeros((8, TILE), F32)
    for h in range(HEADS):
        both = d_out[h * HD : (h + 1) * HD, :].astype(F32) * att[h].astype(F32)
        dl_out[h : h + 1, :] = jnp.sum(both, axis=0, keepdims=True)

    def do_copy(n, mine, h):
        to = 1 - n if mine else n
        rows = slice(h * HD, h * HD + HD)
        return rc(d_out.at[rows], d_near.at[to, rows], do_s.at[n], do_r.at[to, h], near_dev[n])

    def dl_copy(n, mine):
        to = 1 - n if mine else n
        return rc(dl_out, dl_in.at[to], dl_s.at[n], do_r.at[to, 3], near_dev[n])

    half_rows = HD // 2

    def end_grad(h, half):
        rows = slice(h * HD + half * half_rows, h * HD + (half + 1) * half_rows)
        return rc(
            d_out.at[rows], dbuf.at[flow, h], rd_s.at[half], rd_r.at[flow, h], relays[half]
        )

    def forward_grad(h, f):
        rows = pl.ds(pl.multiple_of(h * HD + relay_half * half_rows, 16), half_rows)
        return rc(
            dbuf.at[f, h], d_near.at[f, rows, :], rg_s.at[f], rg_r.at[relay_half, h], relay_to[f]
        )

    def relay_grads(h):
        @pl.when(relay)
        def _():
            for f in range(2):
                ref = dbuf.at[f, h]
                rc(ref, ref, rg_s.at[f], rd_r.at[f, h], relay_to[1 - f]).wait_recv()
                forward_grad(h, f).start()

    def send_grads(h):
        @pl.when(end)
        def _():
            for half in range(2):
                end_grad(h, half).start()

        for n in range(2):

            @pl.when(plain[n])
            def _():
                do_copy(n, True, h).start()

    def wait_grads(h):
        @pl.when(end)
        def _():
            for half in range(2):
                ref = dbuf.at[0, h]
                rc(ref, ref, rg_s.at[0], rg_r.at[half, h], relays[half]).wait_recv()

        for n in range(2):

            @pl.when(plain[n])
            def _():
                do_copy(n, False, h).wait_recv()

    for n in range(2):

        @pl.when(has[n])
        def _():
            dl_copy(n, True).start()

    send_grads(0)
    grad_w(last)
    d_send(3)
    def backward(h):
        lanes = slice(h * HD, (h + 1) * HD)
        grads = d_out[lanes, :]
        delta = dl_out[h : h + 1, :]
        g = dot(vc[h], grads, 1, 0)
        ds = (probs[h].astype(F32) * (g - delta)).astype(BF16)
        ds_keep[h] = ds[0:TILE, :]
        gq = factor * dot(kc[h], ds, 0, 0)
        q_acc[:, lanes] = gq.T.astype(BF16)
        trows = slice(R_TXT, R_TXT + TXT)
        tx[0:TXT, lanes] = (factor * dot(ds[trows, :], qc[h, 0:TILE, :], 1, 0)).astype(BF16)
        tx[TXT : 2 * TXT, lanes] = dot(probs[h, trows, :], grads, 1, 1).astype(BF16)


    backward(0)
    backward(1)
    y_send(3)
    backward(2)
    q_out = pltpu.make_async_copy(q_acc, o_q, loc.at[6])
    q_out.start()
    t_go(0)
    g_early(1)
    y_take(2)
    send_grads(1)
    relay_grads(0)
    g_early(2)
    y_take(3)
    send_grads(2)
    relay_grads(1)
    t_go(1)
    relay_grads(2)
    for n in range(2):

        @pl.when(has[n])
        def _():
            dl_copy(n, False).wait_recv()

    def own_keys(h):
        lanes = slice(h * HD, (h + 1) * HD)
        hrows = lanes
        gk = dot(ds_keep[h], qc[h, 0:TILE, :], 1, 0)
        gv = dot(probs[h, 0:TILE, :], d_out[hrows, :], 1, 1)
        for n in range(2):
            grads = d_near[n, hrows, :]
            p = pnear[n, h]
            g = dot(vc[h, 0:TILE, :], grads, 1, 0)
            ds = (p.astype(F32) * (g - dl_in[n, h : h + 1, :])).astype(BF16)
            gk += dot(ds, qc[h, TILE * (n + 1) : TILE * (n + 2), :], 1, 0)
            gv += dot(p, grads, 1, 1)
        k_acc[:, lanes] = (factor * gk).astype(BF16)
        v_acc[:, lanes] = gv.astype(BF16)

    g_late(1)
    g_early(3)
    t_go(2)
    wait_grads(0)
    own_keys(0)
    g_late(2)
    g_early(4)
    t_go(3)
    wait_grads(1)
    own_keys(1)
    g_late(3)
    wait_grads(2)
    own_keys(2)
    k_out = pltpu.make_async_copy(k_acc, o_k, loc.at[7])
    k_out.start()
    v_out = pltpu.make_async_copy(v_acc, o_v, loc.at[8])
    v_out.start()
    t_go(4)
    g_early(5)
    g_late(4)
    t_go(5)
    tk_out = pltpu.make_async_copy(t_fin.at[0:TXT], o_tk, loc.at[9])
    tk_out.start()
    tv_out = pltpu.make_async_copy(t_fin.at[TXT : 2 * TXT], o_tv, loc.at[10])
    tv_out.start()
    g_late(5)
    w_out = pltpu.make_async_copy(g_fin, o_w, loc.at[11])
    w_out.start()
    def drain_sends(ref, sem):
        rc(ref, ref, sem, zr.at[0, 0, 0], partner).wait_send()

    for d in range(2):
        drain_sends(sbuf.at[0:3], zs.at[d, 0])
        drain_sends(sbuf.at[0, 0:192], zs.at[d, 1])
    for c in (w_part, w_next, w_prev, *w_fwd, *y_sends):
        c.wait_send()
    for i in range(4):

        @pl.when(blocks[i] % 2 != core)
        def _():
            d_copy(i).wait_send()

    for c in (q_out, k_out, v_out, tk_out, tv_out, w_out):
        c.wait()
    for n in range(2):

        @pl.when(plain[n])
        def _():
            drain_sends(kc.at[:, 0 : 2 * TILE], hs_s.at[n])
            q_halo(n, True).wait_send()
            drain_sends(d_out, do_s.at[n])

        @pl.when(has[n])
        def _():
            st_copy(n, True).wait_send()
            dl_copy(n, True).wait_send()

    @pl.when(end)
    def _():
        for half in range(2):
            drain_sends(rbuf.at[0], rs_s.at[half])
            drain_sends(dbuf.at[0], rd_s.at[half])

    @pl.when(relay)
    def _():
        for f in range(2):
            drain_sends(rbuf.at[f], rf_s.at[f])
            drain_sends(dbuf.at[f], rg_s.at[f])


def finish(*refs):
    given, results, held, wide, sems = refs[:6], refs[6:12], refs[12:18], refs[18], refs[19]
    loads = [pltpu.make_async_copy(given[i], held[i], sems.at[0, i]) for i in range(6)]
    for i in (5, 0, 1, 2, 3, 4):
        loads[i].start()
    stores = []
    for i in (5, 0, 1, 2, 3, 4):
        loads[i].wait()
        if i == 5:
            wide[...] = held[i][...].astype(F32)
            stores.append(pltpu.make_async_copy(wide, results[i], sems.at[1, i]))
        else:
            stores.append(pltpu.make_async_copy(held[i], results[i].at[0], sems.at[1, i]))
        stores[-1].start()
    for copy in stores:
        copy.wait()


def per_device(
    query, key, value, text_key, text_value, grad_out, gate, out_weight, windows, tile_map, text_count
):
    anyspec = pl.BlockSpec(memory_space=pl.ANY)
    vmem = pl.BlockSpec(memory_space=pltpu.VMEM)
    smem = pl.BlockSpec(memory_space=pltpu.SMEM)
    sds = jax.ShapeDtypeStruct
    v = pltpu.VMEM
    dma = pltpu.SemaphoreType.DMA
    out = pl.pallas_call(
        body,
        out_shape=(
            sds((TILE, TILE), BF16),
            sds((TILE, TILE), BF16),
            sds((TILE, TILE), BF16),
            sds((TXT, TILE), BF16),
            sds((TXT, TILE), BF16),
            sds((TILE, 768), BF16),
        ),
        in_specs=[anyspec] * 8 + [smem] * 3,
        out_specs=(anyspec,) * 6,
        scratch_shapes=[
            v((HEADS, QS, HD), BF16),
            v((HEADS, KEYS, HD), BF16),
            v((HEADS, KEYS, HD), BF16),
            v((TILE, TILE), BF16),
            v((N_TP, TILE, TILE), BF16),
            v((4, TILE, 768), BF16),
            v((HEADS, KEYS, TILE), F32),
            v((HEADS, KEYS, TILE), BF16),
            v((2, HEADS, TILE, TILE), BF16),
            v((HEADS, HD, TILE), BF16),
            v((TILE, TILE), BF16),
            v((TILE, TILE), F32),
            v((2, TILE, TILE), BF16),
            v((2, 8, TILE), F32),
            v((2, 8, TILE), F32),
            v((8, TILE), F32),
            v((2, 8, TILE), F32),
            v((8, TILE), F32),
            v((HEADS, TILE, TILE), BF16),
            v((4, TILE, 768), BF16),
            v((2, TILE, 768), BF16),
            v((TILE, 768), BF16),
            v((TILE, 768), BF16),
            v((TILE, 768), BF16),
            v((192, 768), BF16),
            v((96, 768), BF16),
            v((96, 768), BF16),
            v((96, 768), BF16),
            v((TILE, 768), BF16),
            v((2 * TXT, TILE), BF16),
            v((TXT, TILE), BF16),
            v((TXT // 2, TILE), BF16),
            v((TXT // 2, TILE), BF16),
            v((TXT // 2, TILE), BF16),
            v((2 * TXT, TILE), BF16),
            v((1, TILE), BF16),
            v((TILE, TILE), BF16),
            v((TILE, TILE), BF16),
            v((TILE, TILE), BF16),
            v((2, 9, 192, HD), BF16),
            v((2, HEADS, HD // 2, TILE), BF16),
            dma((12,)),
            dma((2, 2)),
            dma((2, 4, 2)),
            dma((2,)),
            dma((2, HEADS)),
            dma((2,)),
            dma((2,)),
            dma((2,)),
            dma((2,)),
            dma((2,)),
            dma((2, 4)),
            dma((2,)),
            dma((5,)),
            dma((5,)),
            dma((4,)),
            dma((4,)),
            dma((2,)),
            dma((2,)),
            dma((1,)),
            dma((13,)),
            dma((1,)),
            dma((13,)),
            dma((2,)),
            dma((2, 4)),
            dma((2,)),
            dma((2, 4)),
            dma((2,)),
            dma((2, HEADS)),
            dma((2,)),
            dma((2, HEADS)),
        ],
        compiler_params=pltpu.CompilerParams(
            collective_id=0, has_side_effects=True, vmem_limit_bytes=60 * 1024 * 1024
        ),
    )(
        query[0], key[0], value[0], text_key[0], text_value[0], grad_out[0], gate, out_weight,
        windows.reshape(2), tile_map.reshape(8), text_count,
    )
    return pl.pallas_call(
        finish,
        out_shape=(
            sds((1, TILE, TILE), BF16),
            sds((1, TILE, TILE), BF16),
            sds((1, TILE, TILE), BF16),
            sds((1, TXT, TILE), BF16),
            sds((1, TXT, TILE), BF16),
            sds((TILE, 768), F32),
        ),
        in_specs=[anyspec] * 6,
        out_specs=(anyspec,) * 6,
        scratch_shapes=[
            v((TILE, TILE), BF16),
            v((TILE, TILE), BF16),
            v((TILE, TILE), BF16),
            v((TXT, TILE), BF16),
            v((TXT, TILE), BF16),
            v((TILE, 768), BF16),
            v((TILE, 768), F32),
            dma((2, 6)),
        ],
    )(*out)


def solution(mesh):
    placed = (
        P("dp", "sp", "tp"),
        P("dp", "sp", "tp"),
        P("dp", "sp", "tp"),
        P("dp", None, "tp"),
        P("dp", None, "tp"),
        P("dp", "sp", "tp"),
        P("dp", None),
        P("tp", "dp"),
        P("sp", None),
        P(),
        P("dp"),
    )
    return jax.shard_map(
        per_device,
        mesh=mesh,
        in_specs=placed,
        out_specs=(
            P("dp", "sp", "tp"),
            P("dp", "sp", "tp"),
            P("dp", "sp", "tp"),
            P("dp", None, "tp"),
            P("dp", None, "tp"),
            P("tp", "dp"),
        ),
        check_vma=False,
    )
```

```python
import functools

import jax
import jax.numpy as jnp
from jax import lax
from jax.experimental import pallas as pl
from jax.experimental.pallas import tpu as pltpu
from jax.sharding import PartitionSpec as P

HD = 128
TILE = 384
TXT = 256
HEADS = 3
N_TP = 8
KEYS = 3 * TILE + TXT
R_TXT = TILE
R_NEAR = (TILE + TXT, 2 * TILE + TXT)
QS = 3 * TILE
FAR = 1e30
MESH = pl.DeviceIdType.MESH
F32 = jnp.float32
BF16 = jnp.bfloat16


def dot(a, b, ca, cb):
    return lax.dot_general(a, b, (((ca,), (cb,)), ((), ())), preferred_element_type=F32)


def body(
    q_in, k_in, v_in, tk_in, tv_in, g_in, gate_in, w_in, win, tmap, tcount,
    o_q, o_k, o_v, o_tk, o_tv, o_w,
    qc, kc, vc, graw, sbuf, wbuf, scores, probs, pnear, att, d_out, acc, d_near,
    st_out, st_in, dl_out, dl_in, dl_own, ds_keep,
    gbuf, g_d, g_a, g_y, g_r, g_r1, g_r2, g_hs, g_rh, g_fin,
    tx, t_r1, t_r2, t_hs, t_rh, t_fin,
    gate_ref, q_acc, k_acc, v_acc, rbuf, dbuf, loc, zs, zr, hs_s, hs_r, qs_s, qs_r, ss_s, ss_r, do_s, do_r, dl_s, ws, wr,
    ds_, dr_, ys, yr, gs, gr, ts, tr, rs_s, rs_r, rf_s, rf_r, rd_s, rd_r, rg_s, rg_r,
):
    factor = HD ** (-0.5)
    dp = lax.axis_index("dp")
    sp = lax.axis_index("sp")
    tp = lax.axis_index("tp")
    core = dp % 2
    ylo = dp // 2
    yhi = sp // 4
    x = sp % 4
    y = yhi * 2 + ylo

    def at_xy(xx, yy, cc):
        return ((yy % 2) * 2 + cc, (yy // 2) * 4 + xx, tp)

    z_dev = (
        (dp, sp, (tp + 1) % N_TP),
        (dp, sp, (tp + N_TP - 1) % N_TP),
    )
    partner = ((ylo * 2 + 1 - core), sp, tp)
    y_next = at_xy(x, (y + 1) % 4, core)
    y_prev = at_xy(x, (y + 3) % 4, core)
    p1 = (dp, yhi * 4 + x + 1 - 2 * (x % 2), tp)
    p2 = (dp, yhi * 4 + (x + 3 + 2 * (x % 2)) % 4, tp)
    across = (dp, (1 - yhi) * 4 + x, tp)
    near_dev = ((dp, jnp.maximum(sp - 1, 0), tp), (dp, jnp.minimum(sp + 1, 7), tp))
    has = (sp > 0, sp < 7)

    def rc(src, dst, s_sem, r_sem, dev):
        return pltpu.make_async_remote_copy(
            src_ref=src, dst_ref=dst, send_sem=s_sem, recv_sem=r_sem,
            device_id=dev, device_id_type=MESH,
        )

    barrier = pltpu.get_barrier_semaphore()
    for dev in (z_dev[0], z_dev[1], partner, y_next, y_prev, p1, p2, across):
        pl.semaphore_signal(barrier, inc=1, device_id=dev, device_id_type=MESH)

    other = (1 - ylo) * 2 + core
    end = (sp == 3) | (sp == 4)
    relay = (sp == 0) | (sp == 7)
    relays = ((other, 0, tp), (other, 7, tp))
    relay_to = ((other, 4, tp), (other, 3, tp))
    relay_half = sp // 7
    flow = jnp.where(sp == 3, 0, 1)
    from_side = 1 - flow

    @pl.when(end)
    def _():
        for dev in (*relays, (dp, jnp.where(sp == 3, 4, 3), tp)):
            pl.semaphore_signal(barrier, inc=1, device_id=dev, device_id_type=MESH)

    @pl.when(relay)
    def _():
        for dev in relay_to:
            pl.semaphore_signal(barrier, inc=1, device_id=dev, device_id_type=MESH)

    gcopy = pltpu.make_async_copy(g_in, graw, loc.at[0])
    gcopy.start()
    gate_copy = pltpu.make_async_copy(
        gate_in.at[:, pl.ds(pl.multiple_of(tp * TILE, 128), TILE)], gate_ref, loc.at[5]
    )
    gate_copy.start()
    wcopy = pltpu.make_async_copy(w_in, wbuf.at[dp], loc.at[1])
    wcopy.start()
    kcopies, qcopies, vcopies = [], [], []
    for h in range(HEADS):
        cols = slice(h * HD, (h + 1) * HD)
        kcopies.append(pltpu.make_async_copy(k_in.at[:, cols], kc.at[h, 0:TILE], loc.at[2]))
        vcopies.append(pltpu.make_async_copy(v_in.at[:, cols], vc.at[h, 0:TILE], loc.at[3]))
        qcopies.append(pltpu.make_async_copy(q_in.at[:, cols], qc.at[h, 0:TILE], loc.at[4]))
        kcopies.append(
            pltpu.make_async_copy(tk_in.at[:, cols], kc.at[h, R_TXT : R_TXT + TXT], loc.at[2])
        )
        vcopies.append(
            pltpu.make_async_copy(tv_in.at[:, cols], vc.at[h, R_TXT : R_TXT + TXT], loc.at[3])
        )
    for copy in kcopies + vcopies + qcopies:
        copy.start()

    for n in range(2):

        @pl.when(jnp.logical_not(has[n]))
        def _():
            rows = slice(R_NEAR[n], R_NEAR[n] + TILE)
            qrows = slice(TILE * (n + 1), TILE * (n + 2))
            for h in range(HEADS):
                kc[h, rows, :] = jnp.zeros((TILE, HD), BF16)
                vc[h, rows, :] = jnp.zeros((TILE, HD), BF16)
                qc[h, qrows, :] = jnp.zeros((TILE, HD), BF16)
            d_near[n] = jnp.zeros((TILE, TILE), BF16)
            st_in[n] = jnp.full((8, TILE), FAR, F32)
            dl_in[n] = jnp.zeros((8, TILE), F32)

    gcopy.wait()
    gate_copy.wait()
    gate_own = gate_ref[...].astype(F32)
    sbuf[tp] = (graw[...].astype(F32) * gate_own).astype(BF16)

    n_extra = jnp.where(end, 3, 0) + jnp.where(relay, 2, 0)
    pl.semaphore_wait(barrier, 8 + n_extra)

    def z_unit(k, u, d):
        step = 1 - 2 * d
        chunk = (tp + N_TP - step * k) % N_TP
        ref = sbuf.at[chunk, pl.ds(u * 192, 192), :]
        return rc(ref, ref, zs.at[d, k // 3], zr.at[d, k, u], z_dev[d])

    def z_wait(k, u, d):
        step = 1 - 2 * d
        chunk = (tp + N_TP - step * (k + 1)) % N_TP
        ref = sbuf.at[chunk, pl.ds(u * 192, 192), :]
        rc(ref, ref, zs.at[d, k // 3], zr.at[d, k, u], z_dev[d]).wait_recv()

    for u in range(2):
        for d in range(2):
            z_unit(0, u ^ d, d).start()

    def z_service(k, units=(0, 1)):
        for u in units:
            for d in range(2):
                z_wait(k - 1, u ^ d, d)
                if k < 3 or u == 0:
                    z_unit(k, u ^ d, d).start()

    def drain(ref, sem):
        pltpu.make_async_copy(ref, ref, sem).wait()

    drain(kc.at[:, 0 : TILE + TXT], loc.at[2])
    drain(vc.at[:, 0 : TILE + TXT], loc.at[3])

    def halo(h, n, which, mine):
        src = (kc, vc)[which]
        slot = R_NEAR[1 - n] if mine else R_NEAR[n]
        return rc(
            src.at[h, 0:TILE], src.at[h, pl.ds(slot, TILE)],
            hs_s.at[n], hs_r.at[1 - n if mine else n, h], near_dev[n],
        )

    def q_halo(n, mine):
        slot = TILE * (2 - n) if mine else TILE * (1 + n)
        return rc(
            qc.at[:, pl.ds(0, TILE)], qc.at[:, pl.ds(slot, TILE)],
            qs_s.at[n], qs_r.at[1 - n if mine else n], near_dev[n],
        )

    drain(qc.at[:, 0:TILE], loc.at[4])
    wcopy.wait()
    w_part = rc(wbuf.at[dp], wbuf.at[dp], ws.at[0], wr.at[0], partner)
    w_next = rc(wbuf.at[dp, 0:192], wbuf.at[dp, 0:192], ws.at[0], wr.at[1], y_next)
    w_prev = rc(wbuf.at[dp, 192:384], wbuf.at[dp, 192:384], ws.at[0], wr.at[2], y_prev)
    def side(n):
        return (sp == 4) if n == 0 else (sp == 3)

    plain = tuple(has[n] & jnp.logical_not(side(n)) for n in range(2))

    def piece_src(piece):
        if piece < 6:
            return (kc, vc)[piece % 2].at[piece // 2]
        return qc.at[piece - 6]

    def end_send(piece, half):
        rows = slice(half * 192, half * 192 + 192)
        return rc(
            piece_src(piece).at[rows], rbuf.at[flow, piece],
            rs_s.at[0], rs_r.at[flow, min(piece // 2, 3)], relays[half],
        )

    def forward_piece(piece, f):
        start = (R_NEAR[0] if piece < 6 else TILE) + f * TILE + relay_half * 192
        dst = piece_src(piece).at[pl.ds(pl.multiple_of(start, 16), 192), :]
        return rc(rbuf.at[f, piece], dst, rf_s.at[0], rf_r.at[relay_half, min(piece // 2, 3)], relay_to[f])

    def relay_pieces(pieces):
        @pl.when(relay)
        def _():
            group = min(pieces[0] // 2, 3)
            for f in range(2):
                ref = rbuf.at[f, pieces[0] : pieces[-1] + 1]
                rc(ref, ref, rf_s.at[0], rs_r.at[f, group], relay_to[1 - f]).wait_recv()
                for piece in pieces:
                    forward_piece(piece, f).start()

    def end_wait(group):
        for half in range(2):
            ref = rbuf.at[0, 2 * group : 2 * group + (2 if group < 3 else 3)]
            rc(ref, ref, rf_s.at[0], rf_r.at[half, group], relays[half]).wait_recv()

    @pl.when(end)
    def _():
        for piece in range(9):
            for half in range(2):
                end_send(piece, half).start()

    for n in range(2):

        @pl.when(plain[n])
        def _():
            for h in range(HEADS):
                halo(h, n, 0, True).start()
                halo(h, n, 1, True).start()
            q_halo(n, True).start()

    own_pos = tmap[sp]
    bias = []
    for n in range(2):
        near_pos = tmap[(jnp.maximum(sp - 1, 0), jnp.minimum(sp + 1, 7))[n]]
        reach = jnp.where((win[0] >= 1) & has[n], win[1], -1)
        bias.append(jnp.where(jnp.abs(own_pos - near_pos) <= reach, 0.0, -FAR).astype(F32))
    text_rows = lax.broadcasted_iota(jnp.int32, (TXT, 1), 0)
    text_bias = jnp.where(text_rows < tcount[0], 0.0, -FAR).astype(F32)

    def early(h, carry):
        queries = qc[h, 0:TILE, :]
        own = factor * dot(kc[h, 0:TILE, :], queries, 1, 1)
        scores[h, 0:TILE, :] = own
        text = factor * dot(kc[h, R_TXT : R_TXT + TXT, :], queries, 1, 1) + text_bias
        scores[h, R_TXT : R_TXT + TXT, :] = text
        return carry

    lax.fori_loop(0, HEADS, early, 0)

    def take(chunk):
        cols = pl.ds(pl.multiple_of((chunk % 2) * TILE, 128), TILE)
        return dot(wbuf[chunk // 2, :, cols], sbuf[chunk], 1, 1)

    def forward(h):
        queries = qc[h, 0:TILE, :]
        for n in range(2):

            @pl.when(plain[n])
            def _():
                both = kc.at[0:2, 0:TILE]
                rc(both, both, hs_s.at[n], hs_r.at[n, h], near_dev[n]).wait_recv()

        @pl.when(end)
        def _():
            end_wait(h)

        for n in range(2):
            rows = slice(R_NEAR[n], R_NEAR[n] + TILE)
            scores[h, rows, :] = factor * dot(kc[h, rows, :], queries, 1, 1) + bias[n]
        top = jnp.max(scores[h], axis=0, keepdims=True)
        weights = jnp.exp(scores[h] - top)
        inv = 1.0 / jnp.sum(weights, axis=0, keepdims=True)
        probs[h] = (weights * inv).astype(BF16)
        for n in range(2):
            st_out[n, h : h + 1, :] = jnp.where(bias[n] < 0.0, FAR, top)
            st_out[n, h + 4 : h + 5, :] = inv
        att[h] = dot(vc[h], probs[h], 0, 0).astype(BF16)

    z_service(1, (0,))
    relay_pieces((0, 1))
    z_service(1, (1,))
    forward(0)
    relay_pieces((2, 3))
    w_part.start()

    @pl.when(jnp.logical_not(relay))
    def _():
        w_next.start()
        w_prev.start()

    forward(1)
    relay_pieces((4, 5))

    @pl.when(relay)
    def _():
        w_next.start()
        w_prev.start()

    z_service(2)
    forward(2)
    def st_copy(n, mine):
        return rc(
            st_out.at[n], st_in.at[1 - n if mine else n],
            ss_s.at[n], ss_r.at[1 - n if mine else n], near_dev[n],
        )

    for n in range(2):

        @pl.when(has[n])
        def _():
            st_copy(n, True).start()

    def grad_w(chunk):
        full = dot(att[...].reshape(HEADS * HD, TILE), sbuf[chunk], 1, 0)
        cols = pl.ds(pl.multiple_of((chunk % 2) * TILE, 128), TILE)
        gbuf[chunk // 2, :, cols] = full.astype(BF16)

    def grad_w_step(i, carry):
        grad_w((tp + i + 5) % N_TP)
        return carry

    g1 = (x % 2 + x // 2) % 2
    g2 = x // 2

    def summer(src, fin, r1, r2, hs, rh, s_sem, r_sem, sent):
        rows = src.shape[0]
        part, half, q = rows // 2, rows // 4, rows // 8

        def at(ref, start):
            return ref.at[pl.ds(pl.multiple_of(start, 16), q), :]

        def rd(ref, start):
            return ref[pl.ds(pl.multiple_of(start, 16), q), :].astype(F32)

        def low(ref, i):
            return ref[i * q : i * q + q, :].astype(F32)

        def send(from_ref, start, to_ref, sem, dev):
            return rc(at(from_ref, start), to_ref, s_sem.at[0], r_sem.at[sem], dev)

        def same(start, sem, dev):
            return send(fin, start, at(fin, start), sem, dev)

        ka, kb = g1 * half + g2 * q, part + g2 * half + g1 * q
        sa, sb = g1 * half + (1 - g2) * q, part + g2 * half + (1 - g1) * q
        fa, fb = (1 - g1) * half + (1 - g2) * q, part + (1 - g2) * half + (1 - g1) * q
        la, lb = (1 - g1) * half + g2 * q, part + (1 - g2) * half + g1 * q
        first = (
            send(src, fa, r1.at[0:q], 0, p1),
            send(src, fb, r1.at[q : 2 * q], 1, p2),
            send(src, la, r1.at[2 * q : 3 * q], 2, p1),
            send(src, lb, r1.at[3 * q : 4 * q], 2, p2),
        )
        second = (
            send(src, sa, r2.at[0:q], 2, p2),
            send(src, sb, r2.at[q : 2 * q], 2, p1),
        )
        swap = rc(hs, rh, s_sem.at[0], r_sem.at[3], across)
        spread = (same(ka, 4, p2), same(kb, 5, p1), same(ka, 6, p1), same(kb, 6, p2))
        onward = (same(sa, 6, p1), same(sb, 6, p2))
        near = (same(sa, 4, p2), same(sb, 5, p1))
        far = rc(r1, r1, s_sem.at[0], r_sem.at[6], p1)

        def go(stage):
            if stage == 0:
                for c in first:
                    c.start()
            elif stage == 1:
                for i, start in ((0, sa), (1, sb)):
                    first[i].wait_recv()
                    at(src, start)[...] = (rd(src, start) + low(r1, i)).astype(BF16)
                    second[i].start()
            elif stage == 2:
                rc(r1, r1, s_sem.at[0], r_sem.at[2], p1).wait_recv()
                for i, start in ((0, ka), (1, kb)):
                    total = rd(src, start) + low(r1, 2 + i) + low(r2, i)
                    hs[i * q : i * q + q, :] = total.astype(BF16)
                swap.start()
            elif stage == 3:
                swap.wait_recv()
                for i, start in ((0, ka), (1, kb)):
                    at(fin, start)[...] = (low(hs, i) + low(rh, i)).astype(BF16)
                for c in spread:
                    c.start()
            elif stage == 4:
                for i in range(2):
                    near[i].wait_recv()
                    onward[i].start()
            else:
                far.wait_recv()
                rc(sent, sent, s_sem.at[0], r_sem.at[0], p1).wait_send()

        return go

    g_go = summer(g_r, g_fin, g_r1, g_r2, g_hs, g_rh, gs, gr, gbuf.at[0:2, 0:336])
    t_go = summer(tx, t_fin, t_r1, t_r2, t_hs, t_rh, ts, tr, sbuf.at[0:4, 0:224])

    turn = 2 * (tp % 2) - 1
    blocks = tuple((tp // 2 + d + 4) % 4 for d in (0, turn, -turn, 2))

    def d_copy(i):
        b = blocks[i]
        return rc(gbuf.at[b], g_d.at[b // 2], ds_.at[0], dr_.at[i], partner)

    def d_send(i):
        @pl.when(blocks[i] % 2 != core)
        def _():
            d_copy(i).start()

    y_sends = [
        rc(g_a.at[0:192], g_y.at[0:192], ys.at[0], yr.at[0], y_next),
        rc(g_a.at[192:384], g_y.at[192:384], ys.at[0], yr.at[0], y_prev),
    ]

    def y_send(i):
        b = blocks[i]

        @pl.when(b % 2 == core)
        def _():
            d_copy(i).wait_recv()
            both = (gbuf[b].astype(F32) + g_d[b // 2].astype(F32)).astype(BF16)

            @pl.when(b != dp)
            def _():
                g_a[...] = both
                for c in y_sends:
                    c.start()

            @pl.when(b == dp)
            def _():
                g_r[...] = both

    def y_take(i):
        @pl.when(blocks[i] == dp)
        def _():
            rc(g_a, g_y, ys.at[0], yr.at[0], y_next).wait_recv()
            g_r[...] = (g_r[...].astype(F32) + g_y[...].astype(F32)).astype(BF16)
            g_go(0)

    def g_early(stage):
        @pl.when((blocks[0] == dp) | (blocks[1] == dp))
        def _():
            g_go(stage)

    def g_late(stage):
        @pl.when((blocks[2] == dp) | (blocks[3] == dp))
        def _():
            g_go(stage)

    lax.fori_loop(2, 5, grad_w_step, 0)
    d_send(0)
    grad_w((tp + 6) % N_TP)
    grad_w((tp + 2) % N_TP)
    d_send(1)
    def near_all():
        for n in range(2):

            @pl.when(plain[n])
            def _():
                q_halo(n, False).wait_recv()

            @pl.when(side(n))
            def _():
                end_wait(3)

            @pl.when(has[n])
            def _():
                st_copy(n, False).wait_recv()

            def near_probs(h, carry):
                s = factor * dot(kc[h, 0:TILE, :], qc[h, TILE * (n + 1) : TILE * (n + 2), :], 1, 1)
                p = jnp.exp(s - st_in[n, pl.ds(h, 1), :]) * st_in[n, pl.ds(h + 4, 1), :]
                pnear[n, h] = p.astype(BF16)
                return carry

            lax.fori_loop(0, HEADS, near_probs, 0)


    z_service(3, (0,))
    relay_pieces((6, 7, 8))
    y_send(0)
    acc[...] = jnp.zeros_like(acc)
    last = (tp + 4) % N_TP

    def take_group(first, least, most):
        def one(i, carry):
            away = (first + i + N_TP - tp) % N_TP
            away = jnp.minimum(away, N_TP - away)

            @pl.when((away >= least) & (away <= most))
            def _():
                acc[...] += take(first + i)

            return carry

        lax.fori_loop(0, 4, one, 0)

    mate = ylo * 2 + 1 - core
    rc(wbuf.at[mate], wbuf.at[mate], ws.at[0], wr.at[0], partner).wait_recv()
    take_group(ylo * 4, 0, 2)
    w_fwd = []
    for half in range(2):
        rows = slice(half * 192, half * 192 + 192)
        ref = wbuf.at[other, rows]
        rc(ref, ref, ws.at[0], wr.at[1 + half], y_next).wait_recv()
        fwd = rc(ref, ref, ws.at[0], wr.at[3 + half], partner)
        fwd.start()
        w_fwd.append(fwd)
    y_send(1)
    @pl.when(jnp.logical_not(end))
    def _():
        near_all()

    z_service(3, (1,))
    take_group(ylo * 4, 3, 3)
    grad_w((tp + 5) % N_TP)
    grad_w((tp + 3) % N_TP)
    d_send(2)

    mate_other = (1 - ylo) * 2 + 1 - core
    for half in range(2):
        ref = wbuf.at[mate_other, half * 192 : half * 192 + 192]
        rc(ref, ref, ws.at[0], wr.at[3 + half], partner).wait_recv()

    take_group(4 - ylo * 4, 0, 3)
    @pl.when(end)
    def _():
        near_all()

    y_take(0)
    y_send(2)
    y_take(1)
    z_wait(3, 0, 0)
    z_wait(3, 1, 1)
    total = acc[...] + take(last)
    d_out[...] = total.astype(BF16)
    dl_out[...] = jnp.zeros((8, TILE), F32)
    for h in range(HEADS):
        both = d_out[h * HD : (h + 1) * HD, :].astype(F32) * att[h].astype(F32)
        dl_out[h : h + 1, :] = jnp.sum(both, axis=0, keepdims=True)

    def do_copy(n, mine, h):
        to = 1 - n if mine else n
        rows = slice(h * HD, h * HD + HD)
        return rc(d_out.at[rows], d_near.at[to, rows], do_s.at[n], do_r.at[to, h], near_dev[n])

    def dl_copy(n, mine):
        to = 1 - n if mine else n
        return rc(dl_out, dl_in.at[to], dl_s.at[n], do_r.at[to, 3], near_dev[n])

    half_rows = HD // 2

    def end_grad(h, half):
        rows = slice(h * HD + half * half_rows, h * HD + (half + 1) * half_rows)
        return rc(
            d_out.at[rows], dbuf.at[flow, h], rd_s.at[0], rd_r.at[flow, h], relays[half]
        )

    def forward_grad(h, f):
        rows = pl.ds(pl.multiple_of(h * HD + relay_half * half_rows, 16), half_rows)
        return rc(
            dbuf.at[f, h], d_near.at[f, rows, :], rg_s.at[0], rg_r.at[relay_half, h], relay_to[f]
        )

    def relay_grads(h):
        @pl.when(relay)
        def _():
            for f in range(2):
                ref = dbuf.at[f, h]
                rc(ref, ref, rg_s.at[0], rd_r.at[f, h], relay_to[1 - f]).wait_recv()
                forward_grad(h, f).start()

    def relay_send(h):
        @pl.when(end)
        def _():
            for half in range(2):
                end_grad(h, half).start()

    def send_grads(h):
        for n in range(2):

            @pl.when(plain[n])
            def _():
                do_copy(n, True, h).start()

    def wait_grads(h):
        @pl.when(end)
        def _():
            for half in range(2):
                ref = dbuf.at[0, h]
                rc(ref, ref, rg_s.at[0], rg_r.at[half, h], relays[half]).wait_recv()

        for n in range(2):

            @pl.when(plain[n])
            def _():
                do_copy(n, False, h).wait_recv()

    for n in range(2):

        @pl.when(has[n])
        def _():
            dl_copy(n, True).start()

    relay_send(0)
    grad_w(last)
    d_send(3)
    def backward(h):
        lanes = slice(h * HD, (h + 1) * HD)
        grads = d_out[lanes, :]
        delta = dl_out[h : h + 1, :]
        g = dot(vc[h], grads, 1, 0)
        ds = (probs[h].astype(F32) * (g - delta)).astype(BF16)
        ds_keep[h] = ds[0:TILE, :]
        gq = factor * dot(kc[h], ds, 0, 0)
        q_acc[:, lanes] = gq.T.astype(BF16)
        trows = slice(R_TXT, R_TXT + TXT)
        tx[0:TXT, lanes] = (factor * dot(ds[trows, :], qc[h, 0:TILE, :], 1, 0)).astype(BF16)
        tx[TXT : 2 * TXT, lanes] = dot(probs[h, trows, :], grads, 1, 1).astype(BF16)


    backward(0)
    backward(1)
    y_send(3)
    backward(2)
    q_out = pltpu.make_async_copy(q_acc, o_q, loc.at[6])
    q_out.start()
    t_go(0)
    g_early(1)
    y_take(2)
    send_grads(0)
    relay_send(1)
    relay_grads(0)
    g_early(2)
    y_take(3)
    relay_send(2)
    t_go(1)
    send_grads(1)
    for n in range(2):

        @pl.when(has[n])
        def _():
            dl_copy(n, False).wait_recv()

    def own_keys(h):
        lanes = slice(h * HD, (h + 1) * HD)
        hrows = lanes
        gk = dot(ds_keep[h], qc[h, 0:TILE, :], 1, 0)
        gv = dot(probs[h, 0:TILE, :], d_out[hrows, :], 1, 1)
        for n in range(2):
            grads = d_near[n, hrows, :]
            p = pnear[n, h]
            g = dot(vc[h, 0:TILE, :], grads, 1, 0)
            ds = (p.astype(F32) * (g - dl_in[n, h : h + 1, :])).astype(BF16)
            gk += dot(ds, qc[h, TILE * (n + 1) : TILE * (n + 2), :], 1, 0)
            gv += dot(p, grads, 1, 1)
        k_acc[:, lanes] = (factor * gk).astype(BF16)
        v_acc[:, lanes] = gv.astype(BF16)

    g_late(1)
    relay_grads(1)
    g_early(3)
    send_grads(2)
    relay_grads(2)
    t_go(2)
    wait_grads(0)
    own_keys(0)
    g_late(2)
    g_early(4)
    t_go(3)
    wait_grads(1)
    own_keys(1)
    g_late(3)
    wait_grads(2)
    own_keys(2)
    k_out = pltpu.make_async_copy(k_acc, o_k, loc.at[6])
    k_out.start()
    v_out = pltpu.make_async_copy(v_acc, o_v, loc.at[6])
    v_out.start()
    t_go(4)
    g_early(5)
    g_late(4)
    t_go(5)
    tk_out = pltpu.make_async_copy(t_fin.at[0:TXT], o_tk, loc.at[6])
    tk_out.start()
    tv_out = pltpu.make_async_copy(t_fin.at[TXT : 2 * TXT], o_tv, loc.at[6])
    tv_out.start()
    g_late(5)
    w_out = pltpu.make_async_copy(g_fin, o_w, loc.at[6])
    w_out.start()
    def drain_sends(ref, sem):
        rc(ref, ref, sem, zr.at[0, 0, 0], partner).wait_send()

    for d in range(2):
        drain_sends(sbuf.at[0:3], zs.at[d, 0])
        drain_sends(sbuf.at[0, 0:192], zs.at[d, 1])
    drain_sends(gbuf.at[0:3], ws.at[0])
    drain_sends(g_a, ys.at[0])
    drain_sends(gbuf.at[0:2], ds_.at[0])

    drain(sbuf.at[:, 0:304], loc.at[6])
    for n in range(2):

        @pl.when(plain[n])
        def _():
            drain_sends(kc.at[:, 0 : 2 * TILE], hs_s.at[n])
            q_halo(n, True).wait_send()
            drain_sends(d_out, do_s.at[n])

        @pl.when(has[n])
        def _():
            st_copy(n, True).wait_send()
            dl_copy(n, True).wait_send()

    @pl.when(end)
    def _():
        drain_sends(rbuf, rs_s.at[0])
        drain_sends(dbuf, rd_s.at[0])

    @pl.when(relay)
    def _():
        drain_sends(rbuf, rf_s.at[0])
        drain_sends(dbuf, rg_s.at[0])


def finish(*refs):
    given, results, held, wide, sems = refs[:6], refs[6:12], refs[12:18], refs[18], refs[19]
    loads = [pltpu.make_async_copy(given[i], held[i], sems.at[0, i]) for i in range(6)]
    for i in (5, 0, 1, 2, 3, 4):
        loads[i].start()
    stores = []
    for i in (5, 0, 1, 2, 3, 4):
        loads[i].wait()
        if i == 5:
            wide[...] = held[i][...].astype(F32)
            stores.append(pltpu.make_async_copy(wide, results[i], sems.at[1, i]))
        else:
            stores.append(pltpu.make_async_copy(held[i], results[i].at[0], sems.at[1, i]))
        stores[-1].start()
    for copy in stores:
        copy.wait()


def per_device(
    query, key, value, text_key, text_value, grad_out, gate, out_weight, windows, tile_map, text_count
):
    anyspec = pl.BlockSpec(memory_space=pl.ANY)
    vmem = pl.BlockSpec(memory_space=pltpu.VMEM)
    smem = pl.BlockSpec(memory_space=pltpu.SMEM)
    sds = jax.ShapeDtypeStruct
    v = pltpu.VMEM
    dma = pltpu.SemaphoreType.DMA
    out = pl.pallas_call(
        body,
        out_shape=(
            sds((TILE, TILE), BF16),
            sds((TILE, TILE), BF16),
            sds((TILE, TILE), BF16),
            sds((TXT, TILE), BF16),
            sds((TXT, TILE), BF16),
            sds((TILE, 768), BF16),
        ),
        in_specs=[anyspec] * 8 + [smem] * 3,
        out_specs=(anyspec,) * 6,
        scratch_shapes=[
            v((HEADS, QS, HD), BF16),
            v((HEADS, KEYS, HD), BF16),
            v((HEADS, KEYS, HD), BF16),
            v((TILE, TILE), BF16),
            v((N_TP, TILE, TILE), BF16),
            v((4, TILE, 768), BF16),
            v((HEADS, KEYS, TILE), F32),
            v((HEADS, KEYS, TILE), BF16),
            v((2, HEADS, TILE, TILE), BF16),
            v((HEADS, HD, TILE), BF16),
            v((TILE, TILE), BF16),
            v((TILE, TILE), F32),
            v((2, TILE, TILE), BF16),
            v((2, 8, TILE), F32),
            v((2, 8, TILE), F32),
            v((8, TILE), F32),
            v((2, 8, TILE), F32),
            v((8, TILE), F32),
            v((HEADS, TILE, TILE), BF16),
            v((4, TILE, 768), BF16),
            v((2, TILE, 768), BF16),
            v((TILE, 768), BF16),
            v((TILE, 768), BF16),
            v((TILE, 768), BF16),
            v((192, 768), BF16),
            v((96, 768), BF16),
            v((96, 768), BF16),
            v((96, 768), BF16),
            v((TILE, 768), BF16),
            v((2 * TXT, TILE), BF16),
            v((TXT, TILE), BF16),
            v((TXT // 2, TILE), BF16),
            v((TXT // 2, TILE), BF16),
            v((TXT // 2, TILE), BF16),
            v((2 * TXT, TILE), BF16),
            v((1, TILE), BF16),
            v((TILE, TILE), BF16),
            v((TILE, TILE), BF16),
            v((TILE, TILE), BF16),
            v((2, 9, 192, HD), BF16),
            v((2, HEADS, HD // 2, TILE), BF16),
            dma((7,)),
            dma((2, 2)),
            dma((2, 4, 2)),
            dma((2,)),
            dma((2, HEADS)),
            dma((2,)),
            dma((2,)),
            dma((2,)),
            dma((2,)),
            dma((2,)),
            dma((2, 4)),
            dma((2,)),
            dma((1,)),
            dma((5,)),
            dma((1,)),
            dma((4,)),
            dma((1,)),
            dma((1,)),
            dma((1,)),
            dma((7,)),
            dma((1,)),
            dma((7,)),
            dma((1,)),
            dma((2, 4)),
            dma((1,)),
            dma((2, 4)),
            dma((1,)),
            dma((2, HEADS)),
            dma((1,)),
            dma((2, HEADS)),
        ],
        compiler_params=pltpu.CompilerParams(
            collective_id=0, has_side_effects=True, vmem_limit_bytes=60 * 1024 * 1024
        ),
    )(
        query[0], key[0], value[0], text_key[0], text_value[0], grad_out[0], gate, out_weight,
        windows.reshape(2), tile_map.reshape(8), text_count,
    )
    return pl.pallas_call(
        finish,
        out_shape=(
            sds((1, TILE, TILE), BF16),
            sds((1, TILE, TILE), BF16),
            sds((1, TILE, TILE), BF16),
            sds((1, TXT, TILE), BF16),
            sds((1, TXT, TILE), BF16),
            sds((TILE, 768), F32),
        ),
        in_specs=[anyspec] * 6,
        out_specs=(anyspec,) * 6,
        scratch_shapes=[
            v((TILE, TILE), BF16),
            v((TILE, TILE), BF16),
            v((TILE, TILE), BF16),
            v((TXT, TILE), BF16),
            v((TXT, TILE), BF16),
            v((TILE, 768), BF16),
            v((TILE, 768), F32),
            dma((2, 6)),
        ],
    )(*out)


def solution(mesh):
    placed = (
        P("dp", "sp", "tp"),
        P("dp", "sp", "tp"),
        P("dp", "sp", "tp"),
        P("dp", None, "tp"),
        P("dp", None, "tp"),
        P("dp", "sp", "tp"),
        P("dp", None),
        P("tp", "dp"),
        P("sp", None),
        P(),
        P("dp"),
    )
    return jax.shard_map(
        per_device,
        mesh=mesh,
        in_specs=placed,
        out_specs=(
            P("dp", "sp", "tp"),
            P("dp", "sp", "tp"),
            P("dp", "sp", "tp"),
            P("dp", None, "tp"),
            P("dp", None, "tp"),
            P("tp", "dp"),
        ),
        check_vma=False,
    )
```

```python
import functools

import jax
import jax.numpy as jnp
from jax import lax
from jax.experimental import pallas as pl
from jax.experimental.pallas import tpu as pltpu
from jax.sharding import PartitionSpec as P

HD = 128
TILE = 384
TXT = 256
HEADS = 3
N_TP = 8
KEYS = 3 * TILE + TXT
R_TXT = TILE
R_NEAR = (TILE + TXT, 2 * TILE + TXT)
QS = 3 * TILE
FAR = 1e30
MESH = pl.DeviceIdType.MESH
F32 = jnp.float32
BF16 = jnp.bfloat16


def dot(a, b, ca, cb):
    return lax.dot_general(a, b, (((ca,), (cb,)), ((), ())), preferred_element_type=F32)


def body(
    q_in, k_in, v_in, tk_in, tv_in, g_in, gate_in, w_in, win, tmap, tcount,
    o_q, o_k, o_v, o_tk, o_tv, o_w,
    qc, kc, vc, graw, sbuf, wbuf, scores, probs, pnear, att, d_out, acc, d_near,
    st_out, st_in, dl_out, dl_in, dl_own, ds_keep,
    gbuf, g_d, g_a, g_y, g_r, g_r1, g_r2, g_hs, g_rh, g_fin,
    tx, t_r1, t_r2, t_hs, t_rh, t_fin,
    gate_ref, q_acc, k_acc, v_acc, rbuf, dbuf, loc, zs, zr, hs_s, hs_r, qs_s, qs_r, ss_s, ss_r, do_s, do_r, dl_s, ws, wr,
    ds_, dr_, ys, yr, gs, gr, ts, tr, rs_s, rs_r, rf_s, rf_r, rd_s, rd_r, rg_s, rg_r,
):
    factor = HD ** (-0.5)
    dp = lax.axis_index("dp")
    sp = lax.axis_index("sp")
    tp = lax.axis_index("tp")
    core = dp % 2
    ylo = dp // 2
    yhi = sp // 4
    x = sp % 4
    y = yhi * 2 + ylo

    def at_xy(xx, yy, cc):
        return ((yy % 2) * 2 + cc, (yy // 2) * 4 + xx, tp)

    z_dev = (
        (dp, sp, (tp + 1) % N_TP),
        (dp, sp, (tp + N_TP - 1) % N_TP),
    )
    partner = ((ylo * 2 + 1 - core), sp, tp)
    y_next = at_xy(x, (y + 1) % 4, core)
    y_prev = at_xy(x, (y + 3) % 4, core)
    p1 = (dp, yhi * 4 + x + 1 - 2 * (x % 2), tp)
    p2 = (dp, yhi * 4 + (x + 3 + 2 * (x % 2)) % 4, tp)
    across = (dp, (1 - yhi) * 4 + x, tp)
    near_dev = ((dp, jnp.maximum(sp - 1, 0), tp), (dp, jnp.minimum(sp + 1, 7), tp))
    has = (sp > 0, sp < 7)

    def rc(src, dst, s_sem, r_sem, dev):
        return pltpu.make_async_remote_copy(
            src_ref=src, dst_ref=dst, send_sem=s_sem, recv_sem=r_sem,
            device_id=dev, device_id_type=MESH,
        )

    barrier = pltpu.get_barrier_semaphore()
    for dev in (z_dev[0], z_dev[1], partner, y_next, y_prev, p1, p2, across):
        pl.semaphore_signal(barrier, inc=1, device_id=dev, device_id_type=MESH)

    other = (1 - ylo) * 2 + core
    end = (sp == 3) | (sp == 4)
    relay = (sp == 0) | (sp == 7)
    relays = ((other, 0, tp), (other, 7, tp))
    relay_to = ((other, 4, tp), (other, 3, tp))
    relay_half = sp // 7
    flow = jnp.where(sp == 3, 0, 1)
    from_side = 1 - flow

    @pl.when(end)
    def _():
        for dev in (*relays, (dp, jnp.where(sp == 3, 4, 3), tp)):
            pl.semaphore_signal(barrier, inc=1, device_id=dev, device_id_type=MESH)

    @pl.when(relay)
    def _():
        for dev in relay_to:
            pl.semaphore_signal(barrier, inc=1, device_id=dev, device_id_type=MESH)

    gcopy = pltpu.make_async_copy(g_in, graw, loc.at[0])
    gcopy.start()
    gate_copy = pltpu.make_async_copy(
        gate_in.at[:, pl.ds(pl.multiple_of(tp * TILE, 128), TILE)], gate_ref, loc.at[5]
    )
    gate_copy.start()
    wcopy = pltpu.make_async_copy(w_in, wbuf.at[dp], loc.at[1])
    wcopy.start()
    kcopies, qcopies, vcopies = [], [], []
    for h in range(HEADS):
        cols = slice(h * HD, (h + 1) * HD)
        kcopies.append(pltpu.make_async_copy(k_in.at[:, cols], kc.at[h, 0:TILE], loc.at[2]))
        vcopies.append(pltpu.make_async_copy(v_in.at[:, cols], vc.at[h, 0:TILE], loc.at[3]))
        qcopies.append(pltpu.make_async_copy(q_in.at[:, cols], qc.at[h, 0:TILE], loc.at[4]))
        kcopies.append(
            pltpu.make_async_copy(tk_in.at[:, cols], kc.at[h, R_TXT : R_TXT + TXT], loc.at[2])
        )
        vcopies.append(
            pltpu.make_async_copy(tv_in.at[:, cols], vc.at[h, R_TXT : R_TXT + TXT], loc.at[3])
        )
    for copy in kcopies + vcopies + qcopies:
        copy.start()

    for n in range(2):

        @pl.when(jnp.logical_not(has[n]))
        def _():
            rows = slice(R_NEAR[n], R_NEAR[n] + TILE)
            qrows = slice(TILE * (n + 1), TILE * (n + 2))
            for h in range(HEADS):
                kc[h, rows, :] = jnp.zeros((TILE, HD), BF16)
                vc[h, rows, :] = jnp.zeros((TILE, HD), BF16)
                qc[h, qrows, :] = jnp.zeros((TILE, HD), BF16)
            d_near[n] = jnp.zeros((TILE, TILE), BF16)
            st_in[n] = jnp.full((8, TILE), FAR, F32)
            dl_in[n] = jnp.zeros((8, TILE), F32)

    gcopy.wait()
    gate_copy.wait()
    gate_own = gate_ref[...].astype(F32)
    sbuf[tp] = (graw[...].astype(F32) * gate_own).astype(BF16)

    n_extra = jnp.where(end, 3, 0) + jnp.where(relay, 2, 0)
    pl.semaphore_wait(barrier, 8 + n_extra)

    def z_unit(k, u, d):
        step = 1 - 2 * d
        chunk = (tp + N_TP - step * k) % N_TP
        ref = sbuf.at[chunk, pl.ds(u * 192, 192), :]
        return rc(ref, ref, zs.at[d, k // 3], zr.at[d, k, u], z_dev[d])

    def z_wait(k, u, d):
        step = 1 - 2 * d
        chunk = (tp + N_TP - step * (k + 1)) % N_TP
        ref = sbuf.at[chunk, pl.ds(u * 192, 192), :]
        rc(ref, ref, zs.at[d, k // 3], zr.at[d, k, u], z_dev[d]).wait_recv()

    for u in range(2):
        for d in range(2):
            z_unit(0, u ^ d, d).start()

    def z_service(k, units=(0, 1)):
        for u in units:
            for d in range(2):
                z_wait(k - 1, u ^ d, d)
                if k < 3 or u == 0:
                    z_unit(k, u ^ d, d).start()

    def drain(ref, sem):
        pltpu.make_async_copy(ref, ref, sem).wait()

    drain(kc.at[:, 0 : TILE + TXT], loc.at[2])
    drain(vc.at[:, 0 : TILE + TXT], loc.at[3])

    def halo(h, n, which, mine):
        src = (kc, vc)[which]
        slot = R_NEAR[1 - n] if mine else R_NEAR[n]
        return rc(
            src.at[h, 0:TILE], src.at[h, pl.ds(slot, TILE)],
            hs_s.at[n], hs_r.at[1 - n if mine else n, h], near_dev[n],
        )

    def q_halo(n, mine):
        slot = TILE * (2 - n) if mine else TILE * (1 + n)
        return rc(
            qc.at[:, pl.ds(0, TILE)], qc.at[:, pl.ds(slot, TILE)],
            qs_s.at[n], qs_r.at[1 - n if mine else n], near_dev[n],
        )

    drain(qc.at[:, 0:TILE], loc.at[4])
    wcopy.wait()
    w_part = rc(wbuf.at[dp], wbuf.at[dp], ws.at[0], wr.at[0], partner)
    w_next = rc(wbuf.at[dp, 0:192], wbuf.at[dp, 0:192], ws.at[0], wr.at[1], y_next)
    w_prev = rc(wbuf.at[dp, 192:384], wbuf.at[dp, 192:384], ws.at[0], wr.at[2], y_prev)
    def side(n):
        return (sp == 4) if n == 0 else (sp == 3)

    plain = tuple(has[n] & jnp.logical_not(side(n)) for n in range(2))

    def piece_src(piece):
        if piece < 6:
            return (kc, vc)[piece % 2].at[piece // 2]
        return qc.at[piece - 6]

    def end_send(piece, half):
        rows = slice(half * 192, half * 192 + 192)
        return rc(
            piece_src(piece).at[rows], rbuf.at[flow, piece],
            rs_s.at[0], rs_r.at[flow, min(piece // 2, 3)], relays[half],
        )

    def forward_piece(piece, f):
        start = (R_NEAR[0] if piece < 6 else TILE) + f * TILE + relay_half * 192
        dst = piece_src(piece).at[pl.ds(pl.multiple_of(start, 16), 192), :]
        return rc(rbuf.at[f, piece], dst, rf_s.at[0], rf_r.at[relay_half, min(piece // 2, 3)], relay_to[f])

    def relay_pieces(pieces):
        @pl.when(relay)
        def _():
            group = min(pieces[0] // 2, 3)
            for f in range(2):
                ref = rbuf.at[f, pieces[0] : pieces[-1] + 1]
                rc(ref, ref, rf_s.at[0], rs_r.at[f, group], relay_to[1 - f]).wait_recv()
                for piece in pieces:
                    forward_piece(piece, f).start()

    def end_wait(group):
        for half in range(2):
            ref = rbuf.at[0, 2 * group : 2 * group + (2 if group < 3 else 3)]
            rc(ref, ref, rf_s.at[0], rf_r.at[half, group], relays[half]).wait_recv()

    @pl.when(end)
    def _():
        for piece in range(9):
            for half in range(2):
                end_send(piece, half).start()

    for n in range(2):

        @pl.when(plain[n])
        def _():
            for h in range(HEADS):
                halo(h, n, 0, True).start()
                halo(h, n, 1, True).start()
            q_halo(n, True).start()

    own_pos = tmap[sp]
    bias = []
    for n in range(2):
        near_pos = tmap[(jnp.maximum(sp - 1, 0), jnp.minimum(sp + 1, 7))[n]]
        reach = jnp.where((win[0] >= 1) & has[n], win[1], -1)
        bias.append(jnp.where(jnp.abs(own_pos - near_pos) <= reach, 0.0, -FAR).astype(F32))
    text_rows = lax.broadcasted_iota(jnp.int32, (TXT, 1), 0)
    text_bias = jnp.where(text_rows < tcount[0], 0.0, -FAR).astype(F32)

    def early(h, carry):
        queries = qc[h, 0:TILE, :]
        own = factor * dot(kc[h, 0:TILE, :], queries, 1, 1)
        scores[h, 0:TILE, :] = own
        text = factor * dot(kc[h, R_TXT : R_TXT + TXT, :], queries, 1, 1) + text_bias
        scores[h, R_TXT : R_TXT + TXT, :] = text
        return carry

    lax.fori_loop(0, HEADS, early, 0)

    def take(chunk):
        cols = pl.ds(pl.multiple_of((chunk % 2) * TILE, 128), TILE)
        return dot(wbuf[chunk // 2, :, cols], sbuf[chunk], 1, 1)

    def forward(h):
        queries = qc[h, 0:TILE, :]
        for n in range(2):

            @pl.when(plain[n])
            def _():
                both = kc.at[0:2, 0:TILE]
                rc(both, both, hs_s.at[n], hs_r.at[n, h], near_dev[n]).wait_recv()

        @pl.when(end)
        def _():
            end_wait(h)

        for n in range(2):
            rows = slice(R_NEAR[n], R_NEAR[n] + TILE)
            scores[h, rows, :] = factor * dot(kc[h, rows, :], queries, 1, 1) + bias[n]
        top = jnp.max(scores[h], axis=0, keepdims=True)
        weights = jnp.exp(scores[h] - top)
        inv = 1.0 / jnp.sum(weights, axis=0, keepdims=True)
        probs[h] = (weights * inv).astype(BF16)
        for n in range(2):
            st_out[n, h : h + 1, :] = jnp.where(bias[n] < 0.0, FAR, top)
            st_out[n, h + 4 : h + 5, :] = inv
        att[h] = dot(vc[h], probs[h], 0, 0).astype(BF16)

    z_service(1, (0,))
    relay_pieces((0, 1))
    z_service(1, (1,))
    forward(0)
    relay_pieces((2, 3))
    w_part.start()

    @pl.when(jnp.logical_not(relay))
    def _():
        w_next.start()
        w_prev.start()

    forward(1)
    relay_pieces((4, 5))

    @pl.when(relay)
    def _():
        w_next.start()
        w_prev.start()

    z_service(2)
    forward(2)
    def st_copy(n, mine):
        return rc(
            st_out.at[n], st_in.at[1 - n if mine else n],
            ss_s.at[n], ss_r.at[1 - n if mine else n], near_dev[n],
        )

    for n in range(2):

        @pl.when(has[n])
        def _():
            st_copy(n, True).start()

    def grad_w(chunk):
        full = dot(att[...].reshape(HEADS * HD, TILE), sbuf[chunk], 1, 0)
        cols = pl.ds(pl.multiple_of((chunk % 2) * TILE, 128), TILE)
        gbuf[chunk // 2, :, cols] = full.astype(BF16)

    def grad_w_step(i, carry):
        grad_w((tp + i + 5) % N_TP)
        return carry

    g1 = (x % 2 + x // 2) % 2
    g2 = x // 2

    def summer(src, fin, r1, r2, hs, rh, s_sem, r_sem, sent):
        rows = src.shape[0]
        part, half, q = rows // 2, rows // 4, rows // 8

        def at(ref, start):
            return ref.at[pl.ds(pl.multiple_of(start, 16), q), :]

        def rd(ref, start):
            return ref[pl.ds(pl.multiple_of(start, 16), q), :].astype(F32)

        def low(ref, i):
            return ref[i * q : i * q + q, :].astype(F32)

        def send(from_ref, start, to_ref, sem, dev):
            return rc(at(from_ref, start), to_ref, s_sem.at[0], r_sem.at[sem], dev)

        def same(start, sem, dev):
            return send(fin, start, at(fin, start), sem, dev)

        ka, kb = g1 * half + g2 * q, part + g2 * half + g1 * q
        sa, sb = g1 * half + (1 - g2) * q, part + g2 * half + (1 - g1) * q
        fa, fb = (1 - g1) * half + (1 - g2) * q, part + (1 - g2) * half + (1 - g1) * q
        la, lb = (1 - g1) * half + g2 * q, part + (1 - g2) * half + g1 * q
        first = (
            send(src, fa, r1.at[0:q], 0, p1),
            send(src, fb, r1.at[q : 2 * q], 1, p2),
            send(src, la, r1.at[2 * q : 3 * q], 2, p1),
            send(src, lb, r1.at[3 * q : 4 * q], 2, p2),
        )
        second = (
            send(src, sa, r2.at[0:q], 2, p2),
            send(src, sb, r2.at[q : 2 * q], 2, p1),
        )
        swap = rc(hs, rh, s_sem.at[0], r_sem.at[3], across)
        spread = (same(ka, 4, p2), same(kb, 5, p1), same(ka, 6, p1), same(kb, 6, p2))
        onward = (same(sa, 6, p1), same(sb, 6, p2))
        near = (same(sa, 4, p2), same(sb, 5, p1))
        far = rc(r1, r1, s_sem.at[0], r_sem.at[6], p1)

        def go(stage):
            if stage == 0:
                for c in first:
                    c.start()
            elif stage == 1:
                for i, start in ((0, sa), (1, sb)):
                    first[i].wait_recv()
                    at(src, start)[...] = (rd(src, start) + low(r1, i)).astype(BF16)
                    second[i].start()
            elif stage == 2:
                rc(r1, r1, s_sem.at[0], r_sem.at[2], p1).wait_recv()
                for i, start in ((0, ka), (1, kb)):
                    total = rd(src, start) + low(r1, 2 + i) + low(r2, i)
                    hs[i * q : i * q + q, :] = total.astype(BF16)
                swap.start()
            elif stage == 3:
                swap.wait_recv()
                for i, start in ((0, ka), (1, kb)):
                    at(fin, start)[...] = (low(hs, i) + low(rh, i)).astype(BF16)
                for c in spread:
                    c.start()
            elif stage == 4:
                for i in range(2):
                    near[i].wait_recv()
                    onward[i].start()
            else:
                far.wait_recv()
                rc(sent, sent, s_sem.at[0], r_sem.at[0], p1).wait_send()

        return go

    g_go = summer(g_r, g_fin, g_r1, g_r2, g_hs, g_rh, gs, gr, gbuf.at[0:2, 0:336])
    t_go = summer(tx, t_fin, t_r1, t_r2, t_hs, t_rh, ts, tr, sbuf.at[0:4, 0:224])

    turn = 2 * (tp % 2) - 1
    blocks = tuple((tp // 2 + d + 4) % 4 for d in (0, turn, -turn, 2))

    def d_copy(i):
        b = blocks[i]
        return rc(gbuf.at[b], g_d.at[b // 2], ds_.at[0], dr_.at[i], partner)

    def d_send(i):
        @pl.when(blocks[i] % 2 != core)
        def _():
            d_copy(i).start()

    y_sends = [
        rc(g_a.at[0:192], g_y.at[0:192], ys.at[0], yr.at[0], y_next),
        rc(g_a.at[192:384], g_y.at[192:384], ys.at[0], yr.at[0], y_prev),
    ]

    def y_send(i):
        b = blocks[i]

        @pl.when(b % 2 == core)
        def _():
            d_copy(i).wait_recv()
            both = (gbuf[b].astype(F32) + g_d[b // 2].astype(F32)).astype(BF16)

            @pl.when(b != dp)
            def _():
                g_a[...] = both
                for c in y_sends:
                    c.start()

            @pl.when(b == dp)
            def _():
                g_r[...] = both

    def y_take(i):
        @pl.when(blocks[i] == dp)
        def _():
            rc(g_a, g_y, ys.at[0], yr.at[0], y_next).wait_recv()
            g_r[...] = (g_r[...].astype(F32) + g_y[...].astype(F32)).astype(BF16)
            g_go(0)

    def g_early(stage):
        @pl.when((blocks[0] == dp) | (blocks[1] == dp))
        def _():
            g_go(stage)

    def g_late(stage):
        @pl.when((blocks[2] == dp) | (blocks[3] == dp))
        def _():
            g_go(stage)

    lax.fori_loop(2, 5, grad_w_step, 0)
    d_send(0)
    grad_w((tp + 6) % N_TP)
    grad_w((tp + 2) % N_TP)
    d_send(1)
    def near_all():
        for n in range(2):

            @pl.when(plain[n])
            def _():
                q_halo(n, False).wait_recv()

            @pl.when(side(n))
            def _():
                end_wait(3)

            @pl.when(has[n])
            def _():
                st_copy(n, False).wait_recv()

            def near_probs(h, carry):
                s = factor * dot(kc[h, 0:TILE, :], qc[h, TILE * (n + 1) : TILE * (n + 2), :], 1, 1)
                p = jnp.exp(s - st_in[n, pl.ds(h, 1), :]) * st_in[n, pl.ds(h + 4, 1), :]
                pnear[n, h] = p.astype(BF16)
                return carry

            lax.fori_loop(0, HEADS, near_probs, 0)


    z_service(3, (0,))
    relay_pieces((6, 7, 8))
    y_send(0)
    acc[...] = jnp.zeros_like(acc)
    last = (tp + 4) % N_TP

    def take_group(first, least, most):
        def one(i, carry):
            away = (first + i + N_TP - tp) % N_TP
            away = jnp.minimum(away, N_TP - away)

            @pl.when((away >= least) & (away <= most))
            def _():
                acc[...] += take(first + i)

            return carry

        lax.fori_loop(0, 4, one, 0)

    mate = ylo * 2 + 1 - core
    rc(wbuf.at[mate], wbuf.at[mate], ws.at[0], wr.at[0], partner).wait_recv()
    take_group(ylo * 4, 0, 2)
    w_fwd = []
    for half in range(2):
        rows = slice(half * 192, half * 192 + 192)
        ref = wbuf.at[other, rows]
        rc(ref, ref, ws.at[0], wr.at[1 + half], y_next).wait_recv()
        fwd = rc(ref, ref, ws.at[0], wr.at[3 + half], partner)
        fwd.start()
        w_fwd.append(fwd)
    y_send(1)
    @pl.when(jnp.logical_not(end))
    def _():
        near_all()

    z_service(3, (1,))
    take_group(ylo * 4, 3, 3)
    grad_w((tp + 5) % N_TP)
    grad_w((tp + 3) % N_TP)
    d_send(2)

    mate_other = (1 - ylo) * 2 + 1 - core
    for half in range(2):
        ref = wbuf.at[mate_other, half * 192 : half * 192 + 192]
        rc(ref, ref, ws.at[0], wr.at[3 + half], partner).wait_recv()

    take_group(4 - ylo * 4, 0, 3)
    @pl.when(end)
    def _():
        near_all()

    y_take(0)
    y_send(2)
    y_take(1)
    z_wait(3, 0, 0)
    z_wait(3, 1, 1)
    total = acc[...] + take(last)
    d_out[...] = total.astype(BF16)
    dl_out[...] = jnp.zeros((8, TILE), F32)
    for h in range(HEADS):
        both = d_out[h * HD : (h + 1) * HD, :].astype(F32) * att[h].astype(F32)
        dl_out[h : h + 1, :] = jnp.sum(both, axis=0, keepdims=True)

    def do_copy(n, mine, h):
        to = 1 - n if mine else n
        rows = slice(h * HD, h * HD + HD)
        return rc(d_out.at[rows], d_near.at[to, rows], do_s.at[n], do_r.at[to, h], near_dev[n])

    def dl_copy(n, mine):
        to = 1 - n if mine else n
        return rc(dl_out, dl_in.at[to], dl_s.at[n], do_r.at[to, 3], near_dev[n])

    half_rows = HD // 2

    def end_grad(h, half):
        rows = slice(h * HD + half * half_rows, h * HD + (half + 1) * half_rows)
        return rc(
            d_out.at[rows], dbuf.at[flow, h], rd_s.at[0], rd_r.at[flow, h], relays[half]
        )

    def forward_grad(h, f):
        rows = pl.ds(pl.multiple_of(h * HD + relay_half * half_rows, 16), half_rows)
        return rc(
            dbuf.at[f, h], d_near.at[f, rows, :], rg_s.at[0], rg_r.at[relay_half, h], relay_to[f]
        )

    def relay_grads(h):
        @pl.when(relay)
        def _():
            for f in range(2):
                ref = dbuf.at[f, h]
                rc(ref, ref, rg_s.at[0], rd_r.at[f, h], relay_to[1 - f]).wait_recv()
                forward_grad(h, f).start()

    def relay_send(h):
        @pl.when(end)
        def _():
            for half in range(2):
                end_grad(h, half).start()

    def send_grads(h):
        for n in range(2):

            @pl.when(plain[n])
            def _():
                do_copy(n, True, h).start()

    def wait_grads(h):
        @pl.when(end)
        def _():
            for half in range(2):
                ref = dbuf.at[0, h]
                rc(ref, ref, rg_s.at[0], rg_r.at[half, h], relays[half]).wait_recv()

        for n in range(2):

            @pl.when(plain[n])
            def _():
                do_copy(n, False, h).wait_recv()

    for n in range(2):

        @pl.when(has[n])
        def _():
            dl_copy(n, True).start()

    relay_send(0)
    grad_w(last)
    d_send(3)
    def backward(h):
        lanes = slice(h * HD, (h + 1) * HD)
        grads = d_out[lanes, :]
        delta = dl_out[h : h + 1, :]
        g = dot(vc[h], grads, 1, 0)
        ds = (probs[h].astype(F32) * (g - delta)).astype(BF16)
        ds_keep[h] = ds[0:TILE, :]
        gq = factor * dot(kc[h], ds, 0, 0)
        q_acc[:, lanes] = gq.T.astype(BF16)
        trows = slice(R_TXT, R_TXT + TXT)
        tx[0:TXT, lanes] = (factor * dot(ds[trows, :], qc[h, 0:TILE, :], 1, 0)).astype(BF16)
        tx[TXT : 2 * TXT, lanes] = dot(probs[h, trows, :], grads, 1, 1).astype(BF16)


    backward(0)
    backward(1)
    y_send(3)
    backward(2)
    q_out = pltpu.make_async_copy(q_acc, o_q, loc.at[6])
    q_out.start()
    t_go(0)
    g_early(1)
    y_take(2)
    send_grads(0)
    relay_send(1)
    relay_grads(0)
    g_early(2)
    y_take(3)
    relay_send(2)
    t_go(1)
    send_grads(1)
    for n in range(2):

        @pl.when(has[n])
        def _():
            dl_copy(n, False).wait_recv()

    def own_keys(h):
        lanes = slice(h * HD, (h + 1) * HD)
        hrows = lanes
        gk = dot(ds_keep[h], qc[h, 0:TILE, :], 1, 0)
        gv = dot(probs[h, 0:TILE, :], d_out[hrows, :], 1, 1)
        for n in range(2):
            grads = d_near[n, hrows, :]
            p = pnear[n, h]
            g = dot(vc[h, 0:TILE, :], grads, 1, 0)
            ds = (p.astype(F32) * (g - dl_in[n, h : h + 1, :])).astype(BF16)
            gk += dot(ds, qc[h, TILE * (n + 1) : TILE * (n + 2), :], 1, 0)
            gv += dot(p, grads, 1, 1)
        k_acc[:, lanes] = (factor * gk).astype(BF16)
        v_acc[:, lanes] = gv.astype(BF16)

    g_late(1)
    relay_grads(1)
    g_early(3)
    send_grads(2)
    relay_grads(2)
    t_go(2)
    wait_grads(0)
    own_keys(0)
    g_late(2)
    g_early(4)
    t_go(3)
    wait_grads(1)
    own_keys(1)
    g_late(3)
    t_go(4)
    wait_grads(2)
    own_keys(2)
    k_out = pltpu.make_async_copy(k_acc, o_k, loc.at[6])
    k_out.start()
    v_out = pltpu.make_async_copy(v_acc, o_v, loc.at[6])
    v_out.start()
    g_early(5)
    g_late(4)
    t_go(5)
    tk_out = pltpu.make_async_copy(t_fin.at[0:TXT], o_tk, loc.at[6])
    tk_out.start()
    tv_out = pltpu.make_async_copy(t_fin.at[TXT : 2 * TXT], o_tv, loc.at[6])
    tv_out.start()
    g_late(5)
    w_out = pltpu.make_async_copy(g_fin, o_w, loc.at[6])
    w_out.start()
    def drain_sends(ref, sem):
        rc(ref, ref, sem, zr.at[0, 0, 0], partner).wait_send()

    for d in range(2):
        drain_sends(sbuf.at[0:3], zs.at[d, 0])
        drain_sends(sbuf.at[0, 0:192], zs.at[d, 1])
    drain_sends(gbuf.at[0:3], ws.at[0])
    drain_sends(g_a, ys.at[0])
    drain_sends(gbuf.at[0:2], ds_.at[0])

    drain(sbuf.at[:, 0:304], loc.at[6])
    for n in range(2):

        @pl.when(plain[n])
        def _():
            drain_sends(kc.at[:, 0 : 2 * TILE], hs_s.at[n])
            q_halo(n, True).wait_send()
            drain_sends(d_out, do_s.at[n])

        @pl.when(has[n])
        def _():
            st_copy(n, True).wait_send()
            dl_copy(n, True).wait_send()

    @pl.when(end)
    def _():
        drain_sends(rbuf, rs_s.at[0])
        drain_sends(dbuf, rd_s.at[0])

    @pl.when(relay)
    def _():
        drain_sends(rbuf, rf_s.at[0])
        drain_sends(dbuf, rg_s.at[0])


def finish(*refs):
    given, results, held, wide, sems = refs[:6], refs[6:12], refs[12:18], refs[18], refs[19]
    loads = [pltpu.make_async_copy(given[i], held[i], sems.at[0, i]) for i in range(6)]
    for i in (5, 0, 1, 2, 3, 4):
        loads[i].start()
    stores = []
    for i in (5, 0, 1, 2, 3, 4):
        loads[i].wait()
        if i == 5:
            wide[...] = held[i][...].astype(F32)
            stores.append(pltpu.make_async_copy(wide, results[i], sems.at[1, i]))
        else:
            stores.append(pltpu.make_async_copy(held[i], results[i].at[0], sems.at[1, i]))
        stores[-1].start()
    for copy in stores:
        copy.wait()


def per_device(
    query, key, value, text_key, text_value, grad_out, gate, out_weight, windows, tile_map, text_count
):
    anyspec = pl.BlockSpec(memory_space=pl.ANY)
    vmem = pl.BlockSpec(memory_space=pltpu.VMEM)
    smem = pl.BlockSpec(memory_space=pltpu.SMEM)
    sds = jax.ShapeDtypeStruct
    v = pltpu.VMEM
    dma = pltpu.SemaphoreType.DMA
    out = pl.pallas_call(
        body,
        out_shape=(
            sds((TILE, TILE), BF16),
            sds((TILE, TILE), BF16),
            sds((TILE, TILE), BF16),
            sds((TXT, TILE), BF16),
            sds((TXT, TILE), BF16),
            sds((TILE, 768), BF16),
        ),
        in_specs=[anyspec] * 8 + [smem] * 3,
        out_specs=(anyspec,) * 6,
        scratch_shapes=[
            v((HEADS, QS, HD), BF16),
            v((HEADS, KEYS, HD), BF16),
            v((HEADS, KEYS, HD), BF16),
            v((TILE, TILE), BF16),
            v((N_TP, TILE, TILE), BF16),
            v((4, TILE, 768), BF16),
            v((HEADS, KEYS, TILE), F32),
            v((HEADS, KEYS, TILE), BF16),
            v((2, HEADS, TILE, TILE), BF16),
            v((HEADS, HD, TILE), BF16),
            v((TILE, TILE), BF16),
            v((TILE, TILE), F32),
            v((2, TILE, TILE), BF16),
            v((2, 8, TILE), F32),
            v((2, 8, TILE), F32),
            v((8, TILE), F32),
            v((2, 8, TILE), F32),
            v((8, TILE), F32),
            v((HEADS, TILE, TILE), BF16),
            v((4, TILE, 768), BF16),
            v((2, TILE, 768), BF16),
            v((TILE, 768), BF16),
            v((TILE, 768), BF16),
            v((TILE, 768), BF16),
            v((192, 768), BF16),
            v((96, 768), BF16),
            v((96, 768), BF16),
            v((96, 768), BF16),
            v((TILE, 768), BF16),
            v((2 * TXT, TILE), BF16),
            v((TXT, TILE), BF16),
            v((TXT // 2, TILE), BF16),
            v((TXT // 2, TILE), BF16),
            v((TXT // 2, TILE), BF16),
            v((2 * TXT, TILE), BF16),
            v((1, TILE), BF16),
            v((TILE, TILE), BF16),
            v((TILE, TILE), BF16),
            v((TILE, TILE), BF16),
            v((2, 9, 192, HD), BF16),
            v((2, HEADS, HD // 2, TILE), BF16),
            dma((7,)),
            dma((2, 2)),
            dma((2, 4, 2)),
            dma((2,)),
            dma((2, HEADS)),
            dma((2,)),
            dma((2,)),
            dma((2,)),
            dma((2,)),
            dma((2,)),
            dma((2, 4)),
            dma((2,)),
            dma((1,)),
            dma((5,)),
            dma((1,)),
            dma((4,)),
            dma((1,)),
            dma((1,)),
            dma((1,)),
            dma((7,)),
            dma((1,)),
            dma((7,)),
            dma((1,)),
            dma((2, 4)),
            dma((1,)),
            dma((2, 4)),
            dma((1,)),
            dma((2, HEADS)),
            dma((1,)),
            dma((2, HEADS)),
        ],
        compiler_params=pltpu.CompilerParams(
            collective_id=0, has_side_effects=True, vmem_limit_bytes=60 * 1024 * 1024
        ),
    )(
        query[0], key[0], value[0], text_key[0], text_value[0], grad_out[0], gate, out_weight,
        windows.reshape(2), tile_map.reshape(8), text_count,
    )
    return pl.pallas_call(
        finish,
        out_shape=(
            sds((1, TILE, TILE), BF16),
            sds((1, TILE, TILE), BF16),
            sds((1, TILE, TILE), BF16),
            sds((1, TXT, TILE), BF16),
            sds((1, TXT, TILE), BF16),
            sds((TILE, 768), F32),
        ),
        in_specs=[anyspec] * 6,
        out_specs=(anyspec,) * 6,
        scratch_shapes=[
            v((TILE, TILE), BF16),
            v((TILE, TILE), BF16),
            v((TILE, TILE), BF16),
            v((TXT, TILE), BF16),
            v((TXT, TILE), BF16),
            v((TILE, 768), BF16),
            v((TILE, 768), F32),
            dma((2, 6)),
        ],
    )(*out)


def solution(mesh):
    placed = (
        P("dp", "sp", "tp"),
        P("dp", "sp", "tp"),
        P("dp", "sp", "tp"),
        P("dp", None, "tp"),
        P("dp", None, "tp"),
        P("dp", "sp", "tp"),
        P("dp", None),
        P("tp", "dp"),
        P("sp", None),
        P(),
        P("dp"),
    )
    return jax.shard_map(
        per_device,
        mesh=mesh,
        in_specs=placed,
        out_specs=(
            P("dp", "sp", "tp"),
            P("dp", "sp", "tp"),
            P("dp", "sp", "tp"),
            P("dp", None, "tp"),
            P("dp", None, "tp"),
            P("tp", "dp"),
        ),
        check_vma=False,
    )
```
